256 devices in a mesh: gx: 32 (over x, y, core), gy: 8 (over z).
Axes of the slice: x: 4, y: 4, z: 8, core: 2. Of those that a mesh axis runs over, the one named last changes fastest.
Arguments:
- rhs_conc: float32 [64, 128, 2048], P('gx', 'gy'), may hold values from -60 to 60
- rhs_pots: float32 [64, 128, 33], P('gx', 'gy'), may hold values from -60 to 60
- diffusion: float32 [64, 128, 32], P('gx', 'gy'), may hold values from 0.05 to 5
- exchange: float32 [64, 128, 32], P('gx', 'gy'), may hold values from 0.2 to 4
- slope: float32 [64, 128, 32], P('gx', 'gy'), may hold values from 0.1 to 1
Outputs:
- sol_conc: float32 [64, 128, 2048], P('gx', 'gy')
- sol_pots: float32 [64, 128, 33], P('gx', 'gy')
The draws below stay inside these ranges and needn't reach their ends.
All inputs are finite; a program needn't handle non-finite values.
Results may differ from the reference program's by a relative error of at most 0.0003.
Values sent between devices are 32-bit elements; how exact they have to be, the bound alone decides.
A program may use at most 64 MiB of HBM per device.

```python
import math
import jax
import jax.numpy as jnp
from jax import lax

NE = 32
NR = 64
ITERS = 10
NX = 64
NY = 128


def column_scale(key):
    scale_key = jax.random.fold_in(key, 7)
    row_place = jnp.arange(NX, dtype=jnp.float32)[:, None] / max(NX - 1, 1)
    spread_field = jnp.exp(jax.random.uniform(scale_key, (NX, NY), jnp.float32) * math.log(10.0))
    scale_field = spread_field * jnp.exp(row_place * math.log(3.0))
    return 0.25 * scale_field


def draw_values(key, width):
    values = jnp.clip(jax.random.normal(key, (NX, NY, width), jnp.float32), -5.0, 5.0)
    return values


def draw_rhs_conc(key, part):
    scale_field = column_scale(key)
    values = draw_values(jax.random.fold_in(key, 11), NE * NR)
    return scale_field[:, :, None] * values


def draw_rhs_pots(key, part):
    scale_field = column_scale(key)
    values = draw_values(jax.random.fold_in(key, 13), NE + 1)
    return scale_field[:, :, None] * values


def levels(stream_key, extent, cuts, low, high):
    def one(position, blocks):
        heights = jax.random.uniform(jax.random.fold_in(jax.random.fold_in(stream_key, 6), position), (blocks,), jnp.float32, low / len(cuts), high / len(cuts))
        return jnp.repeat(jnp.exp(heights), extent[position] // blocks).reshape((-1,) + (1,) * (len(extent) - position - 1))

    gain = one(*cuts[0])
    for cut in cuts[1:]:
        gain = gain * one(*cut)
    return gain


def setup_inputs(seed: int = 0) -> dict:
    seeds = jax.random.split(jax.random.key(seed), 6)
    rhs_conc = draw_rhs_conc(jax.random.fold_in(seeds[5], 71), 0)
    rhs_pots = draw_rhs_pots(jax.random.fold_in(seeds[5], 71), 0)
    diffusion = jnp.clip(jnp.exp(math.log(5.0) - 4.6051702 * jax.random.uniform(seeds[2], (NX, NY, NE), jnp.float32) ** levels(seeds[2], (NX, NY, NE), ((0, 32), (1, 8)), -0.2, 0.2)), 0.05, 5.0)
    exchange = jnp.clip(jnp.exp(math.log(4.0) - 2.9957323 * jax.random.uniform(seeds[3], (NX, NY, NE), jnp.float32) ** levels(seeds[3], (NX, NY, NE), ((0, 32), (1, 8)), -0.2, 0.2)), 0.2, 4.0)
    slope = jnp.clip(0.1 + 0.9 * jax.random.uniform(seeds[4], (NX, NY, NE), jnp.float32) ** levels(seeds[4], (NX, NY, NE), ((0, 32), (1, 8)), -0.2, 0.2), 0.1, 1.0)
    return dict(rhs_conc=rhs_conc, rhs_pots=rhs_pots, diffusion=diffusion, exchange=exchange, slope=slope)


node_cond = 1.0
plane_cond = 0.5
collector_cond = 2.0
epsilon = 1e-06

def mirror_laplace(values):
    inner = jnp.concatenate([values[..., :1], values[..., :-1]], axis=-1)
    outer = jnp.concatenate([values[..., 1:], values[..., -1:]], axis=-1)
    return 2.0 * values - inner - outer

def local_operator(conc, padded, diffusion, exchange, slope):
    nodes = exchange.shape[2]
    shell_count = conc.shape[2] // nodes
    shells = conc.reshape(conc.shape[0], conc.shape[1], nodes, shell_count)
    center = padded[1:-1, 1:-1]
    lateral = 4.0 * center - padded[2:, 1:-1] - padded[:-2, 1:-1] - padded[1:-1, 2:] - padded[1:-1, :-2]
    node_pot = center[..., :nodes]
    collector = center[..., nodes]
    current = exchange * (node_pot - collector[..., None])
    surface = shells[..., shell_count - 1]
    surface_flag = (lax.broadcasted_iota(jnp.int32, (shell_count,), 0) == shell_count - 1).astype(jnp.float32)
    new_shells = shells + diffusion[..., None] * mirror_laplace(shells) + current[..., None] * surface_flag
    new_nodes = node_cond * mirror_laplace(node_pot) + current - slope * surface + plane_cond * lateral[..., :nodes]
    new_collector = collector_cond * lateral[..., nodes] - lax.optimization_barrier(jnp.mean(current, axis=-1))
    return (new_shells.reshape(conc.shape), jnp.concatenate([new_nodes, new_collector[..., None]], axis=-1))

def least_squares(columns, start_norm):
    count = len(columns)
    target = [start_norm] + [jnp.zeros_like(start_norm) for step in range(count)]
    cosines = []
    sines = []
    upper_rows = []
    for step in range(count):
        entries = list(columns[step])
        for row in range(step):
            first = cosines[row] * entries[row] + sines[row] * entries[row + 1]
            second = cosines[row] * entries[row + 1] - sines[row] * entries[row]
            entries[row] = first
            entries[row + 1] = second
        radius = jnp.sqrt(entries[step] * entries[step] + entries[step + 1] * entries[step + 1])
        cosine = entries[step] / radius
        sine = entries[step + 1] / radius
        entries[step] = radius
        cosines.append(cosine)
        sines.append(sine)
        lead = target[step]
        target[step] = cosine * lead
        target[step + 1] = -sine * lead
        upper_rows.append(entries[:step + 1])
    weights = [None] * count
    for row in range(count - 1, -1, -1):
        total = target[row]
        for later in range(row + 1, count):
            total = total - upper_rows[later][row] * weights[later]
        weights[row] = total / upper_rows[row][row]
    return weights

def apply_operator(conc, pots, diffusion, exchange, slope):
    padded = jnp.pad(pots, ((1, 1), (1, 1), (0, 0)))
    return local_operator(conc, padded, diffusion, exchange, slope)

def reference(rhs_conc, rhs_pots, diffusion, exchange, slope):
    start_norm = jnp.sqrt(jnp.sum(rhs_conc * rhs_conc) + jnp.sum(rhs_pots * rhs_pots) + epsilon)
    basis = [(rhs_conc / start_norm, rhs_pots / start_norm)]
    columns = []
    for step in range(ITERS):
        image_conc, image_pots = apply_operator(basis[step][0], basis[step][1], diffusion, exchange, slope)
        coeffs = [jnp.sum(vector[0] * image_conc) + jnp.sum(vector[1] * image_pots) for vector in basis]
        rest_conc, rest_pots = (image_conc, image_pots)
        for row in range(step + 1):
            rest_conc = rest_conc - coeffs[row] * basis[row][0]
            rest_pots = rest_pots - coeffs[row] * basis[row][1]
        height = jnp.sqrt(jnp.sum(rest_conc * rest_conc) + jnp.sum(rest_pots * rest_pots) + epsilon)
        basis.append((rest_conc / height, rest_pots / height))
        columns.append(coeffs + [height])
    weights = least_squares(columns, start_norm)
    sol_conc = weights[0] * basis[0][0]
    sol_pots = weights[0] * basis[0][1]
    for step in range(1, ITERS):
        sol_conc = sol_conc + weights[step] * basis[step][0]
        sol_pots = sol_pots + weights[step] * basis[step][1]
    return (sol_conc, sol_pots)
```

```python
import functools
import jax
import jax.numpy as jnp
from jax import lax
from jax.experimental import pallas as pl
from jax.experimental.pallas import tpu as pltpu
from jax.sharding import Mesh
from jax.sharding import PartitionSpec as P

ITERS = 10
MESH = pl.DeviceIdType.MESH
GX = ("gx_0", "gx_1", "gx_2")

node_cond = 1.0
plane_cond = 0.5
collector_cond = 2.0
epsilon = 1e-06

CENTER = 11.0
HALF = 10.0
TRUST = 1e-4

CELLS = 32
SHELLS = 64
DIM = ITERS + 1


def kernel(nx, ny, conc, pots, diff, exch, slope, out_c, out_p, flag,
           tall, vecs, planes, halo, rows, sums_a, sums_b,
           hs_sem, hr_sem, as_sem, ar_sem, bs_sem, br_sem):
    n_a = nx // 2
    n_b = 2 * ny
    gx = lax.axis_index("gx")
    gy = lax.axis_index("gy")
    core = lax.rem(gx, 2)
    col = lax.div(gx, 2)
    slot_a = col
    slot_b = core * ny + gy

    def peer_a(step):
        other = lax.rem(col + step, n_a)
        return other, (other * 2 + core, gy)

    def peer_b(step):
        other = lax.rem(slot_b + step, n_b)
        return other, (col * 2 + lax.div(other, ny), lax.rem(other, ny))

    sends = (
        (gx < nx - 1, (gx + 1, gy)),
        (gx > 0, (gx - 1, gy)),
        (gy < ny - 1, (gx, gy + 1)),
        (gy > 0, (gx, gy - 1)),
    )
    receives = (gx > 0, gx < nx - 1, gy > 0, gy < ny - 1)

    barrier = pltpu.get_barrier_semaphore()
    for exists, device in sends:
        @pl.when(exists)
        def _(device=device):
            pl.semaphore_signal(barrier, inc=1, device_id=device, device_id_type=MESH)
    for step in range(1, n_a):
        pl.semaphore_signal(barrier, inc=1, device_id=peer_a(step)[1], device_id_type=MESH)
    for step in range(1, n_b):
        pl.semaphore_signal(barrier, inc=1, device_id=peer_b(step)[1], device_id_type=MESH)

    lane = lax.broadcasted_iota(jnp.int32, (8, 128), 1)
    sub = lax.broadcasted_iota(jnp.int32, (8, 128), 0)
    quarter = lane // 32
    x_of = (lane // 16) % 2
    y_of = lane % 16
    once = jnp.logical_and(sub == 0, quarter == 0)
    zero = jnp.zeros((8, 128), jnp.float32)

    for d in range(4):
        @pl.when(jnp.logical_not(receives[d]))
        def _(d=d):
            for k in range(ITERS):
                halo[k, d] = jnp.zeros((16, 128), jnp.float32)

    def spread(by_node):
        parts = [by_node[8 * q:8 * q + 8, :] for q in range(4)]
        return jnp.concatenate(parts, axis=1)

    def small(ref):
        return spread(ref[...].reshape(CELLS, CELLS).T)

    diffusion = small(diff)
    exchange = small(exch)
    slopes = small(slope)
    pots_t = pots[...].reshape(CELLS, CELLS + 1).T
    pot = spread(pots_t[:CELLS])
    collector = jnp.broadcast_to(
        jnp.concatenate([pots_t[CELLS:CELLS + 1]] * 4, axis=1), (8, 128))
    planes[0, 0:8] = pot
    planes[0, 8:16] = collector
    rows[...] = jnp.zeros((128, 128), jnp.float32)

    flat = conc[...].reshape(CELLS, 2048)
    for g in range(4):
        block = jnp.concatenate(
            [flat[:, (4 * q + g) * 128:(4 * q + g + 1) * 128] for q in range(4)], axis=0)
        tall[g * 128:(g + 1) * 128, :] = block.T

    def first(b, acc):
        for i in range(8):
            r = b * 8 + i
            shell = tall[pl.ds(r, 8, stride=SHELLS), :]
            vecs[0, r] = shell
            acc = acc + shell * shell
        return acc

    def keep(k, i, acc):
        total = jnp.sum(acc, axis=0, keepdims=True)
        rows[DIM * k + i:DIM * k + i + 1, :] = total
        if i != k:
            rows[DIM * i + k:DIM * i + k + 1, :] = total

    acc = lax.fori_loop(0, 8, first, zero)
    keep(0, 0, acc + pot * pot + jnp.where(once, collector * collector, 0.0))

    pl.semaphore_wait(barrier, n_a + n_b - 2 + sum(r.astype(jnp.int32) for r in receives))

    def halo_copy(k, d):
        return pltpu.make_async_remote_copy(
            src_ref=planes.at[k],
            dst_ref=halo.at[k, d],
            send_sem=hs_sem.at[k, d],
            recv_sem=hr_sem.at[k, d],
            device_id=sends[d][1],
            device_id_type=MESH,
        )

    def send_halo(k):
        for d in range(4):
            @pl.when(sends[d][0])
            def _(d=d):
                halo_copy(k, d).start()

    send_halo(0)

    def lateral_inside(v):
        return (4.0 * v
                - jnp.where(x_of == 1, pltpu.roll(v, 16, 1), pltpu.roll(v, 112, 1))
                - jnp.where(y_of > 0, pltpu.roll(v, 1, 1), 0.0)
                - jnp.where(y_of < 15, pltpu.roll(v, 127, 1), 0.0))

    def lateral_outside(k, at):
        low_x, high_x, low_y, high_y = (halo[k, d, at:at + 8] for d in range(4))
        return (jnp.where(x_of == 0, pltpu.roll(low_x, 112, 1), pltpu.roll(high_x, 16, 1))
                + jnp.where(y_of == 0, pltpu.roll(low_y, 113, 1), 0.0)
                + jnp.where(y_of == 15, pltpu.roll(high_y, 15, 1), 0.0))

    def node_mirror(v):
        down = pltpu.roll(v, 1, 0)
        down = jnp.where(sub == 0, pltpu.roll(down, 32, 1), down)
        down = jnp.where(jnp.logical_and(sub == 0, quarter == 0), v, down)
        up = pltpu.roll(v, 7, 0)
        up = jnp.where(sub == 7, pltpu.roll(up, 96, 1), up)
        up = jnp.where(jnp.logical_and(sub == 7, quarter == 3), v, up)
        return 2.0 * v - down - up

    def over_nodes(v):
        v = jnp.broadcast_to(jnp.sum(v, axis=0, keepdims=True), (8, 128))
        v = v + pltpu.roll(v, 64, 1)
        return v + pltpu.roll(v, 32, 1)

    for k in range(ITERS):
        scale = (1.0 if k == 0 else 2.0) / HALF
        pot = planes[k, 0:8]
        collector = planes[k, 8:16]
        current = exchange * (pot - collector)
        own_pot = scale * (
            node_cond * node_mirror(pot) + current - slopes * vecs[k, SHELLS - 1]
            + plane_cond * lateral_inside(pot) - CENTER * pot)
        own_collector = scale * (
            collector_cond * lateral_inside(collector) - over_nodes(current) * (1.0 / 32.0)
            - CENTER * collector)
        if k > 0:
            own_pot = own_pot - planes[k - 1, 0:8]
            own_collector = own_collector - planes[k - 1, 8:16]
        center_coef = scale * (1.0 - CENTER + 2.0 * diffusion)
        side_coef = scale * diffusion

        def shells(base, accs, last, k=k, center_coef=center_coef, side_coef=side_coef,
                   scale=scale, current=current):
            accs = list(accs)
            low = vecs[k, jnp.maximum(base - 1, 0)]
            here = vecs[k, base]
            for i in range(8):
                r = base + i
                high = here if last and i == 7 else vecs[k, r + 1]
                new = center_coef * here - side_coef * (low + high)
                if last and i == 7:
                    new = new + scale * current
                if k > 0:
                    new = new - vecs[k - 1, r]
                vecs[k + 1, r] = new
                for m in range(k):
                    accs[m] = accs[m] + new * vecs[m, r]
                accs[k] = accs[k] + new * here
                accs[k + 1] = accs[k + 1] + new * new
                low, here = here, high
            return tuple(accs)

        accs = lax.fori_loop(
            0, 7, lambda b, accs: shells(b * 8, accs, False), (zero,) * (k + 2))
        accs = shells(SHELLS - 8, accs, True)

        for d in range(4):
            @pl.when(receives[d])
            def _(d=d):
                halo_copy(k, d).wait_recv()
        new_pot = own_pot - (scale * plane_cond) * lateral_outside(k, 0)
        new_collector = own_collector - (scale * collector_cond) * lateral_outside(k, 8)
        planes[k + 1, 0:8] = new_pot
        planes[k + 1, 8:16] = new_collector
        if k + 1 < ITERS:
            send_halo(k + 1)
        for m in range(k + 2):
            acc = accs[m] + new_pot * planes[m, 0:8] + jnp.where(
                once, new_collector * planes[m, 8:16], 0.0)
            keep(k + 1, m, acc)

    def total(mine, count, slot, peer, sums, s_sem, r_sem):
        sums[pl.ds(slot, 1)] = mine.reshape(1, 1, 128)

        def copy(step):
            other, device = peer(step)
            return other, pltpu.make_async_remote_copy(
                src_ref=sums.at[slot],
                dst_ref=sums.at[slot],
                send_sem=s_sem.at[step],
                recv_sem=r_sem.at[slot],
                device_id=device,
                device_id_type=MESH,
            )

        for step in range(1, count):
            copy(step)[1].start()
        for step in range(1, count):
            other = peer(step)[0]
            pltpu.make_async_remote_copy(
                src_ref=sums.at[other],
                dst_ref=sums.at[other],
                send_sem=s_sem.at[step],
                recv_sem=r_sem.at[other],
                device_id=peer(step)[1],
                device_id_type=MESH,
            ).wait_recv()
        return jnp.sum(sums[...], axis=0), copy

    mine = jnp.sum(rows[...].T, axis=0, keepdims=True)
    part, copy_a = total(mine, n_a, slot_a, peer_a, sums_a, as_sem, ar_sem)
    whole, copy_b = total(part, n_b, slot_b, peer_b, sums_b, bs_sem, br_sem)

    lane2 = lax.broadcasted_iota(jnp.int32, (16, 128), 1)
    sub2 = lax.broadcasted_iota(jnp.int32, (16, 128), 0)
    eye = sub2 == lane2
    whole = jnp.broadcast_to(whole, (16, 128))
    gram = jnp.zeros((16, 128), jnp.float32)
    for k in range(DIM):
        moved = whole if k == 0 else pltpu.roll(whole, (128 - DIM * k) % 128, 1)
        gram = jnp.where(sub2 == k, moved, gram)
    gram = jnp.where(lane2 < DIM, gram, 0.0)

    def down(v):
        return jnp.broadcast_to(jnp.sum(v, axis=0, keepdims=True), (16, 128))

    def turned(v):
        return jnp.broadcast_to(
            jnp.sum(jnp.where(eye, v, 0.0), axis=1, keepdims=True), (16, 128))

    diagonal = jnp.broadcast_to(
        jnp.sum(jnp.where(eye, gram, 0.0), axis=1, keepdims=True), (16, 128))
    lengths = jnp.sqrt(jnp.maximum(diagonal, 0.0))
    beta = jnp.sqrt(jnp.broadcast_to(diagonal[0:1], (16, 128)) + epsilon)
    inverse = 1.0 / beta
    up_coef = jnp.where(sub2 == 1, HALF, HALF / 2)
    down_coef = jnp.where(sub2 < ITERS, HALF / 2, 0.0)
    g_lane = jnp.broadcast_to(gram[0:1], (16, 128)) * inverse
    c_lane = jnp.where(lane2 == 0, inverse, 0.0)
    g_sub = turned(g_lane)
    c_sub = jnp.where(sub2 == 0, inverse, 0.0)
    rest_t = jnp.where(eye, 1.0, 0.0) - g_sub * c_lane
    gram_rest_t = gram - g_sub * g_lane
    images = jnp.where(lane2 == 0, g_sub, 0.0)
    coords = [c_sub]
    trust = jnp.ones((16, 128), jnp.float32)

    cosines, sines, inverse_radii, upper = [], [], [], []
    target = [beta[0:1]]
    for j in range(ITERS):
        w_sub = (CENTER * c_sub + up_coef * pltpu.roll(c_sub, 1, 0)
                 + down_coef * pltpu.roll(c_sub, 15, 0))
        u_lane = down(rest_t * w_sub)
        gu_lane = down(gram_rest_t * w_sub)
        h_lane = down(images * w_sub)
        u_sub, gu_sub, h_sub = turned(u_lane), turned(gu_lane), turned(h_lane)
        square = down(u_sub * gu_sub)
        spread_square = down(jnp.abs(u_sub) * lengths)
        trust = jnp.where(square > TRUST * spread_square * spread_square, trust, 0.0)
        height = jnp.sqrt(jnp.maximum(square, 0.0) + epsilon)
        inverse = 1.0 / height
        if j + 1 < ITERS:
            c_sub, g_sub = u_sub * inverse, gu_sub * inverse
            c_lane, g_lane = u_lane * inverse, gu_lane * inverse
            rest_t = rest_t - g_sub * c_lane
            gram_rest_t = gram_rest_t - g_sub * g_lane
            images = jnp.where(lane2 == j + 1, g_sub, images)
            coords.append(c_sub)
        entries = [h_sub[i:i + 1] for i in range(j + 1)] + [height[0:1]]
        for row in range(j):
            entries[row], entries[row + 1] = (
                cosines[row] * entries[row] + sines[row] * entries[row + 1],
                cosines[row] * entries[row + 1] - sines[row] * entries[row])
        radius = jnp.sqrt(entries[j] * entries[j] + entries[j + 1] * entries[j + 1])
        inverse_radius = 1.0 / radius
        cosines.append(entries[j] * inverse_radius)
        sines.append(entries[j + 1] * inverse_radius)
        inverse_radii.append(inverse_radius)
        upper.append(entries[:j])
        lead = target[j]
        target[j] = cosines[j] * lead
        target.append(-sines[j] * lead)
    weights = [None] * ITERS
    for row in range(ITERS - 1, -1, -1):
        value = target[row]
        for later in range(ITERS - 1, row, -1):
            value = value - upper[later][row] * weights[later]
        weights[row] = value * inverse_radii[row]
    coef = weights[0] * coords[0]
    for j in range(1, ITERS):
        coef = coef + weights[j] * coords[j]
    flag[...] = trust[0:8]
    coefs = [jnp.broadcast_to(coef[k:k + 1], (8, 128)) for k in range(ITERS)]

    def combine(b, carry):
        for i in range(8):
            r = b * 8 + i
            value = coefs[0] * vecs[0, r]
            for k in range(1, ITERS):
                value = value + coefs[k] * vecs[k, r]
            tall[pl.ds(r, 8, stride=SHELLS), :] = value
        return carry

    lax.fori_loop(0, 8, combine, 0)
    sol = coefs[0] * planes[0, 0:8]
    sol_collector = coefs[0] * planes[0, 8:16]
    for k in range(1, ITERS):
        sol = sol + coefs[k] * planes[k, 0:8]
        sol_collector = sol_collector + coefs[k] * planes[k, 8:16]
    for g in range(4):
        block = tall[g * 128:(g + 1) * 128, :].T
        for q in range(4):
            at = (4 * q + g) * 128
            out_c[:, :, at:at + 128] = block[q * 32:(q + 1) * 32].reshape(2, 16, 128)
    by_node = [sol if q == 0 else pltpu.roll(sol, 128 - 32 * q, 1) for q in range(4)]
    by_node = jnp.concatenate(by_node + [sol_collector] + [jnp.zeros((88, 128), jnp.float32)], axis=0)
    out_p[...] = by_node.T[:CELLS, :CELLS + 1].reshape(2, 16, CELLS + 1)

    for k in range(ITERS):
        for d in range(4):
            @pl.when(sends[d][0])
            def _(k=k, d=d):
                halo_copy(k, d).wait_send()
    for step in range(1, n_a):
        copy_a(step)[1].wait_send()
    for step in range(1, n_b):
        copy_b(step)[1].wait_send()


def fast(nx, ny, *args):
    n_a, n_b = nx // 2, 2 * ny
    f32 = jnp.float32
    vmem = pl.BlockSpec(memory_space=pltpu.VMEM)
    return pl.pallas_call(
        functools.partial(kernel, nx, ny),
        out_shape=(
            jax.ShapeDtypeStruct(args[0].shape, f32),
            jax.ShapeDtypeStruct(args[1].shape, f32),
            jax.ShapeDtypeStruct((8, 128), f32),
        ),
        in_specs=[vmem] * 5,
        out_specs=(vmem,) * 3,
        scratch_shapes=[
            pltpu.VMEM((512, 128), f32),
            pltpu.VMEM((DIM, SHELLS, 8, 128), f32),
            pltpu.VMEM((DIM, 16, 128), f32),
            pltpu.VMEM((ITERS, 4, 16, 128), f32),
            pltpu.VMEM((128, 128), f32),
            pltpu.VMEM((n_a, 1, 128), f32),
            pltpu.VMEM((n_b, 1, 128), f32),
            pltpu.SemaphoreType.DMA((ITERS, 4)),
            pltpu.SemaphoreType.DMA((ITERS, 4)),
            pltpu.SemaphoreType.DMA((n_a,)),
            pltpu.SemaphoreType.DMA((n_a,)),
            pltpu.SemaphoreType.DMA((n_b,)),
            pltpu.SemaphoreType.DMA((n_b,)),
        ],
        compiler_params=pltpu.CompilerParams(collective_id=0, has_side_effects=True),
    )(*args)


def with_halo(shard, sides, width):
    edges = {}
    for axis, dim in sides:
        size, length = (lax.axis_size(axis), shard.shape[dim])
        up = [(i, (i + 1) % size) for i in range(size - 1)]
        last = lax.slice_in_dim(shard, length - width, length, axis=dim)
        initial = lax.slice_in_dim(shard, 0, width, axis=dim)
        edges[dim] = (
            lax.ppermute(last, axis, up),
            lax.ppermute(initial, axis, [(b, a) for a, b in up]),
        )
    done = []
    for _, dim in sides:
        low, high = edges[dim]
        around = [(width, width) if d in done else (0, 0) for d in range(shard.ndim)]
        shard = jnp.concatenate([jnp.pad(low, around), shard, jnp.pad(high, around)], axis=dim)
        done.append(dim)
    return shard


def total_of(shard):
    return lax.all_gather(shard, ("gx", "gy")).sum(axis=0)


def mirror_laplace(values):
    inner = jnp.concatenate([values[..., :1], values[..., :-1]], axis=-1)
    outer = jnp.concatenate([values[..., 1:], values[..., -1:]], axis=-1)
    return 2.0 * values - inner - outer


def local_operator(conc, padded, diffusion, exchange, slope):
    nodes = exchange.shape[2]
    shell_count = conc.shape[2] // nodes
    shells = conc.reshape(conc.shape[0], conc.shape[1], nodes, shell_count)
    center = padded[1:-1, 1:-1]
    lateral = (
        4.0 * center - padded[2:, 1:-1] - padded[:-2, 1:-1] - padded[1:-1, 2:] - padded[1:-1, :-2]
    )
    node_pot = center[..., :nodes]
    collector = center[..., nodes]
    current = exchange * (node_pot - collector[..., None])
    surface = shells[..., shell_count - 1]
    surface_flag = (lax.broadcasted_iota(jnp.int32, (shell_count,), 0) == shell_count - 1).astype(
        jnp.float32
    )
    new_shells = (
        shells + diffusion[..., None] * mirror_laplace(shells) + current[..., None] * surface_flag
    )
    new_nodes = (
        node_cond * mirror_laplace(node_pot)
        + current
        - slope * surface
        + plane_cond * lateral[..., :nodes]
    )
    new_collector = collector_cond * lateral[..., nodes] - jnp.mean(current, axis=-1)
    return (
        new_shells.reshape(conc.shape),
        jnp.concatenate([new_nodes, new_collector[..., None]], axis=-1),
    )


def step_by_step(rhs_conc, rhs_pots, diffusion, exchange, slope):
    first = jnp.sum(rhs_conc * rhs_conc) + jnp.sum(rhs_pots * rhs_pots)
    start_norm = jnp.sqrt(total_of(first.reshape(1))[0] + epsilon)
    all_conc = jnp.zeros((DIM, *rhs_conc.shape), jnp.float32).at[0].set(rhs_conc / start_norm)
    all_pots = jnp.zeros((DIM, *rhs_pots.shape), jnp.float32).at[0].set(rhs_pots / start_norm)
    matrix = jnp.zeros((DIM, DIM), jnp.float32)

    def arnoldi(step, state):
        all_conc, all_pots, matrix = state
        padded = with_halo(all_pots[step], (("gx", 0), ("gy", 1)), 1)
        image_conc, image_pots = local_operator(all_conc[step], padded, diffusion, exchange, slope)
        local_dots = jnp.sum(all_conc * image_conc, axis=(1, 2, 3)) + jnp.sum(
            all_pots * image_pots, axis=(1, 2, 3))
        coeffs = total_of(local_dots)
        rest_conc = image_conc - jnp.sum(coeffs[:, None, None, None] * all_conc, axis=0)
        rest_pots = image_pots - jnp.sum(coeffs[:, None, None, None] * all_pots, axis=0)
        rest = jnp.sum(rest_conc * rest_conc) + jnp.sum(rest_pots * rest_pots)
        height = jnp.sqrt(total_of(rest.reshape(1))[0] + epsilon)
        column = jnp.where(jnp.arange(DIM) == step + 1, height, coeffs)
        return (
            lax.dynamic_update_index_in_dim(all_conc, rest_conc / height, step + 1, 0),
            lax.dynamic_update_index_in_dim(all_pots, rest_pots / height, step + 1, 0),
            lax.dynamic_update_index_in_dim(matrix, column, step, 0),
        )

    all_conc, all_pots, matrix = lax.fori_loop(
        0, ITERS, arnoldi, (all_conc, all_pots, matrix))

    def rotate(step, state):
        matrix, target = state
        pair = matrix[step]
        lead, under = pair[step], pair[step + 1]
        radius = jnp.sqrt(lead * lead + under * under)
        cosine, sine = lead / radius, under / radius

        def turn(values):
            a = lax.dynamic_index_in_dim(values, step, values.ndim - 1)
            b = lax.dynamic_index_in_dim(values, step + 1, values.ndim - 1)
            values = lax.dynamic_update_slice_in_dim(
                values, cosine * a + sine * b, step, values.ndim - 1)
            return lax.dynamic_update_slice_in_dim(
                values, cosine * b - sine * a, step + 1, values.ndim - 1)

        return turn(matrix), turn(target)

    target = jnp.zeros((DIM,), jnp.float32).at[0].set(start_norm)
    matrix, target = lax.fori_loop(0, ITERS, rotate, (matrix, target))

    def back(i, weights):
        row = ITERS - 1 - i
        known = jnp.sum(matrix[:, row] * weights)
        return weights.at[row].set((target[row] - known) / matrix[row, row])

    weights = lax.fori_loop(0, ITERS, back, jnp.zeros((DIM,), jnp.float32))
    weights = weights[:, None, None, None]
    return jnp.sum(weights * all_conc, axis=0), jnp.sum(weights * all_pots, axis=0)


def solution(mesh):
    nx, ny = mesh.shape["gx"], mesh.shape["gy"]

    def shards(*args):
        conc, pots, flag = fast(nx, ny, *args)

        def again(state):
            conc, pots = step_by_step(*args)
            return conc, pots, jnp.ones_like(state[2])

        return lax.while_loop(
            lambda state: state[2] < 0.5, again, (conc, pots, jnp.min(flag)))[:2]

    spec = P("gx", "gy", None)
    return jax.shard_map(
        shards, mesh=mesh, in_specs=(spec,) * 5, out_specs=(spec,) * 2, check_vma=False)
```

```python
import functools
import jax
import jax.numpy as jnp
from jax import lax
from jax.experimental import pallas as pl
from jax.experimental.pallas import tpu as pltpu
from jax.sharding import Mesh
from jax.sharding import PartitionSpec as P

ITERS = 10
MESH = pl.DeviceIdType.MESH
GX = ("gx_0", "gx_1", "gx_2")

node_cond = 1.0
plane_cond = 0.5
collector_cond = 2.0
epsilon = 1e-06

ROUNDS = (5, 5)
CENTER = 11.0
HALF = 10.0
TRUST = 1e-4

CELLS = 32
SHELLS = 64
DIM = ITERS + 1
STARTS = tuple(sum(ROUNDS[:i]) for i in range(len(ROUNDS)))


def steps_away(block):
    a, b = block
    return max(2 * abs(a) - 1, 0) + abs(b)


DEEPEST = max(ROUNDS)
BLOCKS = sorted(
    ((a, b) for a in range(-DEEPEST, DEEPEST + 1) for b in (-1, 0, 1)
     if 0 < steps_away((a, b)) <= DEEPEST),
    key=lambda block: (-steps_away(block), block))
SLOT = {block: i for i, block in enumerate(BLOCKS)}
COEFS = 24
OUTBOX = 16 + COEFS + 8 * (DEEPEST - 1)


def message_rows(turn, block):
    updates = ROUNDS[turn] - steps_away(block)
    if updates < 0:
        return 0
    if updates == 0:
        return 16
    return 16 + (COEFS if turn == 0 else 0) + 8 * updates


def is_first(k):
    return k in STARTS


def kernel(nx, ny, conc, pots, diff, exch, slope, out_c, out_p, flag,
           tall, vecs, planes, outbox, halo, rows, sums_a, sums_b,
           hs_sem, hr_sem, as_sem, ar_sem, bs_sem, br_sem):
    n_a = nx // 2
    n_b = 2 * ny
    gx = lax.axis_index("gx")
    gy = lax.axis_index("gy")
    core = lax.rem(gx, 2)
    col = lax.div(gx, 2)
    slot_a = col
    slot_b = core * ny + gy

    def peer_a(step):
        other = lax.rem(col + step, n_a)
        return other, (other * 2 + core, gy)

    def peer_b(step):
        other = lax.rem(slot_b + step, n_b)
        return other, (col * 2 + lax.div(other, ny), lax.rem(other, ny))

    exists = {}
    for a, b in BLOCKS:
        inside = []
        if a:
            inside.append(gx + a < nx if a > 0 else gx + a >= 0)
        if b:
            inside.append(gy + b < ny if b > 0 else gy + b >= 0)
        exists[a, b] = inside[0] if len(inside) == 1 else jnp.logical_and(*inside)

    barrier = pltpu.get_barrier_semaphore()
    for step in range(1, n_b):
        pl.semaphore_signal(barrier, inc=1, device_id=peer_b(step)[1], device_id_type=MESH)
    for step in range(1, n_a):
        pl.semaphore_signal(barrier, inc=1, device_id=peer_a(step)[1], device_id_type=MESH)
    expected = n_a + n_b - 2
    for block in BLOCKS:
        @pl.when(exists[block])
        def _(block=block):
            pl.semaphore_signal(
                barrier, inc=1, device_id=(gx + block[0], gy + block[1]), device_id_type=MESH)
        expected = expected + exists[block].astype(jnp.int32)

    lane = lax.broadcasted_iota(jnp.int32, (8, 128), 1)
    sub = lax.broadcasted_iota(jnp.int32, (8, 128), 0)
    quarter = lane // 32
    x_of = (lane // 16) % 2
    y_of = lane % 16
    once = jnp.logical_and(sub == 0, quarter == 0)
    zero = jnp.zeros((8, 128), jnp.float32)

    for block in BLOCKS:
        @pl.when(jnp.logical_not(exists[block]))
        def _(block=block):
            for turn in range(len(ROUNDS)):
                count = message_rows(turn, block)
                if count:
                    halo[turn, SLOT[block], 0:count] = jnp.zeros((count, 128), jnp.float32)

    def spread(by_node):
        parts = [by_node[8 * q:8 * q + 8, :] for q in range(4)]
        return jnp.concatenate(parts, axis=1)

    def small(ref):
        return spread(ref[...].reshape(CELLS, CELLS).T)

    diffusion = small(diff)
    exchange = small(exch)
    slopes = small(slope)
    pots_t = pots[...].reshape(CELLS, CELLS + 1).T
    pot = spread(pots_t[:CELLS])
    collector = jnp.broadcast_to(
        jnp.concatenate([pots_t[CELLS:CELLS + 1]] * 4, axis=1), (8, 128))
    planes[0, 0:8] = pot
    planes[0, 8:16] = collector
    outbox[0, 0:8] = pot
    outbox[0, 8:16] = collector
    outbox[0, 16:24] = exchange
    outbox[0, 24:32] = slopes
    outbox[0, 32:40] = diffusion
    rows[...] = jnp.zeros((128, 128), jnp.float32)

    flat = conc[...].reshape(CELLS, 2048)
    for g in range(4):
        block = jnp.concatenate(
            [flat[:, (4 * q + g) * 128:(4 * q + g + 1) * 128] for q in range(4)], axis=0)
        tall[g * 128:(g + 1) * 128, :] = block.T
    for i in range(ROUNDS[0] - 1):
        outbox[0, 40 + 8 * i:48 + 8 * i] = tall[pl.ds(SHELLS - 1 - i, 8, stride=SHELLS), :]

    def first(b, acc):
        for i in range(8):
            r = b * 8 + i
            shell = tall[pl.ds(r, 8, stride=SHELLS), :]
            vecs[0, r] = shell
            acc = acc + shell * shell
        return acc

    def keep(k, i, acc):
        total = jnp.sum(acc, axis=0, keepdims=True)
        rows[DIM * k + i:DIM * k + i + 1, :] = total
        if i != k:
            rows[DIM * i + k:DIM * i + k + 1, :] = total

    def halo_copy(turn, block):
        a, b = block
        count = message_rows(turn, block)
        return pltpu.make_async_remote_copy(
            src_ref=outbox.at[turn, pl.ds(0, count)],
            dst_ref=halo.at[turn, SLOT[-a, -b], pl.ds(0, count)],
            send_sem=hs_sem.at[turn, SLOT[block]],
            recv_sem=hr_sem.at[turn, SLOT[-a, -b]],
            device_id=(gx + a, gy + b),
            device_id_type=MESH,
        )

    def each_message(turn, act):
        for block in BLOCKS:
            if message_rows(turn, block):
                @pl.when(exists[block])
                def _(block=block):
                    act(block)

    def receive(turn, block):
        a, b = block
        count = message_rows(turn, block)
        pltpu.make_async_remote_copy(
            src_ref=outbox.at[turn, pl.ds(0, count)],
            dst_ref=halo.at[turn, SLOT[block], pl.ds(0, count)],
            send_sem=hs_sem.at[turn, SLOT[block]],
            recv_sem=hr_sem.at[turn, SLOT[block]],
            device_id=(gx + a, gy + b),
            device_id_type=MESH,
        ).wait_recv()

    def send_round(turn):
        each_message(turn, lambda block: halo_copy(turn, block).start())

    pl.semaphore_wait(barrier, expected)
    send_round(0)
    acc = lax.fori_loop(0, 8, first, zero)
    keep(0, 0, acc + pot * pot + jnp.where(once, collector * collector, 0.0))

    def around(own, low_x, high_x, low_y, high_y):
        high = own if high_x is None else own + high_x
        low = own if low_x is None else own + low_x
        before = 0.0 if low_y is None else pltpu.roll(low_y, 113, 1)
        after = 0.0 if high_y is None else pltpu.roll(high_y, 15, 1)
        return (jnp.where(x_of == 1, pltpu.roll(high, 16, 1), pltpu.roll(low, 112, 1))
                + jnp.where(y_of > 0, pltpu.roll(own, 1, 1), before)
                + jnp.where(y_of < 15, pltpu.roll(own, 127, 1), after))

    def node_mirror(v):
        down = pltpu.roll(v, 1, 0)
        down = jnp.where(sub == 0, pltpu.roll(down, 32, 1), down)
        down = jnp.where(jnp.logical_and(sub == 0, quarter == 0), v, down)
        up = pltpu.roll(v, 7, 0)
        up = jnp.where(sub == 7, pltpu.roll(up, 96, 1), up)
        up = jnp.where(jnp.logical_and(sub == 7, quarter == 3), v, up)
        return 2.0 * v - down - up

    def over_nodes(v):
        v = jnp.broadcast_to(jnp.sum(v, axis=0, keepdims=True), (8, 128))
        v = v + pltpu.roll(v, 64, 1)
        return v + pltpu.roll(v, 32, 1)

    def potentials(turn):
        depth, start = ROUNDS[turn], STARTS[turn]
        carried = ROUNDS[turn + 1] - 1 if turn + 1 < len(ROUNDS) else 0
        own = (0, 0)
        now = {own: (planes[start, 0:8], planes[start, 8:16],
                     [vecs[start, SHELLS - 1 - i] for i in range(depth + carried)])}
        coefs = {own: (exchange, slopes, diffusion)}
        for block in BLOCKS:
            if message_rows(turn, block) == 0:
                continue
            updates = depth - steps_away(block)
            inbox = halo.at[turn, SLOT[block]]
            shells_at = 16 + (COEFS if turn == 0 else 0)
            now[block] = (inbox[0:8], inbox[8:16],
                          [inbox[shells_at + 8 * i:shells_at + 8 * i + 8] for i in range(updates)])
            if updates:
                source = halo.at[0, SLOT[block]]
                coefs[block] = (source[16:24], source[24:32], source[32:40])
        before = None
        for m in range(1, depth + 1):
            scale = (1.0 if m == 1 else 2.0) / HALF
            after = {}
            for block in now:
                if steps_away(block) > depth - m:
                    continue
                a, b = block
                pot, collector, shells = now[block]
                exchange_of, slope_of, diffusion_of = coefs[block]
                beside = [now.get(other) for other in (
                    (a - 1, b), (a + 1, b), (a, b - 1), (a, b + 1))]

                def lateral(which, own):
                    return 4.0 * own - around(
                        own, *(None if other is None else other[which] for other in beside))

                current = exchange_of * (pot - collector)
                new_pot = scale * (
                    node_cond * node_mirror(pot) + current - slope_of * shells[0]
                    + plane_cond * lateral(0, pot) - CENTER * pot)
                new_collector = scale * (
                    collector_cond * lateral(1, collector)
                    - over_nodes(current) * (1.0 / 32.0) - CENTER * collector)
                count = depth - m + carried if block == own_block else depth - steps_away(block) - m
                center_coef = scale * (1.0 - CENTER + 2.0 * diffusion_of)
                side_coef = scale * diffusion_of
                new_shells = []
                for i in range(count):
                    new = center_coef * shells[i] - side_coef * (shells[max(i - 1, 0)] + shells[i + 1])
                    if i == 0:
                        new = new + scale * current
                    if m > 1:
                        new = new - before[block][2][i]
                    new_shells.append(new)
                if m > 1:
                    new_pot = new_pot - before[block][0]
                    new_collector = new_collector - before[block][1]
                if block != own_block:
                    new_pot = jnp.where(exists[block], new_pot, 0.0)
                    new_collector = jnp.where(exists[block], new_collector, 0.0)
                after[block] = (new_pot, new_collector, new_shells)
            planes[start + m, 0:8] = after[own_block][0]
            planes[start + m, 8:16] = after[own_block][1]
            before, now = now, after
        if turn + 1 < len(ROUNDS):
            outbox[turn + 1, 0:8] = now[own_block][0]
            outbox[turn + 1, 8:16] = now[own_block][1]
            for i in range(carried):
                outbox[turn + 1, 16 + 8 * i:24 + 8 * i] = now[own_block][2][i]

    own_block = (0, 0)

    def bulk_shells(k):
        scale = (1.0 if is_first(k) else 2.0) / HALF
        current = exchange * (planes[k, 0:8] - planes[k, 8:16])
        center_coef = scale * (1.0 - CENTER + 2.0 * diffusion)
        side_coef = scale * diffusion

        def shells(base, accs, last):
            accs = list(accs)
            low = vecs[k, jnp.maximum(base - 1, 0)]
            here = vecs[k, base]
            for i in range(8):
                r = base + i
                high = here if last and i == 7 else vecs[k, r + 1]
                new = center_coef * here - side_coef * (low + high)
                if last and i == 7:
                    new = new + scale * current
                if not is_first(k):
                    new = new - vecs[k - 1, r]
                vecs[k + 1, r] = new
                for m in range(k):
                    accs[m] = accs[m] + new * vecs[m, r]
                accs[k] = accs[k] + new * here
                accs[k + 1] = accs[k + 1] + new * new
                low, here = here, high
            return tuple(accs)

        accs = lax.fori_loop(
            0, 7, lambda b, accs: shells(b * 8, accs, False), (zero,) * (k + 2))
        return shells(SHELLS - 8, accs, True)

    def products(k, accs):
        new_pot, new_collector = planes[k + 1, 0:8], planes[k + 1, 8:16]
        for m in range(k + 2):
            acc = accs[m] + new_pot * planes[m, 0:8] + jnp.where(
                once, new_collector * planes[m, 8:16], 0.0)
            keep(k + 1, m, acc)

    for turn, start in enumerate(STARTS):
        accs = bulk_shells(start)
        each_message(turn, functools.partial(receive, turn))
        potentials(turn)
        if turn + 1 < len(ROUNDS):
            send_round(turn + 1)
        products(start, accs)
        for k in range(start + 1, start + ROUNDS[turn]):
            products(k, bulk_shells(k))

    def total(mine, count, slot, peer, sums, s_sem, r_sem):
        sums[pl.ds(slot, 1)] = mine.reshape(1, 1, 128)

        def copy(step):
            other, device = peer(step)
            return other, pltpu.make_async_remote_copy(
                src_ref=sums.at[slot],
                dst_ref=sums.at[slot],
                send_sem=s_sem.at[step],
                recv_sem=r_sem.at[slot],
                device_id=device,
                device_id_type=MESH,
            )

        for step in range(1, count):
            copy(step)[1].start()
        for step in range(1, count):
            other = peer(step)[0]
            pltpu.make_async_remote_copy(
                src_ref=sums.at[other],
                dst_ref=sums.at[other],
                send_sem=s_sem.at[step],
                recv_sem=r_sem.at[other],
                device_id=peer(step)[1],
                device_id_type=MESH,
            ).wait_recv()
        return jnp.sum(sums[...], axis=0), copy

    mine = jnp.sum(rows[...].T, axis=0, keepdims=True)
    part, copy_a = total(mine, n_a, slot_a, peer_a, sums_a, as_sem, ar_sem)
    whole, copy_b = total(part, n_b, slot_b, peer_b, sums_b, bs_sem, br_sem)

    lane2 = lax.broadcasted_iota(jnp.int32, (16, 128), 1)
    sub2 = lax.broadcasted_iota(jnp.int32, (16, 128), 0)
    eye = sub2 == lane2
    whole = jnp.broadcast_to(whole, (16, 128))
    gram = jnp.zeros((16, 128), jnp.float32)
    for k in range(DIM):
        moved = whole if k == 0 else pltpu.roll(whole, (128 - DIM * k) % 128, 1)
        gram = jnp.where(sub2 == k, moved, gram)
    gram = jnp.where(lane2 < DIM, gram, 0.0)

    def down(v):
        return jnp.broadcast_to(jnp.sum(v, axis=0, keepdims=True), (16, 128))

    def turned(v):
        return jnp.broadcast_to(
            jnp.sum(jnp.where(eye, v, 0.0), axis=1, keepdims=True), (16, 128))

    diagonal = jnp.broadcast_to(
        jnp.sum(jnp.where(eye, gram, 0.0), axis=1, keepdims=True), (16, 128))
    lengths = jnp.sqrt(jnp.maximum(diagonal, 0.0))
    beta = jnp.sqrt(jnp.broadcast_to(diagonal[0:1], (16, 128)) + epsilon)
    inverse = 1.0 / beta
    up_coef = jnp.zeros((16, 128), jnp.float32)
    down_coef = jnp.zeros((16, 128), jnp.float32)
    for k in range(ITERS):
        up_coef = jnp.where(sub2 == k + 1, HALF if is_first(k) else HALF / 2, up_coef)
        if not is_first(k):
            down_coef = jnp.where(sub2 == k - 1, HALF / 2, down_coef)
    g_lane = jnp.broadcast_to(gram[0:1], (16, 128)) * inverse
    c_lane = jnp.where(lane2 == 0, inverse, 0.0)
    g_sub = turned(g_lane)
    c_sub = jnp.where(sub2 == 0, inverse, 0.0)
    rest_t = jnp.where(eye, 1.0, 0.0) - g_sub * c_lane
    gram_rest_t = gram - g_sub * g_lane
    images = jnp.where(lane2 == 0, g_sub, 0.0)
    coords = [c_sub]
    trust = jnp.ones((16, 128), jnp.float32)

    cosines, sines, inverse_radii, upper = [], [], [], []
    target = [beta[0:1]]
    for j in range(ITERS):
        w_sub = (CENTER * c_sub + up_coef * pltpu.roll(c_sub, 1, 0)
                 + down_coef * pltpu.roll(c_sub, 15, 0))
        u_lane = down(rest_t * w_sub)
        gu_lane = down(gram_rest_t * w_sub)
        h_lane = down(images * w_sub)
        u_sub, gu_sub, h_sub = turned(u_lane), turned(gu_lane), turned(h_lane)
        square = down(u_sub * gu_sub)
        spread_square = down(jnp.abs(u_sub) * lengths)
        trust = jnp.where(square > TRUST * spread_square * spread_square, trust, 0.0)
        height = jnp.sqrt(jnp.maximum(square, 0.0) + epsilon)
        inverse = 1.0 / height
        if j + 1 < ITERS:
            c_sub, g_sub = u_sub * inverse, gu_sub * inverse
            c_lane, g_lane = u_lane * inverse, gu_lane * inverse
            rest_t = rest_t - g_sub * c_lane
            gram_rest_t = gram_rest_t - g_sub * g_lane
            images = jnp.where(lane2 == j + 1, g_sub, images)
            coords.append(c_sub)
        entries = [h_sub[i:i + 1] for i in range(j + 1)] + [height[0:1]]
        for row in range(j):
            entries[row], entries[row + 1] = (
                cosines[row] * entries[row] + sines[row] * entries[row + 1],
                cosines[row] * entries[row + 1] - sines[row] * entries[row])
        radius = jnp.sqrt(entries[j] * entries[j] + entries[j + 1] * entries[j + 1])
        inverse_radius = 1.0 / radius
        cosines.append(entries[j] * inverse_radius)
        sines.append(entries[j + 1] * inverse_radius)
        inverse_radii.append(inverse_radius)
        upper.append(entries[:j])
        lead = target[j]
        target[j] = cosines[j] * lead
        target.append(-sines[j] * lead)
    weights = [None] * ITERS
    for row in range(ITERS - 1, -1, -1):
        value = target[row]
        for later in range(ITERS - 1, row, -1):
            value = value - upper[later][row] * weights[later]
        weights[row] = value * inverse_radii[row]
    coef = weights[0] * coords[0]
    for j in range(1, ITERS):
        coef = coef + weights[j] * coords[j]
    flag[...] = trust[0:8]
    coefs = [jnp.broadcast_to(coef[k:k + 1], (8, 128)) for k in range(ITERS)]

    def combine(b, carry):
        for i in range(8):
            r = b * 8 + i
            value = coefs[0] * vecs[0, r]
            for k in range(1, ITERS):
                value = value + coefs[k] * vecs[k, r]
            tall[pl.ds(r, 8, stride=SHELLS), :] = value
        return carry

    lax.fori_loop(0, 8, combine, 0)
    sol = coefs[0] * planes[0, 0:8]
    sol_collector = coefs[0] * planes[0, 8:16]
    for k in range(1, ITERS):
        sol = sol + coefs[k] * planes[k, 0:8]
        sol_collector = sol_collector + coefs[k] * planes[k, 8:16]
    for g in range(4):
        block = tall[g * 128:(g + 1) * 128, :].T
        for q in range(4):
            at = (4 * q + g) * 128
            out_c[:, :, at:at + 128] = block[q * 32:(q + 1) * 32].reshape(2, 16, 128)
    by_node = [sol if q == 0 else pltpu.roll(sol, 128 - 32 * q, 1) for q in range(4)]
    by_node = jnp.concatenate(by_node + [sol_collector] + [jnp.zeros((88, 128), jnp.float32)], axis=0)
    out_p[...] = by_node.T[:CELLS, :CELLS + 1].reshape(2, 16, CELLS + 1)

    for turn in range(len(ROUNDS)):
        each_message(turn, lambda block: halo_copy(turn, block).wait_send())
    for step in range(1, n_a):
        copy_a(step)[1].wait_send()
    for step in range(1, n_b):
        copy_b(step)[1].wait_send()


def fast(nx, ny, *args):
    n_a, n_b = nx // 2, 2 * ny
    f32 = jnp.float32
    vmem = pl.BlockSpec(memory_space=pltpu.VMEM)
    return pl.pallas_call(
        functools.partial(kernel, nx, ny),
        out_shape=(
            jax.ShapeDtypeStruct(args[0].shape, f32),
            jax.ShapeDtypeStruct(args[1].shape, f32),
            jax.ShapeDtypeStruct((8, 128), f32),
        ),
        in_specs=[vmem] * 5,
        out_specs=(vmem,) * 3,
        scratch_shapes=[
            pltpu.VMEM((512, 128), f32),
            pltpu.VMEM((DIM, SHELLS, 8, 128), f32),
            pltpu.VMEM((DIM, 16, 128), f32),
            pltpu.VMEM((len(ROUNDS), OUTBOX, 128), f32),
            pltpu.VMEM((len(ROUNDS), len(BLOCKS), OUTBOX, 128), f32),
            pltpu.VMEM((128, 128), f32),
            pltpu.VMEM((n_a, 1, 128), f32),
            pltpu.VMEM((n_b, 1, 128), f32),
            pltpu.SemaphoreType.DMA((len(ROUNDS), len(BLOCKS))),
            pltpu.SemaphoreType.DMA((len(ROUNDS), len(BLOCKS))),
            pltpu.SemaphoreType.DMA((n_a,)),
            pltpu.SemaphoreType.DMA((n_a,)),
            pltpu.SemaphoreType.DMA((n_b,)),
            pltpu.SemaphoreType.DMA((n_b,)),
        ],
        compiler_params=pltpu.CompilerParams(collective_id=0, has_side_effects=True),
    )(*args)


def with_halo(shard, sides, width):
    edges = {}
    for axis, dim in sides:
        size, length = (lax.axis_size(axis), shard.shape[dim])
        up = [(i, (i + 1) % size) for i in range(size - 1)]
        last = lax.slice_in_dim(shard, length - width, length, axis=dim)
        initial = lax.slice_in_dim(shard, 0, width, axis=dim)
        edges[dim] = (
            lax.ppermute(last, axis, up),
            lax.ppermute(initial, axis, [(b, a) for a, b in up]),
        )
    done = []
    for _, dim in sides:
        low, high = edges[dim]
        around = [(width, width) if d in done else (0, 0) for d in range(shard.ndim)]
        shard = jnp.concatenate([jnp.pad(low, around), shard, jnp.pad(high, around)], axis=dim)
        done.append(dim)
    return shard


def total_of(shard):
    return lax.all_gather(shard, ("gx", "gy")).sum(axis=0)


def mirror_laplace(values):
    inner = jnp.concatenate([values[..., :1], values[..., :-1]], axis=-1)
    outer = jnp.concatenate([values[..., 1:], values[..., -1:]], axis=-1)
    return 2.0 * values - inner - outer


def local_operator(conc, padded, diffusion, exchange, slope):
    nodes = exchange.shape[2]
    shell_count = conc.shape[2] // nodes
    shells = conc.reshape(conc.shape[0], conc.shape[1], nodes, shell_count)
    center = padded[1:-1, 1:-1]
    lateral = (
        4.0 * center - padded[2:, 1:-1] - padded[:-2, 1:-1] - padded[1:-1, 2:] - padded[1:-1, :-2]
    )
    node_pot = center[..., :nodes]
    collector = center[..., nodes]
    current = exchange * (node_pot - collector[..., None])
    surface = shells[..., shell_count - 1]
    surface_flag = (lax.broadcasted_iota(jnp.int32, (shell_count,), 0) == shell_count - 1).astype(
        jnp.float32
    )
    new_shells = (
        shells + diffusion[..., None] * mirror_laplace(shells) + current[..., None] * surface_flag
    )
    new_nodes = (
        node_cond * mirror_laplace(node_pot)
        + current
        - slope * surface
        + plane_cond * lateral[..., :nodes]
    )
    new_collector = collector_cond * lateral[..., nodes] - jnp.mean(current, axis=-1)
    return (
        new_shells.reshape(conc.shape),
        jnp.concatenate([new_nodes, new_collector[..., None]], axis=-1),
    )


def step_by_step(rhs_conc, rhs_pots, diffusion, exchange, slope):
    first = jnp.sum(rhs_conc * rhs_conc) + jnp.sum(rhs_pots * rhs_pots)
    start_norm = jnp.sqrt(total_of(first.reshape(1))[0] + epsilon)
    all_conc = jnp.zeros((DIM, *rhs_conc.shape), jnp.float32).at[0].set(rhs_conc / start_norm)
    all_pots = jnp.zeros((DIM, *rhs_pots.shape), jnp.float32).at[0].set(rhs_pots / start_norm)
    matrix = jnp.zeros((DIM, DIM), jnp.float32)

    def arnoldi(step, state):
        all_conc, all_pots, matrix = state
        padded = with_halo(all_pots[step], (("gx", 0), ("gy", 1)), 1)
        image_conc, image_pots = local_operator(all_conc[step], padded, diffusion, exchange, slope)
        local_dots = jnp.sum(all_conc * image_conc, axis=(1, 2, 3)) + jnp.sum(
            all_pots * image_pots, axis=(1, 2, 3))
        coeffs = total_of(local_dots)
        rest_conc = image_conc - jnp.sum(coeffs[:, None, None, None] * all_conc, axis=0)
        rest_pots = image_pots - jnp.sum(coeffs[:, None, None, None] * all_pots, axis=0)
        rest = jnp.sum(rest_conc * rest_conc) + jnp.sum(rest_pots * rest_pots)
        height = jnp.sqrt(total_of(rest.reshape(1))[0] + epsilon)
        column = jnp.where(jnp.arange(DIM) == step + 1, height, coeffs)
        return (
            lax.dynamic_update_index_in_dim(all_conc, rest_conc / height, step + 1, 0),
            lax.dynamic_update_index_in_dim(all_pots, rest_pots / height, step + 1, 0),
            lax.dynamic_update_index_in_dim(matrix, column, step, 0),
        )

    all_conc, all_pots, matrix = lax.fori_loop(
        0, ITERS, arnoldi, (all_conc, all_pots, matrix))

    def rotate(step, state):
        matrix, target = state
        pair = matrix[step]
        lead, under = pair[step], pair[step + 1]
        radius = jnp.sqrt(lead * lead + under * under)
        cosine, sine = lead / radius, under / radius

        def turn(values):
            a = lax.dynamic_index_in_dim(values, step, values.ndim - 1)
            b = lax.dynamic_index_in_dim(values, step + 1, values.ndim - 1)
            values = lax.dynamic_update_slice_in_dim(
                values, cosine * a + sine * b, step, values.ndim - 1)
            return lax.dynamic_update_slice_in_dim(
                values, cosine * b - sine * a, step + 1, values.ndim - 1)

        return turn(matrix), turn(target)

    target = jnp.zeros((DIM,), jnp.float32).at[0].set(start_norm)
    matrix, target = lax.fori_loop(0, ITERS, rotate, (matrix, target))

    def back(i, weights):
        row = ITERS - 1 - i
        known = jnp.sum(matrix[:, row] * weights)
        return weights.at[row].set((target[row] - known) / matrix[row, row])

    weights = lax.fori_loop(0, ITERS, back, jnp.zeros((DIM,), jnp.float32))
    weights = weights[:, None, None, None]
    return jnp.sum(weights * all_conc, axis=0), jnp.sum(weights * all_pots, axis=0)


def solution(mesh):
    nx, ny = mesh.shape["gx"], mesh.shape["gy"]

    def shards(*args):
        conc, pots, flag = fast(nx, ny, *args)

        def again(state):
            conc, pots = step_by_step(*args)
            return conc, pots, jnp.ones_like(state[2])

        return lax.while_loop(
            lambda state: state[2] < 0.5, again, (conc, pots, jnp.min(flag)))[:2]

    spec = P("gx", "gy", None)
    return jax.shard_map(
        shards, mesh=mesh, in_specs=(spec,) * 5, out_specs=(spec,) * 2, check_vma=False)
```

```python
import functools
import jax
import jax.numpy as jnp
from jax import lax
from jax.experimental import pallas as pl
from jax.experimental.pallas import tpu as pltpu
from jax.sharding import Mesh
from jax.sharding import PartitionSpec as P

ITERS = 10
MESH = pl.DeviceIdType.MESH
GX = ("gx_0", "gx_1", "gx_2")

node_cond = 1.0
plane_cond = 0.5
collector_cond = 2.0
epsilon = 1e-06

ROUNDS = (5, 5)
CENTER = 11.0
HALF = 10.0
TRUST = 1e-4

CELLS = 32
SHELLS = 64
DIM = ITERS + 1
STARTS = tuple(sum(ROUNDS[:i]) for i in range(len(ROUNDS)))


def steps_away(block):
    a, b = block
    return max(2 * abs(a) - 1, 0) + abs(b)


DEEPEST = max(ROUNDS)
BLOCKS = sorted(
    ((a, b) for a in range(-DEEPEST, DEEPEST + 1) for b in (-1, 0, 1)
     if 0 < steps_away((a, b)) <= DEEPEST),
    key=lambda block: (-steps_away(block), block))
SLOT = {block: i for i, block in enumerate(BLOCKS)}
COEFS = 24
OUTBOX = 16 + COEFS + 8 * (DEEPEST - 1)


def message_rows(turn, block):
    updates = ROUNDS[turn] - steps_away(block)
    if updates < 0:
        return 0
    if updates == 0:
        return 16
    return 16 + (COEFS if turn == 0 else 0) + 8 * updates


def is_first(k):
    return k in STARTS


def kernel(nx, ny, conc, pots, diff, exch, slope, tall_out, plane_out, flag,
           tall, vecs, planes, outbox, halo, rows, sums_a, sums_b,
           hs_sem, hr_sem, as_sem, ar_sem, bs_sem, br_sem):
    n_a = nx // 2
    n_b = 2 * ny
    gx = lax.axis_index("gx")
    gy = lax.axis_index("gy")
    core = lax.rem(gx, 2)
    col = lax.div(gx, 2)
    slot_a = col
    slot_b = core * ny + gy

    def peer_a(step):
        other = lax.rem(col + step, n_a)
        return other, (other * 2 + core, gy)

    def peer_b(step):
        other = lax.rem(slot_b + step, n_b)
        return other, (col * 2 + lax.div(other, ny), lax.rem(other, ny))

    exists = {}
    for a, b in BLOCKS:
        inside = []
        if a:
            inside.append(gx + a < nx if a > 0 else gx + a >= 0)
        if b:
            inside.append(gy + b < ny if b > 0 else gy + b >= 0)
        exists[a, b] = inside[0] if len(inside) == 1 else jnp.logical_and(*inside)

    barrier = pltpu.get_barrier_semaphore()
    for step in range(1, n_b):
        pl.semaphore_signal(barrier, inc=1, device_id=peer_b(step)[1], device_id_type=MESH)
    for step in range(1, n_a):
        pl.semaphore_signal(barrier, inc=1, device_id=peer_a(step)[1], device_id_type=MESH)
    expected = n_a + n_b - 2
    for block in BLOCKS:
        @pl.when(exists[block])
        def _(block=block):
            pl.semaphore_signal(
                barrier, inc=1, device_id=(gx + block[0], gy + block[1]), device_id_type=MESH)
        expected = expected + exists[block].astype(jnp.int32)

    lane = lax.broadcasted_iota(jnp.int32, (8, 128), 1)
    sub = lax.broadcasted_iota(jnp.int32, (8, 128), 0)
    quarter = lane // 32
    x_of = (lane // 16) % 2
    y_of = lane % 16
    once = jnp.logical_and(sub == 0, quarter == 0)
    zero = jnp.zeros((8, 128), jnp.float32)

    for block in BLOCKS:
        @pl.when(jnp.logical_not(exists[block]))
        def _(block=block):
            for turn in range(len(ROUNDS)):
                count = message_rows(turn, block)
                if count:
                    halo[turn, SLOT[block], 0:count] = jnp.zeros((count, 128), jnp.float32)

    def spread(by_node):
        parts = [by_node[8 * q:8 * q + 8, :] for q in range(4)]
        return jnp.concatenate(parts, axis=1)

    def small(ref):
        return spread(ref[...].reshape(CELLS, CELLS).T)

    diffusion = small(diff)
    exchange = small(exch)
    slopes = small(slope)
    pots_t = pots[...].reshape(CELLS, CELLS + 1).T
    pot = spread(pots_t[:CELLS])
    collector = jnp.broadcast_to(
        jnp.concatenate([pots_t[CELLS:CELLS + 1]] * 4, axis=1), (8, 128))
    planes[0, 0:8] = pot
    planes[0, 8:16] = collector
    outbox[0, 0:8] = pot
    outbox[0, 8:16] = collector
    outbox[0, 16:24] = exchange
    outbox[0, 24:32] = slopes
    outbox[0, 32:40] = diffusion
    rows[...] = jnp.zeros((128, 128), jnp.float32)

    flat = conc[...].reshape(CELLS, 2048)
    for g in range(4):
        block = jnp.concatenate(
            [flat[:, (4 * q + g) * 128:(4 * q + g + 1) * 128] for q in range(4)], axis=0)
        tall[g * 128:(g + 1) * 128, :] = block.T
    for i in range(ROUNDS[0] - 1):
        outbox[0, 40 + 8 * i:48 + 8 * i] = tall[pl.ds(SHELLS - 1 - i, 8, stride=SHELLS), :]

    def first(b, acc):
        for i in range(8):
            r = b * 8 + i
            shell = tall[pl.ds(r, 8, stride=SHELLS), :]
            vecs[0, r] = shell
            acc = acc + shell * shell
        return acc

    def keep(k, i, acc):
        total = jnp.sum(acc, axis=0, keepdims=True)
        rows[DIM * k + i:DIM * k + i + 1, :] = total
        if i != k:
            rows[DIM * i + k:DIM * i + k + 1, :] = total

    def halo_copy(turn, block):
        a, b = block
        count = message_rows(turn, block)
        return pltpu.make_async_remote_copy(
            src_ref=outbox.at[turn, pl.ds(0, count)],
            dst_ref=halo.at[turn, SLOT[-a, -b], pl.ds(0, count)],
            send_sem=hs_sem.at[turn, SLOT[block]],
            recv_sem=hr_sem.at[turn, SLOT[-a, -b]],
            device_id=(gx + a, gy + b),
            device_id_type=MESH,
        )

    def each_message(turn, act):
        for block in BLOCKS:
            if message_rows(turn, block):
                @pl.when(exists[block])
                def _(block=block):
                    act(block)

    def receive(turn, block):
        a, b = block
        count = message_rows(turn, block)
        pltpu.make_async_remote_copy(
            src_ref=outbox.at[turn, pl.ds(0, count)],
            dst_ref=halo.at[turn, SLOT[block], pl.ds(0, count)],
            send_sem=hs_sem.at[turn, SLOT[block]],
            recv_sem=hr_sem.at[turn, SLOT[block]],
            device_id=(gx + a, gy + b),
            device_id_type=MESH,
        ).wait_recv()

    def send_round(turn):
        each_message(turn, lambda block: halo_copy(turn, block).start())

    pl.semaphore_wait(barrier, expected)
    send_round(0)
    acc = lax.fori_loop(0, 8, first, zero)
    keep(0, 0, acc + pot * pot + jnp.where(once, collector * collector, 0.0))

    def around(own, low_x, high_x, low_y, high_y):
        high = own if high_x is None else own + high_x
        low = own if low_x is None else own + low_x
        before = 0.0 if low_y is None else pltpu.roll(low_y, 113, 1)
        after = 0.0 if high_y is None else pltpu.roll(high_y, 15, 1)
        return (jnp.where(x_of == 1, pltpu.roll(high, 16, 1), pltpu.roll(low, 112, 1))
                + jnp.where(y_of > 0, pltpu.roll(own, 1, 1), before)
                + jnp.where(y_of < 15, pltpu.roll(own, 127, 1), after))

    def node_mirror(v):
        down = pltpu.roll(v, 1, 0)
        down = jnp.where(sub == 0, pltpu.roll(down, 32, 1), down)
        down = jnp.where(jnp.logical_and(sub == 0, quarter == 0), v, down)
        up = pltpu.roll(v, 7, 0)
        up = jnp.where(sub == 7, pltpu.roll(up, 96, 1), up)
        up = jnp.where(jnp.logical_and(sub == 7, quarter == 3), v, up)
        return 2.0 * v - down - up

    def over_nodes(v):
        v = jnp.broadcast_to(jnp.sum(v, axis=0, keepdims=True), (8, 128))
        v = v + pltpu.roll(v, 64, 1)
        return v + pltpu.roll(v, 32, 1)

    def potentials(turn):
        depth, start = ROUNDS[turn], STARTS[turn]
        carried = ROUNDS[turn + 1] - 1 if turn + 1 < len(ROUNDS) else 0
        own = (0, 0)
        now = {own: (planes[start, 0:8], planes[start, 8:16],
                     [vecs[start, SHELLS - 1 - i] for i in range(depth + carried)])}
        coefs = {own: (exchange, slopes, diffusion)}
        for block in BLOCKS:
            if message_rows(turn, block) == 0:
                continue
            updates = depth - steps_away(block)
            inbox = halo.at[turn, SLOT[block]]
            shells_at = 16 + (COEFS if turn == 0 else 0)
            now[block] = (inbox[0:8], inbox[8:16],
                          [inbox[shells_at + 8 * i:shells_at + 8 * i + 8] for i in range(updates)])
            if updates:
                source = halo.at[0, SLOT[block]]
                coefs[block] = (source[16:24], source[24:32], source[32:40])
        before = None
        for m in range(1, depth + 1):
            scale = (1.0 if m == 1 else 2.0) / HALF
            after = {}
            for block in now:
                if steps_away(block) > depth - m:
                    continue
                a, b = block
                pot, collector, shells = now[block]
                exchange_of, slope_of, diffusion_of = coefs[block]
                beside = [now.get(other) for other in (
                    (a - 1, b), (a + 1, b), (a, b - 1), (a, b + 1))]

                def lateral(which, own):
                    return 4.0 * own - around(
                        own, *(None if other is None else other[which] for other in beside))

                current = exchange_of * (pot - collector)
                new_pot = scale * (
                    node_cond * node_mirror(pot) + current - slope_of * shells[0]
                    + plane_cond * lateral(0, pot) - CENTER * pot)
                new_collector = scale * (
                    collector_cond * lateral(1, collector)
                    - over_nodes(current) * (1.0 / 32.0) - CENTER * collector)
                count = depth - m + carried if block == own_block else depth - steps_away(block) - m
                center_coef = scale * (1.0 - CENTER + 2.0 * diffusion_of)
                side_coef = scale * diffusion_of
                new_shells = []
                for i in range(count):
                    new = center_coef * shells[i] - side_coef * (shells[max(i - 1, 0)] + shells[i + 1])
                    if i == 0:
                        new = new + scale * current
                    if m > 1:
                        new = new - before[block][2][i]
                    new_shells.append(new)
                if m > 1:
                    new_pot = new_pot - before[block][0]
                    new_collector = new_collector - before[block][1]
                if block != own_block:
                    new_pot = jnp.where(exists[block], new_pot, 0.0)
                    new_collector = jnp.where(exists[block], new_collector, 0.0)
                after[block] = (new_pot, new_collector, new_shells)
            planes[start + m, 0:8] = after[own_block][0]
            planes[start + m, 8:16] = after[own_block][1]
            before, now = now, after
        if turn + 1 < len(ROUNDS):
            outbox[turn + 1, 0:8] = now[own_block][0]
            outbox[turn + 1, 8:16] = now[own_block][1]
            for i in range(carried):
                outbox[turn + 1, 16 + 8 * i:24 + 8 * i] = now[own_block][2][i]

    own_block = (0, 0)

    def bulk_shells(k):
        scale = (1.0 if is_first(k) else 2.0) / HALF
        current = exchange * (planes[k, 0:8] - planes[k, 8:16])
        center_coef = scale * (1.0 - CENTER + 2.0 * diffusion)
        side_coef = scale * diffusion

        def shells(base, accs, last):
            accs = list(accs)
            low = vecs[k, jnp.maximum(base - 1, 0)]
            here = vecs[k, base]
            for i in range(8):
                r = base + i
                high = here if last and i == 7 else vecs[k, r + 1]
                new = center_coef * here - side_coef * (low + high)
                if last and i == 7:
                    new = new + scale * current
                if not is_first(k):
                    new = new - vecs[k - 1, r]
                vecs[k + 1, r] = new
                for m in range(k):
                    accs[m] = accs[m] + new * vecs[m, r]
                accs[k] = accs[k] + new * here
                accs[k + 1] = accs[k + 1] + new * new
                low, here = here, high
            return tuple(accs)

        accs = lax.fori_loop(
            0, 7, lambda b, accs: shells(b * 8, accs, False), (zero,) * (k + 2))
        return shells(SHELLS - 8, accs, True)

    def products(k, accs):
        new_pot, new_collector = planes[k + 1, 0:8], planes[k + 1, 8:16]
        for m in range(k + 2):
            acc = accs[m] + new_pot * planes[m, 0:8] + jnp.where(
                once, new_collector * planes[m, 8:16], 0.0)
            keep(k + 1, m, acc)

    for turn, start in enumerate(STARTS):
        accs = bulk_shells(start)
        each_message(turn, functools.partial(receive, turn))
        potentials(turn)
        if turn + 1 < len(ROUNDS):
            send_round(turn + 1)
        products(start, accs)
        for k in range(start + 1, start + ROUNDS[turn]):
            products(k, bulk_shells(k))

    def total(mine, count, slot, peer, sums, s_sem, r_sem):
        sums[pl.ds(slot, 1)] = mine.reshape(1, 1, 128)

        def copy(step):
            other, device = peer(step)
            return other, pltpu.make_async_remote_copy(
                src_ref=sums.at[slot],
                dst_ref=sums.at[slot],
                send_sem=s_sem.at[step],
                recv_sem=r_sem.at[slot],
                device_id=device,
                device_id_type=MESH,
            )

        for step in range(1, count):
            copy(step)[1].start()
        for step in range(1, count):
            other = peer(step)[0]
            pltpu.make_async_remote_copy(
                src_ref=sums.at[other],
                dst_ref=sums.at[other],
                send_sem=s_sem.at[step],
                recv_sem=r_sem.at[other],
                device_id=peer(step)[1],
                device_id_type=MESH,
            ).wait_recv()
        return jnp.sum(sums[...], axis=0), copy

    mine = jnp.sum(rows[...].T, axis=0, keepdims=True)
    part, copy_a = total(mine, n_a, slot_a, peer_a, sums_a, as_sem, ar_sem)
    whole, copy_b = total(part, n_b, slot_b, peer_b, sums_b, bs_sem, br_sem)

    lane2 = lax.broadcasted_iota(jnp.int32, (16, 128), 1)
    sub2 = lax.broadcasted_iota(jnp.int32, (16, 128), 0)
    eye = sub2 == lane2
    whole = jnp.broadcast_to(whole, (16, 128))
    gram = jnp.zeros((16, 128), jnp.float32)
    for k in range(DIM):
        moved = whole if k == 0 else pltpu.roll(whole, (128 - DIM * k) % 128, 1)
        gram = jnp.where(sub2 == k, moved, gram)
    gram = jnp.where(lane2 < DIM, gram, 0.0)

    def down(v):
        return jnp.broadcast_to(jnp.sum(v, axis=0, keepdims=True), (16, 128))

    def turned(v):
        return jnp.broadcast_to(
            jnp.sum(jnp.where(eye, v, 0.0), axis=1, keepdims=True), (16, 128))

    diagonal = jnp.broadcast_to(
        jnp.sum(jnp.where(eye, gram, 0.0), axis=1, keepdims=True), (16, 128))
    lengths = jnp.sqrt(jnp.maximum(diagonal, 0.0))
    beta = jnp.sqrt(jnp.broadcast_to(diagonal[0:1], (16, 128)) + epsilon)
    inverse = 1.0 / beta
    up_coef = jnp.zeros((16, 128), jnp.float32)
    down_coef = jnp.zeros((16, 128), jnp.float32)
    for k in range(ITERS):
        up_coef = jnp.where(sub2 == k + 1, HALF if is_first(k) else HALF / 2, up_coef)
        if not is_first(k):
            down_coef = jnp.where(sub2 == k - 1, HALF / 2, down_coef)
    g_lane = jnp.broadcast_to(gram[0:1], (16, 128)) * inverse
    c_lane = jnp.where(lane2 == 0, inverse, 0.0)
    g_sub = turned(g_lane)
    c_sub = jnp.where(sub2 == 0, inverse, 0.0)
    rest_t = jnp.where(eye, 1.0, 0.0) - g_sub * c_lane
    gram_rest_t = gram - g_sub * g_lane
    images = jnp.where(lane2 == 0, g_sub, 0.0)
    coords = [c_sub]
    trust = jnp.ones((16, 128), jnp.float32)

    cosines, sines, inverse_radii, upper = [], [], [], []
    target = [beta[0:1]]
    for j in range(ITERS):
        w_sub = (CENTER * c_sub + up_coef * pltpu.roll(c_sub, 1, 0)
                 + down_coef * pltpu.roll(c_sub, 15, 0))
        u_lane = down(rest_t * w_sub)
        gu_lane = down(gram_rest_t * w_sub)
        h_lane = down(images * w_sub)
        u_sub, gu_sub, h_sub = turned(u_lane), turned(gu_lane), turned(h_lane)
        square = down(u_sub * gu_sub)
        spread_square = down(jnp.abs(u_sub) * lengths)
        trust = jnp.where(square > TRUST * spread_square * spread_square, trust, 0.0)
        height = jnp.sqrt(jnp.maximum(square, 0.0) + epsilon)
        inverse = 1.0 / height
        if j + 1 < ITERS:
            c_sub, g_sub = u_sub * inverse, gu_sub * inverse
            c_lane, g_lane = u_lane * inverse, gu_lane * inverse
            rest_t = rest_t - g_sub * c_lane
            gram_rest_t = gram_rest_t - g_sub * g_lane
            images = jnp.where(lane2 == j + 1, g_sub, images)
            coords.append(c_sub)
        entries = [h_sub[i:i + 1] for i in range(j + 1)] + [height[0:1]]
        for row in range(j):
            entries[row], entries[row + 1] = (
                cosines[row] * entries[row] + sines[row] * entries[row + 1],
                cosines[row] * entries[row + 1] - sines[row] * entries[row])
        radius = jnp.sqrt(entries[j] * entries[j] + entries[j + 1] * entries[j + 1])
        inverse_radius = 1.0 / radius
        cosines.append(entries[j] * inverse_radius)
        sines.append(entries[j + 1] * inverse_radius)
        inverse_radii.append(inverse_radius)
        upper.append(entries[:j])
        lead = target[j]
        target[j] = cosines[j] * lead
        target.append(-sines[j] * lead)
    weights = [None] * ITERS
    for row in range(ITERS - 1, -1, -1):
        value = target[row]
        for later in range(ITERS - 1, row, -1):
            value = value - upper[later][row] * weights[later]
        weights[row] = value * inverse_radii[row]
    coef = weights[0] * coords[0]
    for j in range(1, ITERS):
        coef = coef + weights[j] * coords[j]
    flag[0, 0] = jnp.min(trust)
    coefs = [jnp.broadcast_to(coef[k:k + 1], (8, 128)) for k in range(ITERS)]

    def combine(b, carry):
        for i in range(8):
            r = b * 8 + i
            value = coefs[0] * vecs[0, r]
            for k in range(1, ITERS):
                value = value + coefs[k] * vecs[k, r]
            tall_out[pl.ds(r, 8, stride=SHELLS), :] = value
        return carry

    lax.fori_loop(0, 8, combine, 0)
    sol = coefs[0] * planes[0, 0:8]
    sol_collector = coefs[0] * planes[0, 8:16]
    for k in range(1, ITERS):
        sol = sol + coefs[k] * planes[k, 0:8]
        sol_collector = sol_collector + coefs[k] * planes[k, 8:16]
    plane_out[0:8] = sol
    plane_out[8:16] = sol_collector

    for turn in range(len(ROUNDS)):
        each_message(turn, lambda block: halo_copy(turn, block).wait_send())
    for step in range(1, n_a):
        copy_a(step)[1].wait_send()
    for step in range(1, n_b):
        copy_b(step)[1].wait_send()


def results(tall, planes, out_c, out_p):
    for g in range(4):
        block = tall[g * 128:(g + 1) * 128, :].T
        for q in range(4):
            at = (4 * q + g) * 128
            out_c[:, :, at:at + 128] = block[q * 32:(q + 1) * 32].reshape(2, 16, 128)
    sol = planes[0:8]
    by_node = [sol if q == 0 else pltpu.roll(sol, 128 - 32 * q, 1) for q in range(4)]
    by_node = jnp.concatenate(
        by_node + [planes[8:16], jnp.zeros((88, 128), jnp.float32)], axis=0)
    out_p[...] = by_node.T[:CELLS, :CELLS + 1].reshape(2, 16, CELLS + 1)


def fast(nx, ny, *args):
    n_a, n_b = nx // 2, 2 * ny
    f32 = jnp.float32
    vmem = pl.BlockSpec(memory_space=pltpu.VMEM)
    tall, planes, flag = pl.pallas_call(
        functools.partial(kernel, nx, ny),
        out_shape=(
            pltpu.VMEM((512, 128), f32),
            pltpu.VMEM((16, 128), f32),
            jax.ShapeDtypeStruct((1, 1), f32),
        ),
        in_specs=[vmem] * 5,
        out_specs=(vmem, vmem, pl.BlockSpec(memory_space=pltpu.SMEM)),
        scratch_shapes=[
            pltpu.VMEM((512, 128), f32),
            pltpu.VMEM((DIM, SHELLS, 8, 128), f32),
            pltpu.VMEM((DIM, 16, 128), f32),
            pltpu.VMEM((len(ROUNDS), OUTBOX, 128), f32),
            pltpu.VMEM((len(ROUNDS), len(BLOCKS), OUTBOX, 128), f32),
            pltpu.VMEM((128, 128), f32),
            pltpu.VMEM((n_a, 1, 128), f32),
            pltpu.VMEM((n_b, 1, 128), f32),
            pltpu.SemaphoreType.DMA((len(ROUNDS), len(BLOCKS))),
            pltpu.SemaphoreType.DMA((len(ROUNDS), len(BLOCKS))),
            pltpu.SemaphoreType.DMA((n_a,)),
            pltpu.SemaphoreType.DMA((n_a,)),
            pltpu.SemaphoreType.DMA((n_b,)),
            pltpu.SemaphoreType.DMA((n_b,)),
        ],
        compiler_params=pltpu.CompilerParams(collective_id=0, has_side_effects=True),
    )(*args)
    conc, pots = pl.pallas_call(
        results,
        out_shape=tuple(jax.ShapeDtypeStruct(a.shape, f32) for a in args[:2]),
        in_specs=[vmem] * 2,
        out_specs=(vmem,) * 2,
    )(*(pltpu.with_memory_space_constraint(a, pltpu.VMEM) for a in (tall, planes)))
    return conc, pots, flag


def with_halo(shard, sides, width):
    edges = {}
    for axis, dim in sides:
        size, length = (lax.axis_size(axis), shard.shape[dim])
        up = [(i, (i + 1) % size) for i in range(size - 1)]
        last = lax.slice_in_dim(shard, length - width, length, axis=dim)
        initial = lax.slice_in_dim(shard, 0, width, axis=dim)
        edges[dim] = (
            lax.ppermute(last, axis, up),
            lax.ppermute(initial, axis, [(b, a) for a, b in up]),
        )
    done = []
    for _, dim in sides:
        low, high = edges[dim]
        around = [(width, width) if d in done else (0, 0) for d in range(shard.ndim)]
        shard = jnp.concatenate([jnp.pad(low, around), shard, jnp.pad(high, around)], axis=dim)
        done.append(dim)
    return shard


def total_of(shard):
    return lax.all_gather(shard, ("gx", "gy")).sum(axis=0)


def mirror_laplace(values):
    inner = jnp.concatenate([values[..., :1], values[..., :-1]], axis=-1)
    outer = jnp.concatenate([values[..., 1:], values[..., -1:]], axis=-1)
    return 2.0 * values - inner - outer


def local_operator(conc, padded, diffusion, exchange, slope):
    nodes = exchange.shape[2]
    shell_count = conc.shape[2] // nodes
    shells = conc.reshape(conc.shape[0], conc.shape[1], nodes, shell_count)
    center = padded[1:-1, 1:-1]
    lateral = (
        4.0 * center - padded[2:, 1:-1] - padded[:-2, 1:-1] - padded[1:-1, 2:] - padded[1:-1, :-2]
    )
    node_pot = center[..., :nodes]
    collector = center[..., nodes]
    current = exchange * (node_pot - collector[..., None])
    surface = shells[..., shell_count - 1]
    surface_flag = (lax.broadcasted_iota(jnp.int32, (shell_count,), 0) == shell_count - 1).astype(
        jnp.float32
    )
    new_shells = (
        shells + diffusion[..., None] * mirror_laplace(shells) + current[..., None] * surface_flag
    )
    new_nodes = (
        node_cond * mirror_laplace(node_pot)
        + current
        - slope * surface
        + plane_cond * lateral[..., :nodes]
    )
    new_collector = collector_cond * lateral[..., nodes] - jnp.mean(current, axis=-1)
    return (
        new_shells.reshape(conc.shape),
        jnp.concatenate([new_nodes, new_collector[..., None]], axis=-1),
    )


def step_by_step(rhs_conc, rhs_pots, diffusion, exchange, slope):
    first = jnp.sum(rhs_conc * rhs_conc) + jnp.sum(rhs_pots * rhs_pots)
    start_norm = jnp.sqrt(total_of(first.reshape(1))[0] + epsilon)
    all_conc = jnp.zeros((DIM, *rhs_conc.shape), jnp.float32).at[0].set(rhs_conc / start_norm)
    all_pots = jnp.zeros((DIM, *rhs_pots.shape), jnp.float32).at[0].set(rhs_pots / start_norm)
    matrix = jnp.zeros((DIM, DIM), jnp.float32)

    def arnoldi(step, state):
        all_conc, all_pots, matrix = state
        padded = with_halo(all_pots[step], (("gx", 0), ("gy", 1)), 1)
        image_conc, image_pots = local_operator(all_conc[step], padded, diffusion, exchange, slope)
        local_dots = jnp.sum(all_conc * image_conc, axis=(1, 2, 3)) + jnp.sum(
            all_pots * image_pots, axis=(1, 2, 3))
        coeffs = total_of(local_dots)
        rest_conc = image_conc - jnp.sum(coeffs[:, None, None, None] * all_conc, axis=0)
        rest_pots = image_pots - jnp.sum(coeffs[:, None, None, None] * all_pots, axis=0)
        rest = jnp.sum(rest_conc * rest_conc) + jnp.sum(rest_pots * rest_pots)
        height = jnp.sqrt(total_of(rest.reshape(1))[0] + epsilon)
        column = jnp.where(jnp.arange(DIM) == step + 1, height, coeffs)
        return (
            lax.dynamic_update_index_in_dim(all_conc, rest_conc / height, step + 1, 0),
            lax.dynamic_update_index_in_dim(all_pots, rest_pots / height, step + 1, 0),
            lax.dynamic_update_index_in_dim(matrix, column, step, 0),
        )

    all_conc, all_pots, matrix = lax.fori_loop(
        0, ITERS, arnoldi, (all_conc, all_pots, matrix))

    def rotate(step, state):
        matrix, target = state
        pair = matrix[step]
        lead, under = pair[step], pair[step + 1]
        radius = jnp.sqrt(lead * lead + under * under)
        cosine, sine = lead / radius, under / radius

        def turn(values):
            a = lax.dynamic_index_in_dim(values, step, values.ndim - 1)
            b = lax.dynamic_index_in_dim(values, step + 1, values.ndim - 1)
            values = lax.dynamic_update_slice_in_dim(
                values, cosine * a + sine * b, step, values.ndim - 1)
            return lax.dynamic_update_slice_in_dim(
                values, cosine * b - sine * a, step + 1, values.ndim - 1)

        return turn(matrix), turn(target)

    target = jnp.zeros((DIM,), jnp.float32).at[0].set(start_norm)
    matrix, target = lax.fori_loop(0, ITERS, rotate, (matrix, target))

    def back(i, weights):
        row = ITERS - 1 - i
        known = jnp.sum(matrix[:, row] * weights)
        return weights.at[row].set((target[row] - known) / matrix[row, row])

    weights = lax.fori_loop(0, ITERS, back, jnp.zeros((DIM,), jnp.float32))
    weights = weights[:, None, None, None]
    return jnp.sum(weights * all_conc, axis=0), jnp.sum(weights * all_pots, axis=0)


def solution(mesh):
    nx, ny = mesh.shape["gx"], mesh.shape["gy"]

    def shards(*args):
        conc, pots, flag = fast(nx, ny, *args)

        def again(state):
            conc, pots = step_by_step(*args)
            return conc, pots, jnp.ones_like(state[2])

        return lax.while_loop(
            lambda state: state[2] < 0.5, again, (conc, pots, flag[0, 0]))[:2]

    spec = P("gx", "gy", None)
    return jax.shard_map(
        shards, mesh=mesh, in_specs=(spec,) * 5, out_specs=(spec,) * 2, check_vma=False)
```

```python
import functools
import jax
import jax.numpy as jnp
from jax import lax
from jax.experimental import pallas as pl
from jax.experimental.pallas import tpu as pltpu
from jax.sharding import Mesh
from jax.sharding import PartitionSpec as P

ITERS = 10
MESH = pl.DeviceIdType.MESH
GX = ("gx_0", "gx_1", "gx_2")

node_cond = 1.0
plane_cond = 0.5
collector_cond = 2.0
epsilon = 1e-06

ROUNDS = (5, 5)
CENTER = 11.0
HALF = 10.0
TRUST = 1e-4

CELLS = 32
SHELLS = 64
DIM = ITERS + 1
STARTS = tuple(sum(ROUNDS[:i]) for i in range(len(ROUNDS)))


def steps_away(block):
    a, b = block
    return max(2 * abs(a) - 1, 0) + abs(b)


DEEPEST = max(ROUNDS)
BLOCKS = sorted(
    ((a, b) for a in range(-DEEPEST, DEEPEST + 1) for b in (-1, 0, 1)
     if 0 < steps_away((a, b)) <= DEEPEST),
    key=lambda block: (-steps_away(block), block))
SLOT = {block: i for i, block in enumerate(BLOCKS)}
COEFS = 24
OUTBOX = 16 + COEFS + 8 * (DEEPEST - 1)


def message_rows(turn, block):
    updates = ROUNDS[turn] - steps_away(block)
    if updates < 0:
        return 0
    if block[1]:
        return 8 * len(fields_of(turn, updates))
    if updates == 0:
        return 16
    return 16 + (COEFS if turn == 0 else 0) + 8 * updates


WIDE = 5
assert DEEPEST <= WIDE


def fields_of(turn, updates):
    names = ["pots"]
    if updates and turn == 0:
        names.append("coefs")
    if updates > 1:
        names.append("shells")
    return names


def is_first(k):
    return k in STARTS


def kernel(nx, ny, conc_in, pots_in, diff_in, exch_in, slope_in, tall_out, plane_out, flag,
           tall, vecs, planes, outbox, halo, rows, sums_a, sums_b,
           hs_sem, hr_sem, as_sem, ar_sem, bs_sem, br_sem,
           conc, pots, diff, exch, slope, in_sem):
    loads = [
        pltpu.make_async_copy(source, target, in_sem.at[i])
        for i, (source, target) in enumerate((
            (conc_in, conc), (diff_in, diff), (exch_in, exch), (slope_in, slope), (pots_in, pots)))]
    for load in loads:
        load.start()

    n_a = nx // 2
    n_b = 2 * ny
    gx = lax.axis_index("gx")
    gy = lax.axis_index("gy")
    core = lax.rem(gx, 2)
    col = lax.div(gx, 2)
    slot_a = col
    slot_b = core * ny + gy

    def peer_a(step):
        other = lax.rem(col + step, n_a)
        return other, (other * 2 + core, gy)

    def peer_b(step):
        other = lax.rem(slot_b + step, n_b)
        return other, (col * 2 + lax.div(other, ny), lax.rem(other, ny))

    exists = {}
    for a, b in BLOCKS:
        inside = []
        if a:
            inside.append(gx + a < nx if a > 0 else gx + a >= 0)
        if b:
            inside.append(gy + b < ny if b > 0 else gy + b >= 0)
        exists[a, b] = inside[0] if len(inside) == 1 else jnp.logical_and(*inside)

    barrier = pltpu.get_barrier_semaphore()
    for step in range(1, n_b):
        pl.semaphore_signal(barrier, inc=1, device_id=peer_b(step)[1], device_id_type=MESH)
    for step in range(1, n_a):
        pl.semaphore_signal(barrier, inc=1, device_id=peer_a(step)[1], device_id_type=MESH)
    expected = n_a + n_b - 2
    for block in BLOCKS:
        @pl.when(exists[block])
        def _(block=block):
            pl.semaphore_signal(
                barrier, inc=1, device_id=(gx + block[0], gy + block[1]), device_id_type=MESH)
        expected = expected + exists[block].astype(jnp.int32)

    lane = lax.broadcasted_iota(jnp.int32, (8, 128), 1)
    sub = lax.broadcasted_iota(jnp.int32, (8, 128), 0)
    quarter = lane // 32
    x_of = (lane // 16) % 2
    y_of = lane % 16
    once = jnp.logical_and(sub == 0, quarter == 0)
    zero = jnp.zeros((8, 128), jnp.float32)

    for block in BLOCKS:
        @pl.when(jnp.logical_not(exists[block]))
        def _(block=block):
            for turn in range(len(ROUNDS)):
                count = message_rows(turn, block)
                if count:
                    halo[turn, SLOT[block], 0:count] = jnp.zeros((count, 128), jnp.float32)

    def spread(by_node):
        parts = [by_node[8 * q:8 * q + 8, :] for q in range(4)]
        return jnp.concatenate(parts, axis=1)

    def small(ref):
        return spread(ref[...].reshape(CELLS, CELLS).T)

    for load in loads:
        load.wait()
    diffusion = small(diff)
    exchange = small(exch)
    slopes = small(slope)
    pots_t = pots[...].reshape(CELLS, CELLS + 1).T
    pot = spread(pots_t[:CELLS])
    collector = jnp.broadcast_to(
        jnp.concatenate([pots_t[CELLS:CELLS + 1]] * 4, axis=1), (8, 128))
    planes[0, 0:8] = pot
    planes[0, 8:16] = collector
    rows[...] = jnp.zeros((128, 128), jnp.float32)

    flat = conc[...].reshape(CELLS, 2048)
    for g in range(4):
        block = jnp.concatenate(
            [flat[:, (4 * q + g) * 128:(4 * q + g + 1) * 128] for q in range(4)], axis=0)
        tall[g * 128:(g + 1) * 128, :] = block.T

    def pack(fields, side):
        start = 16 - WIDE if side == 1 else 0
        packed = zero
        for i, field in enumerate(fields):
            shift = (WIDE * i - start) % 128
            moved = pltpu.roll(field, shift, 1) if shift else field
            packed = jnp.where(jnp.logical_and(y_of >= WIDE * i, y_of < WIDE * (i + 1)), moved, packed)
        return packed

    def unpack(packed, i, side):
        start = 16 - WIDE if side == 1 else 0
        shift = (start - WIDE * i) % 128
        return pltpu.roll(packed, shift, 1) if shift else packed

    def fill_outbox(turn, pot, collector, shells, coefs):
        for i, field in enumerate([pot, collector] + coefs + shells):
            outbox[turn, 0, 8 * i:8 * i + 8] = field
        for side in (1, -1):
            fields = [pack([pot, collector] + shells[:1], side)]
            if coefs:
                fields.append(pack(coefs, side))
            if len(shells) > 1:
                fields.append(pack(shells[1:], side))
            for i, field in enumerate(fields):
                outbox[turn, side % 3, 8 * i:8 * i + 8] = field

    fill_outbox(0, pot, collector,
                [tall[pl.ds(SHELLS - 1 - i, 8, stride=SHELLS), :] for i in range(ROUNDS[0] - 1)],
                [exchange, slopes, diffusion])

    def first(b, acc):
        for i in range(8):
            r = b * 8 + i
            shell = tall[pl.ds(r, 8, stride=SHELLS), :]
            vecs[0, r] = shell
            acc = acc + shell * shell
        return acc

    def keep(k, i, acc):
        total = jnp.sum(acc, axis=0, keepdims=True)
        rows[DIM * k + i:DIM * k + i + 1, :] = total
        if i != k:
            rows[DIM * i + k:DIM * i + k + 1, :] = total

    def halo_copy(turn, block):
        a, b = block
        count = message_rows(turn, block)
        return pltpu.make_async_remote_copy(
            src_ref=outbox.at[turn, b % 3, pl.ds(0, count)],
            dst_ref=halo.at[turn, SLOT[-a, -b], pl.ds(0, count)],
            send_sem=hs_sem.at[turn, SLOT[block]],
            recv_sem=hr_sem.at[turn, SLOT[-a, -b]],
            device_id=(gx + a, gy + b),
            device_id_type=MESH,
        )

    def each_message(turn, act):
        for block in BLOCKS:
            if message_rows(turn, block):
                @pl.when(exists[block])
                def _(block=block):
                    act(block)

    def receive(turn, block):
        a, b = block
        count = message_rows(turn, block)
        pltpu.make_async_remote_copy(
            src_ref=outbox.at[turn, b % 3, pl.ds(0, count)],
            dst_ref=halo.at[turn, SLOT[block], pl.ds(0, count)],
            send_sem=hs_sem.at[turn, SLOT[block]],
            recv_sem=hr_sem.at[turn, SLOT[block]],
            device_id=(gx + a, gy + b),
            device_id_type=MESH,
        ).wait_recv()

    def send_round(turn):
        each_message(turn, lambda block: halo_copy(turn, block).start())

    pl.semaphore_wait(barrier, expected)
    send_round(0)
    acc = lax.fori_loop(0, 8, first, zero)
    keep(0, 0, acc + pot * pot + jnp.where(once, collector * collector, 0.0))

    def around(own, low_x, high_x, low_y, high_y):
        high = own if high_x is None else own + high_x
        low = own if low_x is None else own + low_x
        before = 0.0 if low_y is None else pltpu.roll(low_y, 113, 1)
        after = 0.0 if high_y is None else pltpu.roll(high_y, 15, 1)
        return (jnp.where(x_of == 1, pltpu.roll(high, 16, 1), pltpu.roll(low, 112, 1))
                + jnp.where(y_of > 0, pltpu.roll(own, 1, 1), before)
                + jnp.where(y_of < 15, pltpu.roll(own, 127, 1), after))

    def node_mirror(v):
        down = pltpu.roll(v, 1, 0)
        down = jnp.where(sub == 0, pltpu.roll(down, 32, 1), down)
        down = jnp.where(jnp.logical_and(sub == 0, quarter == 0), v, down)
        up = pltpu.roll(v, 7, 0)
        up = jnp.where(sub == 7, pltpu.roll(up, 96, 1), up)
        up = jnp.where(jnp.logical_and(sub == 7, quarter == 3), v, up)
        return 2.0 * v - down - up

    def over_nodes(v):
        v = jnp.broadcast_to(jnp.sum(v, axis=0, keepdims=True), (8, 128))
        return (v + pltpu.roll(v, 32, 1)) + (pltpu.roll(v, 64, 1) + pltpu.roll(v, 96, 1))

    def potentials(turn):
        depth, start = ROUNDS[turn], STARTS[turn]
        carried = ROUNDS[turn + 1] - 1 if turn + 1 < len(ROUNDS) else 0
        own = (0, 0)
        now = {own: (planes[start, 0:8], planes[start, 8:16],
                     [vecs[start, SHELLS - 1 - i] for i in range(depth + carried)])}
        coefs = {own: (exchange, slopes, diffusion)}
        for block in BLOCKS:
            if message_rows(turn, block) == 0:
                continue
            updates = depth - steps_away(block)
            inbox = halo.at[turn, SLOT[block]]
            if block[1]:
                side = -block[1]
                names = fields_of(turn, updates)
                found = {name: inbox[8 * i:8 * i + 8] for i, name in enumerate(names)}
                shells = [unpack(found["pots"], 2, side)] if updates else []
                shells += [unpack(found["shells"], i, side) for i in range(updates - 1)]
                now[block] = (unpack(found["pots"], 0, side), unpack(found["pots"], 1, side), shells)
                if updates:
                    source = halo[0, SLOT[block], 8:16]
                    coefs[block] = tuple(unpack(source, i, side) for i in range(3))
                continue
            shells_at = 16 + (COEFS if turn == 0 else 0)
            now[block] = (inbox[0:8], inbox[8:16],
                          [inbox[shells_at + 8 * i:shells_at + 8 * i + 8] for i in range(updates)])
            if updates:
                source = halo.at[0, SLOT[block]]
                coefs[block] = (source[16:24], source[24:32], source[32:40])
        before = None
        for m in range(1, depth + 1):
            scale = (1.0 if m == 1 else 2.0) / HALF
            after = {}
            for block in now:
                if steps_away(block) > depth - m:
                    continue
                a, b = block
                pot, collector, shells = now[block]
                exchange_of, slope_of, diffusion_of = coefs[block]
                beside = [now.get(other) for other in (
                    (a - 1, b), (a + 1, b), (a, b - 1), (a, b + 1))]

                def lateral(which, own):
                    return 4.0 * own - around(
                        own, *(None if other is None else other[which] for other in beside))

                current = exchange_of * (pot - collector)
                new_pot = scale * (
                    node_cond * node_mirror(pot) + current - slope_of * shells[0]
                    + plane_cond * lateral(0, pot) - CENTER * pot)
                new_collector = scale * (
                    collector_cond * lateral(1, collector)
                    - over_nodes(current) * (1.0 / 32.0) - CENTER * collector)
                count = depth - m + carried if block == own_block else depth - steps_away(block) - m
                center_coef = scale * (1.0 - CENTER + 2.0 * diffusion_of)
                side_coef = scale * diffusion_of
                new_shells = []
                for i in range(count):
                    new = center_coef * shells[i] - side_coef * (shells[max(i - 1, 0)] + shells[i + 1])
                    if i == 0:
                        new = new + scale * current
                    if m > 1:
                        new = new - before[block][2][i]
                    new_shells.append(new)
                if m > 1:
                    new_pot = new_pot - before[block][0]
                    new_collector = new_collector - before[block][1]
                if block != own_block:
                    new_pot = jnp.where(exists[block], new_pot, 0.0)
                    new_collector = jnp.where(exists[block], new_collector, 0.0)
                after[block] = (new_pot, new_collector, new_shells)
            planes[start + m, 0:8] = after[own_block][0]
            planes[start + m, 8:16] = after[own_block][1]
            before, now = now, after
        if turn + 1 < len(ROUNDS):
            fill_outbox(turn + 1, *now[own_block], [])

    own_block = (0, 0)

    def bulk_shells(k):
        scale = (1.0 if is_first(k) else 2.0) / HALF
        current = exchange * (planes[k, 0:8] - planes[k, 8:16])
        center_coef = scale * (1.0 - CENTER + 2.0 * diffusion)
        side_coef = scale * diffusion

        def shells(base, accs, last):
            accs = list(accs)
            low = vecs[k, jnp.maximum(base - 1, 0)]
            here = vecs[k, base]
            for i in range(8):
                r = base + i
                high = here if last and i == 7 else vecs[k, r + 1]
                new = center_coef * here - side_coef * (low + high)
                if last and i == 7:
                    new = new + scale * current
                if not is_first(k):
                    new = new - vecs[k - 1, r]
                vecs[k + 1, r] = new
                for m in range(k):
                    accs[m] = accs[m] + new * vecs[m, r]
                accs[k] = accs[k] + new * here
                accs[k + 1] = accs[k + 1] + new * new
                low, here = here, high
            return tuple(accs)

        accs = lax.fori_loop(
            0, 7, lambda b, accs: shells(b * 8, accs, False), (zero,) * (k + 2))
        return shells(SHELLS - 8, accs, True)

    def products(k, accs):
        new_pot, new_collector = planes[k + 1, 0:8], planes[k + 1, 8:16]
        for m in range(k + 2):
            acc = accs[m] + new_pot * planes[m, 0:8] + jnp.where(
                once, new_collector * planes[m, 8:16], 0.0)
            keep(k + 1, m, acc)

    for turn, start in enumerate(STARTS):
        accs = bulk_shells(start)
        each_message(turn, functools.partial(receive, turn))
        potentials(turn)
        if turn + 1 < len(ROUNDS):
            send_round(turn + 1)
        products(start, accs)
        for k in range(start + 1, start + ROUNDS[turn]):
            products(k, bulk_shells(k))

    def total(mine, count, slot, peer, sums, s_sem, r_sem):
        sums[pl.ds(slot, 1)] = mine.reshape(1, 1, 128)

        def copy(step):
            other, device = peer(step)
            return other, pltpu.make_async_remote_copy(
                src_ref=sums.at[slot],
                dst_ref=sums.at[slot],
                send_sem=s_sem.at[step],
                recv_sem=r_sem.at[slot],
                device_id=device,
                device_id_type=MESH,
            )

        for step in range(1, count):
            copy(step)[1].start()
        for step in range(1, count):
            other = peer(step)[0]
            pltpu.make_async_remote_copy(
                src_ref=sums.at[other],
                dst_ref=sums.at[other],
                send_sem=s_sem.at[step],
                recv_sem=r_sem.at[other],
                device_id=peer(step)[1],
                device_id_type=MESH,
            ).wait_recv()
        return jnp.sum(sums[...], axis=0), copy

    mine = jnp.sum(rows[...].T, axis=0, keepdims=True)
    part, copy_a = total(mine, n_a, slot_a, peer_a, sums_a, as_sem, ar_sem)
    whole, copy_b = total(part, n_b, slot_b, peer_b, sums_b, bs_sem, br_sem)

    lane2 = lax.broadcasted_iota(jnp.int32, (16, 128), 1)
    sub2 = lax.broadcasted_iota(jnp.int32, (16, 128), 0)
    eye = sub2 == lane2
    whole = jnp.broadcast_to(whole, (16, 128))
    gram = jnp.zeros((16, 128), jnp.float32)
    for k in range(DIM):
        moved = whole if k == 0 else pltpu.roll(whole, (128 - DIM * k) % 128, 1)
        gram = jnp.where(sub2 == k, moved, gram)
    gram = jnp.where(lane2 < DIM, gram, 0.0)

    def down(v):
        return jnp.broadcast_to(jnp.sum(v, axis=0, keepdims=True), (16, 128))

    def turned(v):
        return jnp.broadcast_to(
            jnp.sum(jnp.where(eye, v, 0.0), axis=1, keepdims=True), (16, 128))

    diagonal = jnp.broadcast_to(
        jnp.sum(jnp.where(eye, gram, 0.0), axis=1, keepdims=True), (16, 128))
    lengths = jnp.sqrt(jnp.maximum(diagonal, 0.0))
    beta = jnp.sqrt(jnp.broadcast_to(diagonal[0:1], (16, 128)) + epsilon)
    inverse = 1.0 / beta
    up_coef = jnp.zeros((16, 128), jnp.float32)
    down_coef = jnp.zeros((16, 128), jnp.float32)
    for k in range(ITERS):
        up_coef = jnp.where(sub2 == k + 1, HALF if is_first(k) else HALF / 2, up_coef)
        if not is_first(k):
            down_coef = jnp.where(sub2 == k - 1, HALF / 2, down_coef)
    g_lane = jnp.broadcast_to(gram[0:1], (16, 128)) * inverse
    c_lane = jnp.where(lane2 == 0, inverse, 0.0)
    g_sub = turned(g_lane)
    c_sub = jnp.where(sub2 == 0, inverse, 0.0)
    rest_t = jnp.where(eye, 1.0, 0.0) - g_sub * c_lane
    gram_rest_t = gram - g_sub * g_lane
    images = jnp.where(lane2 == 0, g_sub, 0.0)
    coords = [c_sub]
    trust = jnp.ones((16, 128), jnp.float32)

    cosines, sines, inverse_radii, upper = [], [], [], []
    target = [beta[0:1]]
    for j in range(ITERS):
        w_sub = (CENTER * c_sub + up_coef * pltpu.roll(c_sub, 1, 0)
                 + down_coef * pltpu.roll(c_sub, 15, 0))
        u_lane = down(rest_t * w_sub)
        gu_lane = down(gram_rest_t * w_sub)
        h_lane = down(images * w_sub)
        u_sub, gu_sub, h_sub = turned(u_lane), turned(gu_lane), turned(h_lane)
        square = down(u_sub * gu_sub)
        spread_square = down(jnp.abs(u_sub) * lengths)
        trust = jnp.where(square > TRUST * spread_square * spread_square, trust, 0.0)
        height = jnp.sqrt(jnp.maximum(square, 0.0) + epsilon)
        inverse = 1.0 / height
        if j + 1 < ITERS:
            c_sub, g_sub = u_sub * inverse, gu_sub * inverse
            c_lane, g_lane = u_lane * inverse, gu_lane * inverse
            rest_t = rest_t - g_sub * c_lane
            gram_rest_t = gram_rest_t - g_sub * g_lane
            images = jnp.where(lane2 == j + 1, g_sub, images)
            coords.append(c_sub)
        entries = [h_sub[i:i + 1] for i in range(j + 1)] + [height[0:1]]
        for row in range(j):
            entries[row], entries[row + 1] = (
                cosines[row] * entries[row] + sines[row] * entries[row + 1],
                cosines[row] * entries[row + 1] - sines[row] * entries[row])
        radius = jnp.sqrt(entries[j] * entries[j] + entries[j + 1] * entries[j + 1])
        inverse_radius = 1.0 / radius
        cosines.append(entries[j] * inverse_radius)
        sines.append(entries[j + 1] * inverse_radius)
        inverse_radii.append(inverse_radius)
        upper.append(entries[:j])
        lead = target[j]
        target[j] = cosines[j] * lead
        target.append(-sines[j] * lead)
    weights = [None] * ITERS
    for row in range(ITERS - 1, -1, -1):
        value = target[row]
        for later in range(ITERS - 1, row, -1):
            value = value - upper[later][row] * weights[later]
        weights[row] = value * inverse_radii[row]
    coef = weights[0] * coords[0]
    for j in range(1, ITERS):
        coef = coef + weights[j] * coords[j]
    flag[0, 0] = jnp.min(trust)
    coefs = [jnp.broadcast_to(coef[k:k + 1], (8, 128)) for k in range(ITERS)]

    def combine(b, carry):
        for i in range(8):
            r = b * 8 + i
            value = coefs[0] * vecs[0, r]
            for k in range(1, ITERS):
                value = value + coefs[k] * vecs[k, r]
            tall_out[pl.ds(r, 8, stride=SHELLS), :] = value
        return carry

    lax.fori_loop(0, 8, combine, 0)
    sol = coefs[0] * planes[0, 0:8]
    sol_collector = coefs[0] * planes[0, 8:16]
    for k in range(1, ITERS):
        sol = sol + coefs[k] * planes[k, 0:8]
        sol_collector = sol_collector + coefs[k] * planes[k, 8:16]
    plane_out[0:8] = sol
    plane_out[8:16] = sol_collector

    for turn in range(len(ROUNDS)):
        each_message(turn, lambda block: halo_copy(turn, block).wait_send())
    for step in range(1, n_a):
        copy_a(step)[1].wait_send()
    for step in range(1, n_b):
        copy_b(step)[1].wait_send()


def results(tall, planes, out_c, out_p):
    for g in range(4):
        block = tall[g * 128:(g + 1) * 128, :].T
        for q in range(4):
            at = (4 * q + g) * 128
            out_c[:, :, at:at + 128] = block[q * 32:(q + 1) * 32].reshape(2, 16, 128)
    sol = planes[0:8]
    by_node = [sol if q == 0 else pltpu.roll(sol, 128 - 32 * q, 1) for q in range(4)]
    by_node = jnp.concatenate(
        by_node + [planes[8:16], jnp.zeros((88, 128), jnp.float32)], axis=0)
    out_p[...] = by_node.T[:CELLS, :CELLS + 1].reshape(2, 16, CELLS + 1)


def fast(nx, ny, *args):
    n_a, n_b = nx // 2, 2 * ny
    f32 = jnp.float32
    vmem = pl.BlockSpec(memory_space=pltpu.VMEM)
    tall, planes, flag = pl.pallas_call(
        functools.partial(kernel, nx, ny),
        out_shape=(
            pltpu.VMEM((512, 128), f32),
            pltpu.VMEM((16, 128), f32),
            jax.ShapeDtypeStruct((1, 1), f32),
        ),
        in_specs=[pl.BlockSpec(memory_space=pltpu.HBM)] * 5,
        out_specs=(vmem, vmem, pl.BlockSpec(memory_space=pltpu.SMEM)),
        scratch_shapes=[
            pltpu.VMEM((512, 128), f32),
            pltpu.VMEM((DIM, SHELLS, 8, 128), f32),
            pltpu.VMEM((DIM, 16, 128), f32),
            pltpu.VMEM((len(ROUNDS), 3, OUTBOX, 128), f32),
            pltpu.VMEM((len(ROUNDS), len(BLOCKS), OUTBOX, 128), f32),
            pltpu.VMEM((128, 128), f32),
            pltpu.VMEM((n_a, 1, 128), f32),
            pltpu.VMEM((n_b, 1, 128), f32),
            pltpu.SemaphoreType.DMA((len(ROUNDS), len(BLOCKS))),
            pltpu.SemaphoreType.DMA((len(ROUNDS), len(BLOCKS))),
            pltpu.SemaphoreType.DMA((n_a,)),
            pltpu.SemaphoreType.DMA((n_a,)),
            pltpu.SemaphoreType.DMA((n_b,)),
            pltpu.SemaphoreType.DMA((n_b,)),
            *(pltpu.VMEM(a.shape, f32) for a in args),
            pltpu.SemaphoreType.DMA((5,)),
        ],
        compiler_params=pltpu.CompilerParams(collective_id=0, has_side_effects=True),
    )(*args)
    conc, pots = pl.pallas_call(
        results,
        out_shape=tuple(jax.ShapeDtypeStruct(a.shape, f32) for a in args[:2]),
        in_specs=[vmem] * 2,
        out_specs=(vmem,) * 2,
    )(*(pltpu.with_memory_space_constraint(a, pltpu.VMEM) for a in (tall, planes)))
    return conc, pots, flag


def with_halo(shard, sides, width):
    edges = {}
    for axis, dim in sides:
        size, length = (lax.axis_size(axis), shard.shape[dim])
        up = [(i, (i + 1) % size) for i in range(size - 1)]
        last = lax.slice_in_dim(shard, length - width, length, axis=dim)
        initial = lax.slice_in_dim(shard, 0, width, axis=dim)
        edges[dim] = (
            lax.ppermute(last, axis, up),
            lax.ppermute(initial, axis, [(b, a) for a, b in up]),
        )
    done = []
    for _, dim in sides:
        low, high = edges[dim]
        around = [(width, width) if d in done else (0, 0) for d in range(shard.ndim)]
        shard = jnp.concatenate([jnp.pad(low, around), shard, jnp.pad(high, around)], axis=dim)
        done.append(dim)
    return shard


def total_of(shard):
    return lax.all_gather(shard, ("gx", "gy")).sum(axis=0)


def mirror_laplace(values):
    inner = jnp.concatenate([values[..., :1], values[..., :-1]], axis=-1)
    outer = jnp.concatenate([values[..., 1:], values[..., -1:]], axis=-1)
    return 2.0 * values - inner - outer


def local_operator(conc, padded, diffusion, exchange, slope):
    nodes = exchange.shape[2]
    shell_count = conc.shape[2] // nodes
    shells = conc.reshape(conc.shape[0], conc.shape[1], nodes, shell_count)
    center = padded[1:-1, 1:-1]
    lateral = (
        4.0 * center - padded[2:, 1:-1] - padded[:-2, 1:-1] - padded[1:-1, 2:] - padded[1:-1, :-2]
    )
    node_pot = center[..., :nodes]
    collector = center[..., nodes]
    current = exchange * (node_pot - collector[..., None])
    surface = shells[..., shell_count - 1]
    surface_flag = (lax.broadcasted_iota(jnp.int32, (shell_count,), 0) == shell_count - 1).astype(
        jnp.float32
    )
    new_shells = (
        shells + diffusion[..., None] * mirror_laplace(shells) + current[..., None] * surface_flag
    )
    new_nodes = (
        node_cond * mirror_laplace(node_pot)
        + current
        - slope * surface
        + plane_cond * lateral[..., :nodes]
    )
    new_collector = collector_cond * lateral[..., nodes] - jnp.mean(current, axis=-1)
    return (
        new_shells.reshape(conc.shape),
        jnp.concatenate([new_nodes, new_collector[..., None]], axis=-1),
    )


def step_by_step(rhs_conc, rhs_pots, diffusion, exchange, slope):
    first = jnp.sum(rhs_conc * rhs_conc) + jnp.sum(rhs_pots * rhs_pots)
    start_norm = jnp.sqrt(total_of(first.reshape(1))[0] + epsilon)
    all_conc = jnp.zeros((DIM, *rhs_conc.shape), jnp.float32).at[0].set(rhs_conc / start_norm)
    all_pots = jnp.zeros((DIM, *rhs_pots.shape), jnp.float32).at[0].set(rhs_pots / start_norm)
    matrix = jnp.zeros((DIM, DIM), jnp.float32)

    def arnoldi(step, state):
        all_conc, all_pots, matrix = state
        padded = with_halo(all_pots[step], (("gx", 0), ("gy", 1)), 1)
        image_conc, image_pots = local_operator(all_conc[step], padded, diffusion, exchange, slope)
        local_dots = jnp.sum(all_conc * image_conc, axis=(1, 2, 3)) + jnp.sum(
            all_pots * image_pots, axis=(1, 2, 3))
        coeffs = total_of(local_dots)
        rest_conc = image_conc - jnp.sum(coeffs[:, None, None, None] * all_conc, axis=0)
        rest_pots = image_pots - jnp.sum(coeffs[:, None, None, None] * all_pots, axis=0)
        rest = jnp.sum(rest_conc * rest_conc) + jnp.sum(rest_pots * rest_pots)
        height = jnp.sqrt(total_of(rest.reshape(1))[0] + epsilon)
        column = jnp.where(jnp.arange(DIM) == step + 1, height, coeffs)
        return (
            lax.dynamic_update_index_in_dim(all_conc, rest_conc / height, step + 1, 0),
            lax.dynamic_update_index_in_dim(all_pots, rest_pots / height, step + 1, 0),
            lax.dynamic_update_index_in_dim(matrix, column, step, 0),
        )

    all_conc, all_pots, matrix = lax.fori_loop(
        0, ITERS, arnoldi, (all_conc, all_pots, matrix))

    def rotate(step, state):
        matrix, target = state
        pair = matrix[step]
        lead, under = pair[step], pair[step + 1]
        radius = jnp.sqrt(lead * lead + under * under)
        cosine, sine = lead / radius, under / radius

        def turn(values):
            a = lax.dynamic_index_in_dim(values, step, values.ndim - 1)
            b = lax.dynamic_index_in_dim(values, step + 1, values.ndim - 1)
            values = lax.dynamic_update_slice_in_dim(
                values, cosine * a + sine * b, step, values.ndim - 1)
            return lax.dynamic_update_slice_in_dim(
                values, cosine * b - sine * a, step + 1, values.ndim - 1)

        return turn(matrix), turn(target)

    target = jnp.zeros((DIM,), jnp.float32).at[0].set(start_norm)
    matrix, target = lax.fori_loop(0, ITERS, rotate, (matrix, target))

    def back(i, weights):
        row = ITERS - 1 - i
        known = jnp.sum(matrix[:, row] * weights)
        return weights.at[row].set((target[row] - known) / matrix[row, row])

    weights = lax.fori_loop(0, ITERS, back, jnp.zeros((DIM,), jnp.float32))
    weights = weights[:, None, None, None]
    return jnp.sum(weights * all_conc, axis=0), jnp.sum(weights * all_pots, axis=0)


def solution(mesh):
    nx, ny = mesh.shape["gx"], mesh.shape["gy"]

    def shards(*args):
        conc, pots, flag = fast(nx, ny, *args)

        def again(state):
            conc, pots = step_by_step(*args)
            return conc, pots, jnp.ones_like(state[2])

        return lax.while_loop(
            lambda state: state[2] < 0.5, again, (conc, pots, flag[0, 0]))[:2]

    spec = P("gx", "gy", None)
    return jax.shard_map(
        shards, mesh=mesh, in_specs=(spec,) * 5, out_specs=(spec,) * 2, check_vma=False)
```

```python
import functools
import jax
import jax.numpy as jnp
from jax import lax
from jax.experimental import pallas as pl
from jax.experimental.pallas import tpu as pltpu
from jax.sharding import Mesh
from jax.sharding import PartitionSpec as P

ITERS = 10
MESH = pl.DeviceIdType.MESH
GX = ("gx_0", "gx_1", "gx_2")

node_cond = 1.0
plane_cond = 0.5
collector_cond = 2.0
epsilon = 1e-06

ROUNDS = (5, 5)
CENTER = 11.0
HALF = 10.0
TRUST = 1e-4

CELLS = 32
SHELLS = 64
DIM = ITERS + 1
STARTS = tuple(sum(ROUNDS[:i]) for i in range(len(ROUNDS)))


def steps_away(block):
    a, b = block
    return max(2 * abs(a) - 1, 0) + abs(b)


DEEPEST = max(ROUNDS)
BLOCKS = sorted(
    ((a, b) for a in range(-DEEPEST, DEEPEST + 1) for b in (-1, 0, 1)
     if 0 < steps_away((a, b)) <= DEEPEST),
    key=lambda block: (-steps_away(block), block))
SLOT = {block: i for i, block in enumerate(BLOCKS)}
COEFS = 24
OUTBOX = 16 + COEFS + 8 * (DEEPEST - 1)


def message_rows(turn, block):
    updates = ROUNDS[turn] - steps_away(block)
    if updates < 0:
        return 0
    if block[1]:
        return 8 * len(fields_of(turn, updates))
    if updates == 0:
        return 16
    return 16 + (COEFS if turn == 0 else 0) + 8 * updates


WIDE = 5
assert DEEPEST <= WIDE


def fields_of(turn, updates):
    names = ["pots"]
    if updates and turn == 0:
        names.append("coefs")
    if updates > 1:
        names.append("shells")
    return names


STAGES = (("core",), ("z",), ("x", "y"))


def extents(nx, ny):
    columns = min(4, nx // 2)
    return {"x": nx // 2 // columns, "y": columns, "core": 2, "z": ny}


def members(names, nx, ny):
    count = 1
    for name in names:
        count *= extents(nx, ny)[name]
    return count


class Group:
    def __init__(self, names, nx, ny, gx, gy):
        self.names, self.extents = names, extents(nx, ny)
        columns = self.extents["y"]
        self.place = {"core": lax.rem(gx, 2), "y": lax.rem(lax.div(gx, 2), columns),
                      "x": lax.div(gx, 2 * columns), "z": gy}
        self.count = members(names, nx, ny)
        self.slot = 0
        for name in names:
            self.slot = self.slot * self.extents[name] + self.place[name]

    def peer(self, step):
        other = lax.rem(self.slot + step, self.count)
        place, left = dict(self.place), other
        for name in reversed(self.names):
            place[name] = lax.rem(left, self.extents[name])
            left = lax.div(left, self.extents[name])
        row = (place["x"] * self.extents["y"] + place["y"]) * 2 + place["core"]
        return other, (row, place["z"])


def is_first(k):
    return k in STARTS


def kernel(nx, ny, conc_in, pots_in, diff_in, exch_in, slope_in, tall_out, plane_out, flag,
           tall, vecs, planes, outbox, halo, rows, conc, pots, diff, exch, slope, hs_sem, hr_sem, in_sem,
           *for_sums):
    sums, sum_sems = for_sums[:len(STAGES)], for_sums[len(STAGES):]
    loads = [
        pltpu.make_async_copy(source, target, in_sem.at[i])
        for i, (source, target) in enumerate((
            (conc_in, conc), (diff_in, diff), (exch_in, exch), (slope_in, slope), (pots_in, pots)))]
    for load in loads:
        load.start()

    gx = lax.axis_index("gx")
    gy = lax.axis_index("gy")
    groups = [Group(names, nx, ny, gx, gy) for names in STAGES]

    exists = {}
    for a, b in BLOCKS:
        inside = []
        if a:
            inside.append(gx + a < nx if a > 0 else gx + a >= 0)
        if b:
            inside.append(gy + b < ny if b > 0 else gy + b >= 0)
        exists[a, b] = inside[0] if len(inside) == 1 else jnp.logical_and(*inside)

    barrier = pltpu.get_barrier_semaphore()
    expected = 0
    for group in groups:
        for step in range(1, group.count):
            pl.semaphore_signal(
                barrier, inc=1, device_id=group.peer(step)[1], device_id_type=MESH)
        expected = expected + group.count - 1
    for block in BLOCKS:
        @pl.when(exists[block])
        def _(block=block):
            pl.semaphore_signal(
                barrier, inc=1, device_id=(gx + block[0], gy + block[1]), device_id_type=MESH)
        expected = expected + exists[block].astype(jnp.int32)

    lane = lax.broadcasted_iota(jnp.int32, (8, 128), 1)
    sub = lax.broadcasted_iota(jnp.int32, (8, 128), 0)
    quarter = lane // 32
    x_of = (lane // 16) % 2
    y_of = lane % 16
    once = jnp.logical_and(sub == 0, quarter == 0)
    zero = jnp.zeros((8, 128), jnp.float32)

    for block in BLOCKS:
        @pl.when(jnp.logical_not(exists[block]))
        def _(block=block):
            for turn in range(len(ROUNDS)):
                count = message_rows(turn, block)
                if count:
                    halo[turn, SLOT[block], 0:count] = jnp.zeros((count, 128), jnp.float32)

    def spread(by_node):
        parts = [by_node[8 * q:8 * q + 8, :] for q in range(4)]
        return jnp.concatenate(parts, axis=1)

    def small(ref):
        return spread(ref[...].reshape(CELLS, CELLS).T)

    for load in loads:
        load.wait()
    diffusion = small(diff)
    exchange = small(exch)
    slopes = small(slope)
    pots_t = pots[...].reshape(CELLS, CELLS + 1).T
    pot = spread(pots_t[:CELLS])
    collector = jnp.broadcast_to(
        jnp.concatenate([pots_t[CELLS:CELLS + 1]] * 4, axis=1), (8, 128))
    planes[0, 0:8] = pot
    planes[0, 8:16] = collector
    rows[...] = jnp.zeros((128, 128), jnp.float32)

    flat = conc[...].reshape(CELLS, 2048)
    for g in range(4):
        block = jnp.concatenate(
            [flat[:, (4 * q + g) * 128:(4 * q + g + 1) * 128] for q in range(4)], axis=0)
        tall[g * 128:(g + 1) * 128, :] = block.T

    def pack(fields, side):
        start = 16 - WIDE if side == 1 else 0
        packed = zero
        for i, field in enumerate(fields):
            shift = (WIDE * i - start) % 128
            moved = pltpu.roll(field, shift, 1) if shift else field
            packed = jnp.where(jnp.logical_and(y_of >= WIDE * i, y_of < WIDE * (i + 1)), moved, packed)
        return packed

    def unpack(packed, i, side):
        start = 16 - WIDE if side == 1 else 0
        shift = (start - WIDE * i) % 128
        return pltpu.roll(packed, shift, 1) if shift else packed

    def fill_outbox(turn, pot, collector, shells, coefs):
        for i, field in enumerate([pot, collector] + coefs + shells):
            outbox[turn, 0, 8 * i:8 * i + 8] = field
        for side in (1, -1):
            fields = [pack([pot, collector] + shells[:1], side)]
            if coefs:
                fields.append(pack(coefs, side))
            if len(shells) > 1:
                fields.append(pack(shells[1:], side))
            for i, field in enumerate(fields):
                outbox[turn, side % 3, 8 * i:8 * i + 8] = field

    fill_outbox(0, pot, collector,
                [tall[pl.ds(SHELLS - 1 - i, 8, stride=SHELLS), :] for i in range(ROUNDS[0] - 1)],
                [exchange, slopes, diffusion])

    def first(b, acc):
        for i in range(8):
            r = b * 8 + i
            shell = tall[pl.ds(r, 8, stride=SHELLS), :]
            vecs[0, r] = shell
            acc = acc + shell * shell
        return acc

    def keep(k, i, acc):
        total = jnp.sum(acc, axis=0, keepdims=True)
        rows[DIM * k + i:DIM * k + i + 1, :] = total
        if i != k:
            rows[DIM * i + k:DIM * i + k + 1, :] = total

    def halo_copy(turn, block):
        a, b = block
        count = message_rows(turn, block)
        return pltpu.make_async_remote_copy(
            src_ref=outbox.at[turn, b % 3, pl.ds(0, count)],
            dst_ref=halo.at[turn, SLOT[-a, -b], pl.ds(0, count)],
            send_sem=hs_sem.at[turn, SLOT[block]],
            recv_sem=hr_sem.at[turn, SLOT[-a, -b]],
            device_id=(gx + a, gy + b),
            device_id_type=MESH,
        )

    def each_message(turn, act):
        for block in BLOCKS:
            if message_rows(turn, block):
                @pl.when(exists[block])
                def _(block=block):
                    act(block)

    def receive(turn, block):
        a, b = block
        count = message_rows(turn, block)
        pltpu.make_async_remote_copy(
            src_ref=outbox.at[turn, b % 3, pl.ds(0, count)],
            dst_ref=halo.at[turn, SLOT[block], pl.ds(0, count)],
            send_sem=hs_sem.at[turn, SLOT[block]],
            recv_sem=hr_sem.at[turn, SLOT[block]],
            device_id=(gx + a, gy + b),
            device_id_type=MESH,
        ).wait_recv()

    def send_round(turn):
        each_message(turn, lambda block: halo_copy(turn, block).start())

    pl.semaphore_wait(barrier, expected)
    send_round(0)
    acc = lax.fori_loop(0, 8, first, zero)
    keep(0, 0, acc + pot * pot + jnp.where(once, collector * collector, 0.0))

    def around(own, low_x, high_x, low_y, high_y):
        high = own if high_x is None else own + high_x
        low = own if low_x is None else own + low_x
        before = 0.0 if low_y is None else pltpu.roll(low_y, 113, 1)
        after = 0.0 if high_y is None else pltpu.roll(high_y, 15, 1)
        return (jnp.where(x_of == 1, pltpu.roll(high, 16, 1), pltpu.roll(low, 112, 1))
                + jnp.where(y_of > 0, pltpu.roll(own, 1, 1), before)
                + jnp.where(y_of < 15, pltpu.roll(own, 127, 1), after))

    def node_mirror(v):
        down = pltpu.roll(v, 1, 0)
        down = jnp.where(sub == 0, pltpu.roll(down, 32, 1), down)
        down = jnp.where(jnp.logical_and(sub == 0, quarter == 0), v, down)
        up = pltpu.roll(v, 7, 0)
        up = jnp.where(sub == 7, pltpu.roll(up, 96, 1), up)
        up = jnp.where(jnp.logical_and(sub == 7, quarter == 3), v, up)
        return 2.0 * v - down - up

    def over_nodes(v):
        v = jnp.broadcast_to(jnp.sum(v, axis=0, keepdims=True), (8, 128))
        return (v + pltpu.roll(v, 32, 1)) + (pltpu.roll(v, 64, 1) + pltpu.roll(v, 96, 1))

    def potentials(turn, beside_step):
        depth, start = ROUNDS[turn], STARTS[turn]
        carried = ROUNDS[turn + 1] - 1 if turn + 1 < len(ROUNDS) else 0
        own = (0, 0)
        now = {own: (planes[start, 0:8], planes[start, 8:16],
                     [vecs[start, SHELLS - 1 - i] for i in range(depth + carried)])}
        coefs = {own: (exchange, slopes, diffusion)}
        for block in BLOCKS:
            if message_rows(turn, block) == 0:
                continue
            updates = depth - steps_away(block)
            inbox = halo.at[turn, SLOT[block]]
            if block[1]:
                side = -block[1]
                names = fields_of(turn, updates)
                found = {name: inbox[8 * i:8 * i + 8] for i, name in enumerate(names)}
                shells = [unpack(found["pots"], 2, side)] if updates else []
                shells += [unpack(found["shells"], i, side) for i in range(updates - 1)]
                now[block] = (unpack(found["pots"], 0, side), unpack(found["pots"], 1, side), shells)
                if updates:
                    source = halo[0, SLOT[block], 8:16]
                    coefs[block] = tuple(unpack(source, i, side) for i in range(3))
                continue
            shells_at = 16 + (COEFS if turn == 0 else 0)
            now[block] = (inbox[0:8], inbox[8:16],
                          [inbox[shells_at + 8 * i:shells_at + 8 * i + 8] for i in range(updates)])
            if updates:
                source = halo.at[0, SLOT[block]]
                coefs[block] = (source[16:24], source[24:32], source[32:40])
        before = None
        for m in range(1, depth + 1):
            scale = (1.0 if m == 1 else 2.0) / HALF
            after = {}
            for block in now:
                if steps_away(block) > depth - m:
                    continue
                a, b = block
                pot, collector, shells = now[block]
                exchange_of, slope_of, diffusion_of = coefs[block]
                beside = [now.get(other) for other in (
                    (a - 1, b), (a + 1, b), (a, b - 1), (a, b + 1))]

                def lateral(which, own):
                    return 4.0 * own - around(
                        own, *(None if other is None else other[which] for other in beside))

                current = exchange_of * (pot - collector)
                new_pot = scale * (
                    node_cond * node_mirror(pot) + current - slope_of * shells[0]
                    + plane_cond * lateral(0, pot) - CENTER * pot)
                new_collector = scale * (
                    collector_cond * lateral(1, collector)
                    - over_nodes(current) * (1.0 / 32.0) - CENTER * collector)
                count = depth - m + carried if block == own_block else depth - steps_away(block) - m
                center_coef = scale * (1.0 - CENTER + 2.0 * diffusion_of)
                side_coef = scale * diffusion_of
                new_shells = []
                for i in range(count):
                    new = center_coef * shells[i] - side_coef * (shells[max(i - 1, 0)] + shells[i + 1])
                    if i == 0:
                        new = new + scale * current
                    if m > 1:
                        new = new - before[block][2][i]
                    new_shells.append(new)
                if m > 1:
                    new_pot = new_pot - before[block][0]
                    new_collector = new_collector - before[block][1]
                if block != own_block:
                    new_pot = jnp.where(exists[block], new_pot, 0.0)
                    new_collector = jnp.where(exists[block], new_collector, 0.0)
                after[block] = (new_pot, new_collector, new_shells)
            planes[start + m, 0:8] = after[own_block][0]
            planes[start + m, 8:16] = after[own_block][1]
            before, now = now, after
            beside_step(start + m)
        if turn + 1 < len(ROUNDS):
            fill_outbox(turn + 1, *now[own_block], [])

    own_block = (0, 0)

    def bulk_shells(k, unrolled=False):
        scale = (1.0 if is_first(k) else 2.0) / HALF
        current = exchange * (planes[k, 0:8] - planes[k, 8:16])
        center_coef = scale * (1.0 - CENTER + 2.0 * diffusion)
        side_coef = scale * diffusion

        def shells(base, accs, last):
            accs = list(accs)
            low = vecs[k, max(base - 1, 0) if isinstance(base, int) else jnp.maximum(base - 1, 0)]
            here = vecs[k, base]
            for i in range(8):
                r = base + i
                high = here if last and i == 7 else vecs[k, r + 1]
                new = center_coef * here - side_coef * (low + high)
                if last and i == 7:
                    new = new + scale * current
                if not is_first(k):
                    new = new - vecs[k - 1, r]
                vecs[k + 1, r] = new
                for m in range(k):
                    accs[m] = accs[m] + new * vecs[m, r]
                accs[k] = accs[k] + new * here
                accs[k + 1] = accs[k + 1] + new * new
                low, here = here, high
            return tuple(accs)

        accs = (zero,) * (k + 2)
        if unrolled:
            for b in range(7):
                accs = shells(b * 8, accs, False)
        else:
            accs = lax.fori_loop(0, 7, lambda b, accs: shells(b * 8, accs, False), accs)
        return shells(SHELLS - 8, accs, True)

    def products(k, accs):
        new_pot, new_collector = planes[k + 1, 0:8], planes[k + 1, 8:16]
        for m in range(k + 2):
            acc = accs[m] + new_pot * planes[m, 0:8] + jnp.where(
                once, new_collector * planes[m, 8:16], 0.0)
            keep(k + 1, m, acc)

    for turn, start in enumerate(STARTS):
        end = start + ROUNDS[turn]
        accs = {start: bulk_shells(start)}
        each_message(turn, functools.partial(receive, turn))
        if turn + 1 < len(ROUNDS):
            potentials(turn, lambda k: None)
            send_round(turn + 1)
            for k in range(start + 1, end):
                accs[k] = bulk_shells(k)
        else:
            def beside(k):
                if k < end:
                    accs[k] = bulk_shells(k, True)

            potentials(turn, beside)
        for k in range(start, end):
            products(k, accs[k])

    def copy(stage, slot, step):
        group = groups[stage]
        return pltpu.make_async_remote_copy(
            src_ref=sums[stage].at[slot],
            dst_ref=sums[stage].at[slot],
            send_sem=sum_sems[2 * stage].at[step],
            recv_sem=sum_sems[2 * stage + 1].at[slot],
            device_id=group.peer(step)[1],
            device_id_type=MESH,
        )

    whole = jnp.sum(rows[...].T, axis=0, keepdims=True)
    for stage, group in enumerate(groups):
        sums[stage][pl.ds(group.slot, 1)] = whole.reshape(1, 1, 128)
        for step in range(1, group.count):
            copy(stage, group.slot, step).start()
        for step in range(1, group.count):
            copy(stage, group.peer(step)[0], step).wait_recv()
        whole = jnp.sum(sums[stage][...], axis=0)

    lane2 = lax.broadcasted_iota(jnp.int32, (16, 128), 1)
    sub2 = lax.broadcasted_iota(jnp.int32, (16, 128), 0)
    eye = sub2 == lane2
    whole = jnp.broadcast_to(whole, (16, 128))
    gram = jnp.zeros((16, 128), jnp.float32)
    for k in range(DIM):
        moved = whole if k == 0 else pltpu.roll(whole, (128 - DIM * k) % 128, 1)
        gram = jnp.where(sub2 == k, moved, gram)
    gram = jnp.where(lane2 < DIM, gram, 0.0)

    def down(v):
        return jnp.broadcast_to(jnp.sum(v, axis=0, keepdims=True), (16, 128))

    def turned(v):
        return jnp.broadcast_to(
            jnp.sum(jnp.where(eye, v, 0.0), axis=1, keepdims=True), (16, 128))

    diagonal = jnp.broadcast_to(
        jnp.sum(jnp.where(eye, gram, 0.0), axis=1, keepdims=True), (16, 128))
    lengths = jnp.sqrt(jnp.maximum(diagonal, 0.0))
    beta = jnp.sqrt(jnp.broadcast_to(diagonal[0:1], (16, 128)) + epsilon)
    inverse = 1.0 / beta
    up_coef = jnp.zeros((16, 128), jnp.float32)
    down_coef = jnp.zeros((16, 128), jnp.float32)
    for k in range(ITERS):
        up_coef = jnp.where(sub2 == k + 1, HALF if is_first(k) else HALF / 2, up_coef)
        if not is_first(k):
            down_coef = jnp.where(sub2 == k - 1, HALF / 2, down_coef)
    g_lane = jnp.broadcast_to(gram[0:1], (16, 128)) * inverse
    c_lane = jnp.where(lane2 == 0, inverse, 0.0)
    g_sub = turned(g_lane)
    c_sub = jnp.where(sub2 == 0, inverse, 0.0)
    rest_t = jnp.where(eye, 1.0, 0.0) - g_sub * c_lane
    gram_rest_t = gram - g_sub * g_lane
    images = jnp.where(lane2 == 0, g_sub, 0.0)
    coords = [c_sub]
    trust = jnp.ones((16, 128), jnp.float32)

    cosines, sines, inverse_radii, upper = [], [], [], []
    target = [beta[0:1]]
    for j in range(ITERS):
        w_sub = (CENTER * c_sub + up_coef * pltpu.roll(c_sub, 1, 0)
                 + down_coef * pltpu.roll(c_sub, 15, 0))
        u_lane = down(rest_t * w_sub)
        gu_lane = down(gram_rest_t * w_sub)
        h_lane = down(images * w_sub)
        u_sub, gu_sub, h_sub = turned(u_lane), turned(gu_lane), turned(h_lane)
        square = down(u_sub * gu_sub)
        spread_square = down(jnp.abs(u_sub) * lengths)
        trust = jnp.where(square > TRUST * spread_square * spread_square, trust, 0.0)
        height = jnp.sqrt(jnp.maximum(square, 0.0) + epsilon)
        inverse = 1.0 / height
        if j + 1 < ITERS:
            c_sub, g_sub = u_sub * inverse, gu_sub * inverse
            c_lane, g_lane = u_lane * inverse, gu_lane * inverse
            rest_t = rest_t - g_sub * c_lane
            gram_rest_t = gram_rest_t - g_sub * g_lane
            images = jnp.where(lane2 == j + 1, g_sub, images)
            coords.append(c_sub)
        entries = [h_sub[i:i + 1] for i in range(j + 1)] + [height[0:1]]
        for row in range(j):
            entries[row], entries[row + 1] = (
                cosines[row] * entries[row] + sines[row] * entries[row + 1],
                cosines[row] * entries[row + 1] - sines[row] * entries[row])
        radius = jnp.sqrt(entries[j] * entries[j] + entries[j + 1] * entries[j + 1])
        inverse_radius = 1.0 / radius
        cosines.append(entries[j] * inverse_radius)
        sines.append(entries[j + 1] * inverse_radius)
        inverse_radii.append(inverse_radius)
        upper.append(entries[:j])
        lead = target[j]
        target[j] = cosines[j] * lead
        target.append(-sines[j] * lead)
    weights = [None] * ITERS
    for row in range(ITERS - 1, -1, -1):
        value = target[row]
        for later in range(ITERS - 1, row, -1):
            value = value - upper[later][row] * weights[later]
        weights[row] = value * inverse_radii[row]
    coef = weights[0] * coords[0]
    for j in range(1, ITERS):
        coef = coef + weights[j] * coords[j]
    flag[0, 0] = jnp.min(trust)
    coefs = [jnp.broadcast_to(coef[k:k + 1], (8, 128)) for k in range(ITERS)]

    def combine(b, carry):
        for i in range(8):
            r = b * 8 + i
            value = coefs[0] * vecs[0, r]
            for k in range(1, ITERS):
                value = value + coefs[k] * vecs[k, r]
            tall_out[pl.ds(r, 8, stride=SHELLS), :] = value
        return carry

    lax.fori_loop(0, 8, combine, 0)
    sol = coefs[0] * planes[0, 0:8]
    sol_collector = coefs[0] * planes[0, 8:16]
    for k in range(1, ITERS):
        sol = sol + coefs[k] * planes[k, 0:8]
        sol_collector = sol_collector + coefs[k] * planes[k, 8:16]
    plane_out[0:8] = sol
    plane_out[8:16] = sol_collector

    for turn in range(len(ROUNDS)):
        each_message(turn, lambda block: halo_copy(turn, block).wait_send())
    for stage, group in enumerate(groups):
        for step in range(1, group.count):
            copy(stage, group.slot, step).wait_send()


def results(tall, planes, out_c, out_p):
    for g in range(4):
        block = tall[g * 128:(g + 1) * 128, :].T
        for q in range(4):
            at = (4 * q + g) * 128
            out_c[:, :, at:at + 128] = block[q * 32:(q + 1) * 32].reshape(2, 16, 128)
    sol = planes[0:8]
    by_node = [sol if q == 0 else pltpu.roll(sol, 128 - 32 * q, 1) for q in range(4)]
    by_node = jnp.concatenate(
        by_node + [planes[8:16], jnp.zeros((88, 128), jnp.float32)], axis=0)
    out_p[...] = by_node.T[:CELLS, :CELLS + 1].reshape(2, 16, CELLS + 1)


def fast(nx, ny, *args):
    counts = [members(names, nx, ny) for names in STAGES]
    f32 = jnp.float32
    vmem = pl.BlockSpec(memory_space=pltpu.VMEM)
    tall, planes, flag = pl.pallas_call(
        functools.partial(kernel, nx, ny),
        out_shape=(
            pltpu.VMEM((512, 128), f32),
            pltpu.VMEM((16, 128), f32),
            jax.ShapeDtypeStruct((1, 1), f32),
        ),
        in_specs=[pl.BlockSpec(memory_space=pltpu.HBM)] * 5,
        out_specs=(vmem, vmem, pl.BlockSpec(memory_space=pltpu.SMEM)),
        scratch_shapes=[
            pltpu.VMEM((512, 128), f32),
            pltpu.VMEM((DIM, SHELLS, 8, 128), f32),
            pltpu.VMEM((DIM, 16, 128), f32),
            pltpu.VMEM((len(ROUNDS), 3, OUTBOX, 128), f32),
            pltpu.VMEM((len(ROUNDS), len(BLOCKS), OUTBOX, 128), f32),
            pltpu.VMEM((128, 128), f32),
            *(pltpu.VMEM(a.shape, f32) for a in args),
            pltpu.SemaphoreType.DMA((len(ROUNDS), len(BLOCKS))),
            pltpu.SemaphoreType.DMA((len(ROUNDS), len(BLOCKS))),
            pltpu.SemaphoreType.DMA((5,)),
            *(pltpu.VMEM((count, 1, 128), f32) for count in counts),
            *(pltpu.SemaphoreType.DMA((count,)) for count in counts for _ in range(2)),
        ],
        compiler_params=pltpu.CompilerParams(collective_id=0, has_side_effects=True),
    )(*args)
    conc, pots = pl.pallas_call(
        results,
        out_shape=tuple(jax.ShapeDtypeStruct(a.shape, f32) for a in args[:2]),
        in_specs=[vmem] * 2,
        out_specs=(vmem,) * 2,
    )(*(pltpu.with_memory_space_constraint(a, pltpu.VMEM) for a in (tall, planes)))
    return conc, pots, flag


def with_halo(shard, sides, width):
    edges = {}
    for axis, dim in sides:
        size, length = (lax.axis_size(axis), shard.shape[dim])
        up = [(i, (i + 1) % size) for i in range(size - 1)]
        last = lax.slice_in_dim(shard, length - width, length, axis=dim)
        initial = lax.slice_in_dim(shard, 0, width, axis=dim)
        edges[dim] = (
            lax.ppermute(last, axis, up),
            lax.ppermute(initial, axis, [(b, a) for a, b in up]),
        )
    done = []
    for _, dim in sides:
        low, high = edges[dim]
        around = [(width, width) if d in done else (0, 0) for d in range(shard.ndim)]
        shard = jnp.concatenate([jnp.pad(low, around), shard, jnp.pad(high, around)], axis=dim)
        done.append(dim)
    return shard


def total_of(shard):
    return lax.all_gather(shard, ("gx", "gy")).sum(axis=0)


def mirror_laplace(values):
    inner = jnp.concatenate([values[..., :1], values[..., :-1]], axis=-1)
    outer = jnp.concatenate([values[..., 1:], values[..., -1:]], axis=-1)
    return 2.0 * values - inner - outer


def local_operator(conc, padded, diffusion, exchange, slope):
    nodes = exchange.shape[2]
    shell_count = conc.shape[2] // nodes
    shells = conc.reshape(conc.shape[0], conc.shape[1], nodes, shell_count)
    center = padded[1:-1, 1:-1]
    lateral = (
        4.0 * center - padded[2:, 1:-1] - padded[:-2, 1:-1] - padded[1:-1, 2:] - padded[1:-1, :-2]
    )
    node_pot = center[..., :nodes]
    collector = center[..., nodes]
    current = exchange * (node_pot - collector[..., None])
    surface = shells[..., shell_count - 1]
    surface_flag = (lax.broadcasted_iota(jnp.int32, (shell_count,), 0) == shell_count - 1).astype(
        jnp.float32
    )
    new_shells = (
        shells + diffusion[..., None] * mirror_laplace(shells) + current[..., None] * surface_flag
    )
    new_nodes = (
        node_cond * mirror_laplace(node_pot)
        + current
        - slope * surface
        + plane_cond * lateral[..., :nodes]
    )
    new_collector = collector_cond * lateral[..., nodes] - jnp.mean(current, axis=-1)
    return (
        new_shells.reshape(conc.shape),
        jnp.concatenate([new_nodes, new_collector[..., None]], axis=-1),
    )


def step_by_step(rhs_conc, rhs_pots, diffusion, exchange, slope):
    first = jnp.sum(rhs_conc * rhs_conc) + jnp.sum(rhs_pots * rhs_pots)
    start_norm = jnp.sqrt(total_of(first.reshape(1))[0] + epsilon)
    all_conc = jnp.zeros((DIM, *rhs_conc.shape), jnp.float32).at[0].set(rhs_conc / start_norm)
    all_pots = jnp.zeros((DIM, *rhs_pots.shape), jnp.float32).at[0].set(rhs_pots / start_norm)
    matrix = jnp.zeros((DIM, DIM), jnp.float32)

    def arnoldi(step, state):
        all_conc, all_pots, matrix = state
        padded = with_halo(all_pots[step], (("gx", 0), ("gy", 1)), 1)
        image_conc, image_pots = local_operator(all_conc[step], padded, diffusion, exchange, slope)
        local_dots = jnp.sum(all_conc * image_conc, axis=(1, 2, 3)) + jnp.sum(
            all_pots * image_pots, axis=(1, 2, 3))
        coeffs = total_of(local_dots)
        rest_conc = image_conc - jnp.sum(coeffs[:, None, None, None] * all_conc, axis=0)
        rest_pots = image_pots - jnp.sum(coeffs[:, None, None, None] * all_pots, axis=0)
        rest = jnp.sum(rest_conc * rest_conc) + jnp.sum(rest_pots * rest_pots)
        height = jnp.sqrt(total_of(rest.reshape(1))[0] + epsilon)
        column = jnp.where(jnp.arange(DIM) == step + 1, height, coeffs)
        return (
            lax.dynamic_update_index_in_dim(all_conc, rest_conc / height, step + 1, 0),
            lax.dynamic_update_index_in_dim(all_pots, rest_pots / height, step + 1, 0),
            lax.dynamic_update_index_in_dim(matrix, column, step, 0),
        )

    all_conc, all_pots, matrix = lax.fori_loop(
        0, ITERS, arnoldi, (all_conc, all_pots, matrix))

    def rotate(step, state):
        matrix, target = state
        pair = matrix[step]
        lead, under = pair[step], pair[step + 1]
        radius = jnp.sqrt(lead * lead + under * under)
        cosine, sine = lead / radius, under / radius

        def turn(values):
            a = lax.dynamic_index_in_dim(values, step, values.ndim - 1)
            b = lax.dynamic_index_in_dim(values, step + 1, values.ndim - 1)
            values = lax.dynamic_update_slice_in_dim(
                values, cosine * a + sine * b, step, values.ndim - 1)
            return lax.dynamic_update_slice_in_dim(
                values, cosine * b - sine * a, step + 1, values.ndim - 1)

        return turn(matrix), turn(target)

    target = jnp.zeros((DIM,), jnp.float32).at[0].set(start_norm)
    matrix, target = lax.fori_loop(0, ITERS, rotate, (matrix, target))

    def back(i, weights):
        row = ITERS - 1 - i
        known = jnp.sum(matrix[:, row] * weights)
        return weights.at[row].set((target[row] - known) / matrix[row, row])

    weights = lax.fori_loop(0, ITERS, back, jnp.zeros((DIM,), jnp.float32))
    weights = weights[:, None, None, None]
    return jnp.sum(weights * all_conc, axis=0), jnp.sum(weights * all_pots, axis=0)


def solution(mesh):
    nx, ny = mesh.shape["gx"], mesh.shape["gy"]

    def shards(*args):
        conc, pots, flag = fast(nx, ny, *args)

        def again(state):
            conc, pots = step_by_step(*args)
            return conc, pots, jnp.ones_like(state[2])

        return lax.while_loop(
            lambda state: state[2] < 0.5, again, (conc, pots, flag[0, 0]))[:2]

    spec = P("gx", "gy", None)
    return jax.shard_map(
        shards, mesh=mesh, in_specs=(spec,) * 5, out_specs=(spec,) * 2, check_vma=False)
```

```python
import functools
import jax
import jax.numpy as jnp
from jax import lax
from jax.experimental import pallas as pl
from jax.experimental.pallas import tpu as pltpu
from jax.sharding import Mesh
from jax.sharding import PartitionSpec as P

ITERS = 10
MESH = pl.DeviceIdType.MESH
GX = ("gx_0", "gx_1", "gx_2")

node_cond = 1.0
plane_cond = 0.5
collector_cond = 2.0
epsilon = 1e-06

ROUNDS = (5, 5)
CENTER = 11.0
HALF = 10.0
TRUST = 1e-4

CELLS = 32
SHELLS = 64
DIM = ITERS + 1
STARTS = tuple(sum(ROUNDS[:i]) for i in range(len(ROUNDS)))


def steps_away(block):
    a, b = block
    return max(2 * abs(a) - 1, 0) + abs(b)


DEEPEST = max(ROUNDS)
BLOCKS = sorted(
    ((a, b) for a in range(-DEEPEST, DEEPEST + 1) for b in (-1, 0, 1)
     if 0 < steps_away((a, b)) <= DEEPEST),
    key=lambda block: (-steps_away(block), block))
SLOT = {block: i for i, block in enumerate(BLOCKS)}
COEFS = 24
OUTBOX = 16 + COEFS + 8 * (DEEPEST - 1)


def message_rows(turn, block):
    updates = ROUNDS[turn] - steps_away(block)
    if updates < 0:
        return 0
    if block[1]:
        return 8 * len(fields_of(turn, updates))
    if updates == 0:
        return 16
    return 16 + (COEFS if turn == 0 else 0) + 8 * updates


MIDDLE = 3
assert max(abs(a) for a, _ in BLOCKS) <= MIDDLE
WIDE = 5
assert DEEPEST <= WIDE


def fields_of(turn, updates):
    names = ["pots"]
    if updates and turn == 0:
        names.append("coefs")
    if updates > 1:
        names.append("shells")
    return names


STAGES = ("core", "z", "plane")


def members(name, nx, ny):
    return {"core": 2, "z": ny, "plane": nx // 2}[name]


class Group:
    def __init__(self, name, nx, ny, gx, gy):
        self.name, self.gx, self.gy = name, gx, gy
        self.core, self.plane = lax.rem(gx, 2), lax.div(gx, 2)
        self.count = members(name, nx, ny)
        self.slot = {"core": self.core, "z": gy, "plane": self.plane}[name]

    def peer(self, step):
        if self.count == 2:
            other = 1 - self.slot
        else:
            other = self.slot + step
            other = jnp.where(other >= self.count, other - self.count, other)
        if self.name == "core":
            return 2 * self.plane + other, self.gy
        if self.name == "z":
            return self.gx, other
        return 2 * other + self.core, self.gy


def is_first(k):
    return k in STARTS


def kernel(nx, ny, conc_in, pots_in, diff_in, exch_in, slope_in, tall_out, plane_out, flag,
           tall, vecs, planes, outbox, halo, rows, conc, pots, diff, exch, slope, hs_sem, hr_sem, in_sem,
           *for_sums):
    *sums, sum_sems = for_sums
    loads = [
        pltpu.make_async_copy(source, target, in_sem.at[i])
        for i, (source, target) in enumerate((
            (conc_in, conc), (diff_in, diff), (exch_in, exch), (slope_in, slope), (pots_in, pots)))]
    for load in loads:
        load.start()

    gx = lax.axis_index("gx")
    gy = lax.axis_index("gy")
    groups = [Group(names, nx, ny, gx, gy) for names in STAGES]

    exists = {}
    for a, b in BLOCKS:
        inside = []
        if a:
            inside.append(gx + a < nx if a > 0 else gx + a >= 0)
        if b:
            inside.append(gy + b < ny if b > 0 else gy + b >= 0)
        exists[a, b] = inside[0] if len(inside) == 1 else jnp.logical_and(*inside)

    barrier = pltpu.get_barrier_semaphore()
    expected = 0
    for group in groups:
        for step in range(1, group.count):
            pl.semaphore_signal(
                barrier, inc=1, device_id=group.peer(step), device_id_type=MESH)
        expected = expected + group.count - 1
    for block in BLOCKS:
        @pl.when(exists[block])
        def _(block=block):
            pl.semaphore_signal(
                barrier, inc=1, device_id=(gx + block[0], gy + block[1]), device_id_type=MESH)
        expected = expected + exists[block].astype(jnp.int32)

    lane = lax.broadcasted_iota(jnp.int32, (8, 128), 1)
    sub = lax.broadcasted_iota(jnp.int32, (8, 128), 0)
    quarter = lane // 32
    x_of = (lane // 16) % 2
    y_of = lane % 16
    once = jnp.logical_and(sub == 0, quarter == 0)
    zero = jnp.zeros((8, 128), jnp.float32)

    for block in BLOCKS:
        @pl.when(jnp.logical_not(exists[block]))
        def _(block=block):
            for turn in range(len(ROUNDS)):
                count = message_rows(turn, block)
                if count:
                    halo[turn, SLOT[block], 0:count] = jnp.zeros((count, 128), jnp.float32)

    def spread(by_node):
        parts = [by_node[8 * q:8 * q + 8, :] for q in range(4)]
        return jnp.concatenate(parts, axis=1)

    def small(ref):
        return spread(ref[...].reshape(CELLS, CELLS).T)

    for load in loads:
        load.wait()
    diffusion = small(diff)
    exchange = small(exch)
    slopes = small(slope)
    pots_t = pots[...].reshape(CELLS, CELLS + 1).T
    pot = spread(pots_t[:CELLS])
    collector = jnp.broadcast_to(
        jnp.concatenate([pots_t[CELLS:CELLS + 1]] * 4, axis=1), (8, 128))
    planes[0, 0:8] = pot
    planes[0, 8:16] = collector
    rows[...] = jnp.zeros((128, 128), jnp.float32)

    flat = conc[...].reshape(CELLS, 2048)
    for g in range(4):
        block = jnp.concatenate(
            [flat[:, (4 * q + g) * 128:(4 * q + g + 1) * 128] for q in range(4)], axis=0)
        tall[g * 128:(g + 1) * 128, :] = block.T

    def pack(fields, side):
        start = 16 - WIDE if side == 1 else 0
        packed = zero
        for i, field in enumerate(fields):
            shift = (WIDE * i - start) % 128
            moved = pltpu.roll(field, shift, 1) if shift else field
            packed = jnp.where(jnp.logical_and(y_of >= WIDE * i, y_of < WIDE * (i + 1)), moved, packed)
        return packed

    def unpack(packed, i, side):
        start = 16 - WIDE if side == 1 else 0
        shift = (start - WIDE * i) % 128
        return pltpu.roll(packed, shift, 1) if shift else packed

    def fill_outbox(turn, pot, collector, shells, coefs):
        for i, field in enumerate([pot, collector] + coefs + shells):
            outbox[turn, 0, 8 * i:8 * i + 8] = field
        for side in (1, -1):
            fields = [pack([pot, collector] + shells[:1], side)]
            if coefs:
                fields.append(pack(coefs, side))
            if len(shells) > 1:
                fields.append(pack(shells[1:], side))
            for i, field in enumerate(fields):
                outbox[turn, side % 3, 8 * i:8 * i + 8] = field

    fill_outbox(0, pot, collector,
                [tall[pl.ds(SHELLS - 1 - i, 8, stride=SHELLS), :] for i in range(ROUNDS[0] - 1)],
                [exchange, slopes, diffusion])

    def first(b, acc):
        for i in range(8):
            r = b * 8 + i
            shell = tall[pl.ds(r, 8, stride=SHELLS), :]
            vecs[0, r] = shell
            acc = acc + shell * shell
        return acc

    def keep(k, i, acc):
        total = jnp.sum(acc, axis=0, keepdims=True)
        rows[DIM * k + i:DIM * k + i + 1, :] = total
        if i != k:
            rows[DIM * i + k:DIM * i + k + 1, :] = total

    def halo_copy(turn, block):
        a, b = block
        count = message_rows(turn, block)
        return pltpu.make_async_remote_copy(
            src_ref=outbox.at[turn, b % 3, pl.ds(0, count)],
            dst_ref=halo.at[turn, SLOT[-a, -b], pl.ds(0, count)],
            send_sem=hs_sem.at[turn, SLOT[block]],
            recv_sem=hr_sem.at[turn, SLOT[-a, -b]],
            device_id=(gx + a, gy + b),
            device_id_type=MESH,
        )

    def each_message(turn, act):
        for block in BLOCKS:
            if message_rows(turn, block):
                @pl.when(exists[block])
                def _(block=block):
                    act(block)

    def receive(turn, block):
        a, b = block
        count = message_rows(turn, block)
        pltpu.make_async_remote_copy(
            src_ref=outbox.at[turn, b % 3, pl.ds(0, count)],
            dst_ref=halo.at[turn, SLOT[block], pl.ds(0, count)],
            send_sem=hs_sem.at[turn, SLOT[block]],
            recv_sem=hr_sem.at[turn, SLOT[block]],
            device_id=(gx + a, gy + b),
            device_id_type=MESH,
        ).wait_recv()

    def send_round(turn):
        each_message(turn, lambda block: halo_copy(turn, block).start())

    pl.semaphore_wait(barrier, expected)
    send_round(0)
    acc = lax.fori_loop(0, 8, first, zero)
    keep(0, 0, acc + pot * pot + jnp.where(once, collector * collector, 0.0))

    def around(own, low_x, high_x, low_y, high_y):
        high = own if high_x is None else own + high_x
        low = own if low_x is None else own + low_x
        before = 0.0 if low_y is None else pltpu.roll(low_y, 113, 1)
        after = 0.0 if high_y is None else pltpu.roll(high_y, 15, 1)
        return (jnp.where(x_of == 1, pltpu.roll(high, 16, 1), pltpu.roll(low, 112, 1))
                + jnp.where(y_of > 0, pltpu.roll(own, 1, 1), before)
                + jnp.where(y_of < 15, pltpu.roll(own, 127, 1), after))

    def node_mirror(v):
        down = pltpu.roll(v, 1, 0)
        down = jnp.where(sub == 0, pltpu.roll(down, 32, 1), down)
        down = jnp.where(jnp.logical_and(sub == 0, quarter == 0), v, down)
        up = pltpu.roll(v, 7, 0)
        up = jnp.where(sub == 7, pltpu.roll(up, 96, 1), up)
        up = jnp.where(jnp.logical_and(sub == 7, quarter == 3), v, up)
        return 2.0 * v - down - up

    def over_quarters(v):
        return (v + pltpu.roll(v, 32, 1)) + (pltpu.roll(v, 64, 1) + pltpu.roll(v, 96, 1))

    def placed(block):
        return sub == block[0] + MIDDLE

    inside = {}
    for b in (-1, 0, 1):
        inside[b] = jnp.where(placed((0, b)), 1.0, 0.0) if b == 0 else zero
        for block in BLOCKS:
            if block[1] == b:
                inside[b] = jnp.where(
                    jnp.logical_and(placed(block), exists[block]), 1.0, inside[b])

    def potentials(turn, beside_step):
        depth, start = ROUNDS[turn], STARTS[turn]
        carried = ROUNDS[turn + 1] - 1 if turn + 1 < len(ROUNDS) else 0
        own = (0, 0)
        now = {own: (planes[start, 0:8],
                     [vecs[start, SHELLS - 1 - i] for i in range(depth + carried)])}
        coefs = {own: (exchange, slopes, diffusion)}
        fields = {-1: zero, 0: jnp.where(placed(own), planes[start, 8:16], 0.0), 1: zero}
        for block in BLOCKS:
            if message_rows(turn, block) == 0:
                continue
            updates = depth - steps_away(block)
            inbox = halo.at[turn, SLOT[block]]
            a, b = block
            if b:
                names = fields_of(turn, updates)
                found = {name: inbox[8 * i:8 * i + 8] for i, name in enumerate(names)}
                fields[b] = jnp.where(placed(block), found["pots"], fields[b])
                shells = [unpack(found["pots"], 2, -b)] if updates else []
                shells += [unpack(found["shells"], i, -b) for i in range(updates - 1)]
                now[block] = (unpack(found["pots"], 0, -b), shells)
                if updates:
                    source = halo[0, SLOT[block], 8:16]
                    coefs[block] = tuple(unpack(source, i, -b) for i in range(3))
                continue
            shells_at = 16 + (COEFS if turn == 0 else 0)
            fields[0] = jnp.where(placed(block), inbox[8:16], fields[0])
            now[block] = (inbox[0:8],
                          [inbox[shells_at + 8 * i:shells_at + 8 * i + 8] for i in range(updates)])
            if updates:
                source = halo.at[0, SLOT[block]]
                coefs[block] = (source[16:24], source[24:32], source[32:40])
        for b in (-1, 1):
            fields[b] = unpack(fields[b], 1, -b)
        before = fields_before = None
        for m in range(1, depth + 1):
            scale = (1.0 if m == 1 else 2.0) / HALF
            after, fields_after = {}, {}
            means = {-1: zero, 0: zero, 1: zero}
            for block in now:
                if steps_away(block) > depth - m:
                    continue
                a, b = block
                pot, shells = now[block]
                exchange_of, slope_of, diffusion_of = coefs[block]
                beside = [now.get(other) for other in (
                    (a - 1, b), (a + 1, b), (a, b - 1), (a, b + 1))]
                collector = jnp.broadcast_to(fields[b][a + MIDDLE:a + MIDDLE + 1], (8, 128))
                current = exchange_of * (pot - collector)
                means[b] = jnp.where(
                    placed(block),
                    jnp.broadcast_to(jnp.sum(current, axis=0, keepdims=True), (8, 128)), means[b])
                lateral = 4.0 * pot - around(
                    pot, *(None if other is None else other[0] for other in beside))
                new_pot = scale * (
                    node_cond * node_mirror(pot) + current - slope_of * shells[0]
                    + plane_cond * lateral - CENTER * pot)
                count = depth - m + carried if block == own else depth - steps_away(block) - m
                center_coef = scale * (1.0 - CENTER + 2.0 * diffusion_of)
                side_coef = scale * diffusion_of
                new_shells = []
                for i in range(count):
                    new = center_coef * shells[i] - side_coef * (shells[max(i - 1, 0)] + shells[i + 1])
                    if i == 0:
                        new = new + scale * current
                    if m > 1:
                        new = new - before[block][1][i]
                    new_shells.append(new)
                if m > 1:
                    new_pot = new_pot - before[block][0]
                if block != own:
                    new_pot = jnp.where(exists[block], new_pot, 0.0)
                after[block] = (new_pot, new_shells)
            for b in (-1, 0, 1):
                if m + abs(b) > depth:
                    fields_after[b] = zero
                    continue
                field = fields[b]
                lateral = 4.0 * field - around(
                    field, pltpu.roll(field, 1, 0), pltpu.roll(field, 7, 0),
                    fields.get(b - 1), fields.get(b + 1))
                new = scale * (collector_cond * lateral
                               - over_quarters(means[b]) * (1.0 / 32.0) - CENTER * field)
                if m > 1:
                    new = new - fields_before[b]
                fields_after[b] = jnp.where(inside[b] > 0.0, new, 0.0)
            planes[start + m, 0:8] = after[own][0]
            planes[start + m, 8:16] = jnp.broadcast_to(
                fields_after[0][MIDDLE:MIDDLE + 1], (8, 128))
            before, now = now, after
            fields_before, fields = fields, fields_after
            beside_step(start + m)
        if turn + 1 < len(ROUNDS):
            fill_outbox(turn + 1, now[own][0], planes[start + depth, 8:16], now[own][1], [])


    def bulk_shells(k, unrolled=False):
        scale = (1.0 if is_first(k) else 2.0) / HALF
        current = exchange * (planes[k, 0:8] - planes[k, 8:16])
        center_coef = scale * (1.0 - CENTER + 2.0 * diffusion)
        side_coef = scale * diffusion

        def shells(base, accs, last):
            accs = list(accs)
            low = vecs[k, max(base - 1, 0) if isinstance(base, int) else jnp.maximum(base - 1, 0)]
            here = vecs[k, base]
            for i in range(8):
                r = base + i
                high = here if last and i == 7 else vecs[k, r + 1]
                new = center_coef * here - side_coef * (low + high)
                if last and i == 7:
                    new = new + scale * current
                if not is_first(k):
                    new = new - vecs[k - 1, r]
                vecs[k + 1, r] = new
                for m in range(k):
                    accs[m] = accs[m] + new * vecs[m, r]
                accs[k] = accs[k] + new * here
                accs[k + 1] = accs[k + 1] + new * new
                low, here = here, high
            return tuple(accs)

        accs = (zero,) * (k + 2)
        if unrolled:
            for b in range(7):
                accs = shells(b * 8, accs, False)
        else:
            accs = lax.fori_loop(0, 7, lambda b, accs: shells(b * 8, accs, False), accs)
        return shells(SHELLS - 8, accs, True)

    def products(k, accs):
        new_pot, new_collector = planes[k + 1, 0:8], planes[k + 1, 8:16]
        for m in range(k + 2):
            acc = accs[m] + new_pot * planes[m, 0:8] + jnp.where(
                once, new_collector * planes[m, 8:16], 0.0)
            keep(k + 1, m, acc)

    for turn, start in enumerate(STARTS):
        end = start + ROUNDS[turn]
        accs = {start: bulk_shells(start)}
        each_message(turn, functools.partial(receive, turn))
        if turn + 1 < len(ROUNDS):
            potentials(turn, lambda k: None)
            send_round(turn + 1)
            for k in range(start + 1, end):
                accs[k] = bulk_shells(k)
        else:
            def beside(k):
                if k < end:
                    accs[k] = bulk_shells(k, True)

            potentials(turn, beside)
        for k in range(start, end):
            products(k, accs[k])

    def copy(stage, step):
        group = groups[stage]
        return pltpu.make_async_remote_copy(
            src_ref=sums[stage].at[group.slot],
            dst_ref=sums[stage].at[group.slot],
            send_sem=sum_sems.at[stage, 0],
            recv_sem=sum_sems.at[stage, 1],
            device_id=group.peer(step),
            device_id_type=MESH,
        )

    def all_copies(stage):
        group = groups[stage]
        rest = sums[stage].at[pl.ds(0, group.count - 1)]
        return pltpu.make_async_remote_copy(
            src_ref=rest,
            dst_ref=rest,
            send_sem=sum_sems.at[stage, 0],
            recv_sem=sum_sems.at[stage, 1],
            device_id=group.peer(1),
            device_id_type=MESH,
        )

    whole = jnp.sum(rows[...].T, axis=0, keepdims=True)
    for stage, group in enumerate(groups):
        sums[stage][pl.ds(group.slot, 1)] = whole.reshape(1, 1, 128)
        for step in range(1, group.count):
            copy(stage, step).start()
        all_copies(stage).wait_recv()
        whole = jnp.sum(sums[stage][...], axis=0)

    lane2 = lax.broadcasted_iota(jnp.int32, (16, 128), 1)
    sub2 = lax.broadcasted_iota(jnp.int32, (16, 128), 0)
    eye = sub2 == lane2
    whole = jnp.broadcast_to(whole, (16, 128))
    gram = jnp.zeros((16, 128), jnp.float32)
    for k in range(DIM):
        moved = whole if k == 0 else pltpu.roll(whole, (128 - DIM * k) % 128, 1)
        gram = jnp.where(sub2 == k, moved, gram)
    gram = jnp.where(lane2 < DIM, gram, 0.0)

    def down(v):
        return jnp.broadcast_to(jnp.sum(v, axis=0, keepdims=True), (16, 128))

    def turned(v):
        return jnp.broadcast_to(
            jnp.sum(jnp.where(eye, v, 0.0), axis=1, keepdims=True), (16, 128))

    diagonal = jnp.broadcast_to(
        jnp.sum(jnp.where(eye, gram, 0.0), axis=1, keepdims=True), (16, 128))
    lengths = jnp.sqrt(jnp.maximum(diagonal, 0.0))
    beta = jnp.sqrt(jnp.broadcast_to(diagonal[0:1], (16, 128)) + epsilon)
    inverse = 1.0 / beta
    up_coef = jnp.zeros((16, 128), jnp.float32)
    down_coef = jnp.zeros((16, 128), jnp.float32)
    for k in range(ITERS):
        up_coef = jnp.where(sub2 == k + 1, HALF if is_first(k) else HALF / 2, up_coef)
        if not is_first(k):
            down_coef = jnp.where(sub2 == k - 1, HALF / 2, down_coef)
    g_lane = jnp.broadcast_to(gram[0:1], (16, 128)) * inverse
    c_lane = jnp.where(lane2 == 0, inverse, 0.0)
    g_sub = turned(g_lane)
    c_sub = jnp.where(sub2 == 0, inverse, 0.0)
    rest_t = jnp.where(eye, 1.0, 0.0) - g_sub * c_lane
    gram_rest_t = gram - g_sub * g_lane
    images = jnp.where(lane2 == 0, g_sub, 0.0)
    coords = [c_sub]
    trust = jnp.ones((16, 128), jnp.float32)

    cosines, sines, inverse_radii, upper = [], [], [], []
    target = [beta[0:1]]
    for j in range(ITERS):
        w_sub = (CENTER * c_sub + up_coef * pltpu.roll(c_sub, 1, 0)
                 + down_coef * pltpu.roll(c_sub, 15, 0))
        u_lane = down(rest_t * w_sub)
        gu_lane = down(gram_rest_t * w_sub)
        h_lane = down(images * w_sub)
        u_sub, gu_sub, h_sub = turned(u_lane), turned(gu_lane), turned(h_lane)
        square = down(u_sub * gu_sub)
        spread_square = down(jnp.abs(u_sub) * lengths)
        trust = jnp.where(square > TRUST * spread_square * spread_square, trust, 0.0)
        height = jnp.sqrt(jnp.maximum(square, 0.0) + epsilon)
        inverse = 1.0 / height
        if j + 1 < ITERS:
            c_sub, g_sub = u_sub * inverse, gu_sub * inverse
            c_lane, g_lane = u_lane * inverse, gu_lane * inverse
            rest_t = rest_t - g_sub * c_lane
            gram_rest_t = gram_rest_t - g_sub * g_lane
            images = jnp.where(lane2 == j + 1, g_sub, images)
            coords.append(c_sub)
        entries = [h_sub[i:i + 1] for i in range(j + 1)] + [height[0:1]]
        for row in range(j):
            entries[row], entries[row + 1] = (
                cosines[row] * entries[row] + sines[row] * entries[row + 1],
                cosines[row] * entries[row + 1] - sines[row] * entries[row])
        radius = jnp.sqrt(entries[j] * entries[j] + entries[j + 1] * entries[j + 1])
        inverse_radius = 1.0 / radius
        cosines.append(entries[j] * inverse_radius)
        sines.append(entries[j + 1] * inverse_radius)
        inverse_radii.append(inverse_radius)
        upper.append(entries[:j])
        lead = target[j]
        target[j] = cosines[j] * lead
        target.append(-sines[j] * lead)
    weights = [None] * ITERS
    for row in range(ITERS - 1, -1, -1):
        value = target[row]
        for later in range(ITERS - 1, row, -1):
            value = value - upper[later][row] * weights[later]
        weights[row] = value * inverse_radii[row]
    coef = weights[0] * coords[0]
    for j in range(1, ITERS):
        coef = coef + weights[j] * coords[j]
    flag[0, 0] = jnp.min(trust)
    coefs = [jnp.broadcast_to(coef[k:k + 1], (8, 128)) for k in range(ITERS)]

    def combine(b, carry):
        for i in range(8):
            r = b * 8 + i
            value = coefs[0] * vecs[0, r]
            for k in range(1, ITERS):
                value = value + coefs[k] * vecs[k, r]
            tall_out[pl.ds(r, 8, stride=SHELLS), :] = value
        return carry

    lax.fori_loop(0, 8, combine, 0)
    sol = coefs[0] * planes[0, 0:8]
    sol_collector = coefs[0] * planes[0, 8:16]
    for k in range(1, ITERS):
        sol = sol + coefs[k] * planes[k, 0:8]
        sol_collector = sol_collector + coefs[k] * planes[k, 8:16]
    plane_out[0:8] = sol
    plane_out[8:16] = sol_collector

    for turn in range(len(ROUNDS)):
        each_message(turn, lambda block: halo_copy(turn, block).wait_send())
    for stage in range(len(STAGES)):
        all_copies(stage).wait_send()


def results(tall, planes, out_c, out_p):
    for g in range(4):
        block = tall[g * 128:(g + 1) * 128, :].T
        for q in range(4):
            at = (4 * q + g) * 128
            out_c[:, :, at:at + 128] = block[q * 32:(q + 1) * 32].reshape(2, 16, 128)
    sol = planes[0:8]
    by_node = [sol if q == 0 else pltpu.roll(sol, 128 - 32 * q, 1) for q in range(4)]
    by_node = jnp.concatenate(
        by_node + [planes[8:16], jnp.zeros((88, 128), jnp.float32)], axis=0)
    out_p[...] = by_node.T[:CELLS, :CELLS + 1].reshape(2, 16, CELLS + 1)


def fast(nx, ny, *args):
    counts = [members(names, nx, ny) for names in STAGES]
    f32 = jnp.float32
    vmem = pl.BlockSpec(memory_space=pltpu.VMEM)
    tall, planes, flag = pl.pallas_call(
        functools.partial(kernel, nx, ny),
        out_shape=(
            pltpu.VMEM((512, 128), f32),
            pltpu.VMEM((16, 128), f32),
            jax.ShapeDtypeStruct((1, 1), f32),
        ),
        in_specs=[pl.BlockSpec(memory_space=pltpu.HBM)] * 5,
        out_specs=(vmem, vmem, pl.BlockSpec(memory_space=pltpu.SMEM)),
        scratch_shapes=[
            pltpu.VMEM((512, 128), f32),
            pltpu.VMEM((DIM, SHELLS, 8, 128), f32),
            pltpu.VMEM((DIM, 16, 128), f32),
            pltpu.VMEM((len(ROUNDS), 3, OUTBOX, 128), f32),
            pltpu.VMEM((len(ROUNDS), len(BLOCKS), OUTBOX, 128), f32),
            pltpu.VMEM((128, 128), f32),
            *(pltpu.VMEM(a.shape, f32) for a in args),
            pltpu.SemaphoreType.DMA((len(ROUNDS), len(BLOCKS))),
            pltpu.SemaphoreType.DMA((len(ROUNDS), len(BLOCKS))),
            pltpu.SemaphoreType.DMA((5,)),
            *(pltpu.VMEM((count, 1, 128), f32) for count in counts),
            pltpu.SemaphoreType.DMA((len(STAGES), 2)),
        ],
        compiler_params=pltpu.CompilerParams(collective_id=0, has_side_effects=True),
    )(*args)
    conc, pots = pl.pallas_call(
        results,
        out_shape=tuple(jax.ShapeDtypeStruct(a.shape, f32) for a in args[:2]),
        in_specs=[vmem] * 2,
        out_specs=(vmem,) * 2,
    )(*(pltpu.with_memory_space_constraint(a, pltpu.VMEM) for a in (tall, planes)))
    return conc, pots, flag


def with_halo(shard, sides, width):
    edges = {}
    for axis, dim in sides:
        size, length = (lax.axis_size(axis), shard.shape[dim])
        up = [(i, (i + 1) % size) for i in range(size - 1)]
        last = lax.slice_in_dim(shard, length - width, length, axis=dim)
        initial = lax.slice_in_dim(shard, 0, width, axis=dim)
        edges[dim] = (
            lax.ppermute(last, axis, up),
            lax.ppermute(initial, axis, [(b, a) for a, b in up]),
        )
    done = []
    for _, dim in sides:
        low, high = edges[dim]
        around = [(width, width) if d in done else (0, 0) for d in range(shard.ndim)]
        shard = jnp.concatenate([jnp.pad(low, around), shard, jnp.pad(high, around)], axis=dim)
        done.append(dim)
    return shard


def total_of(shard):
    return lax.all_gather(shard, ("gx", "gy")).sum(axis=0)


def mirror_laplace(values):
    inner = jnp.concatenate([values[..., :1], values[..., :-1]], axis=-1)
    outer = jnp.concatenate([values[..., 1:], values[..., -1:]], axis=-1)
    return 2.0 * values - inner - outer


def local_operator(conc, padded, diffusion, exchange, slope):
    nodes = exchange.shape[2]
    shell_count = conc.shape[2] // nodes
    shells = conc.reshape(conc.shape[0], conc.shape[1], nodes, shell_count)
    center = padded[1:-1, 1:-1]
    lateral = (
        4.0 * center - padded[2:, 1:-1] - padded[:-2, 1:-1] - padded[1:-1, 2:] - padded[1:-1, :-2]
    )
    node_pot = center[..., :nodes]
    collector = center[..., nodes]
    current = exchange * (node_pot - collector[..., None])
    surface = shells[..., shell_count - 1]
    surface_flag = (lax.broadcasted_iota(jnp.int32, (shell_count,), 0) == shell_count - 1).astype(
        jnp.float32
    )
    new_shells = (
        shells + diffusion[..., None] * mirror_laplace(shells) + current[..., None] * surface_flag
    )
    new_nodes = (
        node_cond * mirror_laplace(node_pot)
        + current
        - slope * surface
        + plane_cond * lateral[..., :nodes]
    )
    new_collector = collector_cond * lateral[..., nodes] - jnp.mean(current, axis=-1)
    return (
        new_shells.reshape(conc.shape),
        jnp.concatenate([new_nodes, new_collector[..., None]], axis=-1),
    )


def step_by_step(rhs_conc, rhs_pots, diffusion, exchange, slope):
    first = jnp.sum(rhs_conc * rhs_conc) + jnp.sum(rhs_pots * rhs_pots)
    start_norm = jnp.sqrt(total_of(first.reshape(1))[0] + epsilon)
    all_conc = jnp.zeros((DIM, *rhs_conc.shape), jnp.float32).at[0].set(rhs_conc / start_norm)
    all_pots = jnp.zeros((DIM, *rhs_pots.shape), jnp.float32).at[0].set(rhs_pots / start_norm)
    matrix = jnp.zeros((DIM, DIM), jnp.float32)

    def arnoldi(step, state):
        all_conc, all_pots, matrix = state
        padded = with_halo(all_pots[step], (("gx", 0), ("gy", 1)), 1)
        image_conc, image_pots = local_operator(all_conc[step], padded, diffusion, exchange, slope)
        local_dots = jnp.sum(all_conc * image_conc, axis=(1, 2, 3)) + jnp.sum(
            all_pots * image_pots, axis=(1, 2, 3))
        coeffs = total_of(local_dots)
        rest_conc = image_conc - jnp.sum(coeffs[:, None, None, None] * all_conc, axis=0)
        rest_pots = image_pots - jnp.sum(coeffs[:, None, None, None] * all_pots, axis=0)
        rest = jnp.sum(rest_conc * rest_conc) + jnp.sum(rest_pots * rest_pots)
        height = jnp.sqrt(total_of(rest.reshape(1))[0] + epsilon)
        column = jnp.where(jnp.arange(DIM) == step + 1, height, coeffs)
        return (
            lax.dynamic_update_index_in_dim(all_conc, rest_conc / height, step + 1, 0),
            lax.dynamic_update_index_in_dim(all_pots, rest_pots / height, step + 1, 0),
            lax.dynamic_update_index_in_dim(matrix, column, step, 0),
        )

    all_conc, all_pots, matrix = lax.fori_loop(
        0, ITERS, arnoldi, (all_conc, all_pots, matrix))

    def rotate(step, state):
        matrix, target = state
        pair = matrix[step]
        lead, under = pair[step], pair[step + 1]
        radius = jnp.sqrt(lead * lead + under * under)
        cosine, sine = lead / radius, under / radius

        def turn(values):
            a = lax.dynamic_index_in_dim(values, step, values.ndim - 1)
            b = lax.dynamic_index_in_dim(values, step + 1, values.ndim - 1)
            values = lax.dynamic_update_slice_in_dim(
                values, cosine * a + sine * b, step, values.ndim - 1)
            return lax.dynamic_update_slice_in_dim(
                values, cosine * b - sine * a, step + 1, values.ndim - 1)

        return turn(matrix), turn(target)

    target = jnp.zeros((DIM,), jnp.float32).at[0].set(start_norm)
    matrix, target = lax.fori_loop(0, ITERS, rotate, (matrix, target))

    def back(i, weights):
        row = ITERS - 1 - i
        known = jnp.sum(matrix[:, row] * weights)
        return weights.at[row].set((target[row] - known) / matrix[row, row])

    weights = lax.fori_loop(0, ITERS, back, jnp.zeros((DIM,), jnp.float32))
    weights = weights[:, None, None, None]
    return jnp.sum(weights * all_conc, axis=0), jnp.sum(weights * all_pots, axis=0)


def solution(mesh):
    nx, ny = mesh.shape["gx"], mesh.shape["gy"]

    def shards(*args):
        conc, pots, flag = fast(nx, ny, *args)

        def again(state):
            conc, pots = step_by_step(*args)
            return conc, pots, jnp.ones_like(state[2])

        return lax.while_loop(
            lambda state: state[2] < 0.5, again, (conc, pots, flag[0, 0]))[:2]

    spec = P("gx", "gy", None)
    return jax.shard_map(
        shards, mesh=mesh, in_specs=(spec,) * 5, out_specs=(spec,) * 2, check_vma=False)
```

```python
import functools
import jax
import jax.numpy as jnp
from jax import lax
from jax.experimental import pallas as pl
from jax.experimental.pallas import tpu as pltpu
from jax.sharding import Mesh
from jax.sharding import PartitionSpec as P

ITERS = 10
MESH = pl.DeviceIdType.MESH
GX = ("gx_0", "gx_1", "gx_2")

node_cond = 1.0
plane_cond = 0.5
collector_cond = 2.0
epsilon = 1e-06

ROUNDS = (5, 5)
CENTER = 11.0
HALF = 10.0
TRUST = 1e-4

CELLS = 32
SHELLS = 64
DIM = ITERS + 1
STARTS = tuple(sum(ROUNDS[:i]) for i in range(len(ROUNDS)))


def steps_away(block):
    a, b = block
    return max(2 * abs(a) - 1, 0) + abs(b)


DEEPEST = max(ROUNDS)
BLOCKS = sorted(
    ((a, b) for a in range(-DEEPEST, DEEPEST + 1) for b in (-1, 0, 1)
     if 0 < steps_away((a, b)) <= DEEPEST),
    key=lambda block: (-steps_away(block), block))
SLOT = {block: i for i, block in enumerate(BLOCKS)}
COEFS = 24
OUTBOX = 16 + COEFS + 8 * (DEEPEST - 1)


def message_rows(turn, block):
    updates = ROUNDS[turn] - steps_away(block)
    if updates < 0:
        return 0
    if block[1]:
        return 8 * len(fields_of(turn, updates))
    if updates == 0:
        return 16
    return 16 + (COEFS if turn == 0 else 0) + 8 * updates


MIDDLE = 3
assert max(abs(a) for a, _ in BLOCKS) <= MIDDLE
WIDE = 5
assert DEEPEST <= WIDE


def fields_of(turn, updates):
    names = ["pots"]
    if updates and turn == 0:
        names.append("coefs")
    if updates > 1:
        names.append("shells")
    return names


STAGES = ("core", "z", "plane")


def members(name, nx, ny):
    return {"core": 2, "z": ny, "plane": nx // 2}[name]


class Group:
    def __init__(self, name, nx, ny, gx, gy):
        self.name, self.gx, self.gy = name, gx, gy
        self.core, self.plane = lax.rem(gx, 2), lax.div(gx, 2)
        self.count = members(name, nx, ny)
        self.slot = {"core": self.core, "z": gy, "plane": self.plane}[name]

    def peer(self, step):
        if self.count == 2:
            other = 1 - self.slot
        else:
            other = self.slot + step
            other = jnp.where(other >= self.count, other - self.count, other)
        if self.name == "core":
            return 2 * self.plane + other, self.gy
        if self.name == "z":
            return self.gx, other
        return 2 * other + self.core, self.gy


def is_first(k):
    return k in STARTS


def kernel(nx, ny, conc_in, pots_in, diff_in, exch_in, slope_in, tall_out, plane_out,
           tall, vecs, planes, outbox, halo, rows, conc, pots, diff, exch, slope, hs_sem, hr_sem, in_sem,
           *for_sums):
    *sums, sum_sems = for_sums
    loads = [
        pltpu.make_async_copy(source, target, in_sem.at[i])
        for i, (source, target) in enumerate((
            (conc_in, conc), (diff_in, diff), (exch_in, exch), (slope_in, slope), (pots_in, pots)))]
    for load in loads:
        load.start()

    gx = lax.axis_index("gx")
    gy = lax.axis_index("gy")
    groups = [Group(names, nx, ny, gx, gy) for names in STAGES]

    exists = {}
    for a, b in BLOCKS:
        inside = []
        if a:
            inside.append(gx + a < nx if a > 0 else gx + a >= 0)
        if b:
            inside.append(gy + b < ny if b > 0 else gy + b >= 0)
        exists[a, b] = inside[0] if len(inside) == 1 else jnp.logical_and(*inside)

    barrier = pltpu.get_barrier_semaphore()
    expected = 0
    for group in groups:
        for step in range(1, group.count):
            pl.semaphore_signal(
                barrier, inc=1, device_id=group.peer(step), device_id_type=MESH)
        expected = expected + group.count - 1
    for block in BLOCKS:
        @pl.when(exists[block])
        def _(block=block):
            pl.semaphore_signal(
                barrier, inc=1, device_id=(gx + block[0], gy + block[1]), device_id_type=MESH)
        expected = expected + exists[block].astype(jnp.int32)

    lane = lax.broadcasted_iota(jnp.int32, (8, 128), 1)
    sub = lax.broadcasted_iota(jnp.int32, (8, 128), 0)
    quarter = lane // 32
    x_of = (lane // 16) % 2
    y_of = lane % 16
    once = jnp.logical_and(sub == 0, quarter == 0)
    zero = jnp.zeros((8, 128), jnp.float32)

    for block in BLOCKS:
        @pl.when(jnp.logical_not(exists[block]))
        def _(block=block):
            for turn in range(len(ROUNDS)):
                count = message_rows(turn, block)
                if count:
                    halo[turn, SLOT[block], 0:count] = jnp.zeros((count, 128), jnp.float32)

    def spread(by_node):
        parts = [by_node[8 * q:8 * q + 8, :] for q in range(4)]
        return jnp.concatenate(parts, axis=1)

    def small(ref):
        return spread(ref[...].reshape(CELLS, CELLS).T)

    for load in loads:
        load.wait()
    diffusion = small(diff)
    exchange = small(exch)
    slopes = small(slope)
    pots_t = pots[...].reshape(CELLS, CELLS + 1).T
    pot = spread(pots_t[:CELLS])
    collector = jnp.broadcast_to(
        jnp.concatenate([pots_t[CELLS:CELLS + 1]] * 4, axis=1), (8, 128))
    planes[0, 0:8] = pot
    planes[0, 8:16] = collector
    rows[...] = jnp.zeros((128, 128), jnp.float32)

    flat = conc[...].reshape(CELLS, 2048)
    for g in range(4):
        block = jnp.concatenate(
            [flat[:, (4 * q + g) * 128:(4 * q + g + 1) * 128] for q in range(4)], axis=0)
        tall[g * 128:(g + 1) * 128, :] = block.T

    def pack(fields, side):
        start = 16 - WIDE if side == 1 else 0
        packed = zero
        for i, field in enumerate(fields):
            shift = (WIDE * i - start) % 128
            moved = pltpu.roll(field, shift, 1) if shift else field
            packed = jnp.where(jnp.logical_and(y_of >= WIDE * i, y_of < WIDE * (i + 1)), moved, packed)
        return packed

    def unpack(packed, i, side):
        start = 16 - WIDE if side == 1 else 0
        shift = (start - WIDE * i) % 128
        return pltpu.roll(packed, shift, 1) if shift else packed

    def fill_outbox(turn, pot, collector, shells, coefs):
        for i, field in enumerate([pot, collector] + coefs + shells):
            outbox[turn, 0, 8 * i:8 * i + 8] = field
        for side in (1, -1):
            fields = [pack([pot, collector] + shells[:1], side)]
            if coefs:
                fields.append(pack(coefs, side))
            if len(shells) > 1:
                fields.append(pack(shells[1:], side))
            for i, field in enumerate(fields):
                outbox[turn, side % 3, 8 * i:8 * i + 8] = field

    fill_outbox(0, pot, collector,
                [tall[pl.ds(SHELLS - 1 - i, 8, stride=SHELLS), :] for i in range(ROUNDS[0] - 1)],
                [exchange, slopes, diffusion])

    def first(b, acc):
        for i in range(8):
            r = b * 8 + i
            shell = tall[pl.ds(r, 8, stride=SHELLS), :]
            vecs[0, r] = shell
            acc = acc + shell * shell
        return acc

    def keep(k, i, acc):
        total = jnp.sum(acc, axis=0, keepdims=True)
        rows[DIM * k + i:DIM * k + i + 1, :] = total
        if i != k:
            rows[DIM * i + k:DIM * i + k + 1, :] = total

    def halo_copy(turn, block):
        a, b = block
        count = message_rows(turn, block)
        return pltpu.make_async_remote_copy(
            src_ref=outbox.at[turn, b % 3, pl.ds(0, count)],
            dst_ref=halo.at[turn, SLOT[-a, -b], pl.ds(0, count)],
            send_sem=hs_sem.at[turn, SLOT[block]],
            recv_sem=hr_sem.at[turn, SLOT[-a, -b]],
            device_id=(gx + a, gy + b),
            device_id_type=MESH,
        )

    def each_message(turn, act):
        for block in BLOCKS:
            if message_rows(turn, block):
                @pl.when(exists[block])
                def _(block=block):
                    act(block)

    def receive(turn, block):
        a, b = block
        count = message_rows(turn, block)
        pltpu.make_async_remote_copy(
            src_ref=outbox.at[turn, b % 3, pl.ds(0, count)],
            dst_ref=halo.at[turn, SLOT[block], pl.ds(0, count)],
            send_sem=hs_sem.at[turn, SLOT[block]],
            recv_sem=hr_sem.at[turn, SLOT[block]],
            device_id=(gx + a, gy + b),
            device_id_type=MESH,
        ).wait_recv()

    def send_round(turn):
        each_message(turn, lambda block: halo_copy(turn, block).start())

    pl.semaphore_wait(barrier, expected)
    send_round(0)
    acc = lax.fori_loop(0, 8, first, zero)
    keep(0, 0, acc + pot * pot + jnp.where(once, collector * collector, 0.0))

    def around(own, low_x, high_x, low_y, high_y):
        high = own if high_x is None else own + high_x
        low = own if low_x is None else own + low_x
        before = 0.0 if low_y is None else pltpu.roll(low_y, 113, 1)
        after = 0.0 if high_y is None else pltpu.roll(high_y, 15, 1)
        return (jnp.where(x_of == 1, pltpu.roll(high, 16, 1), pltpu.roll(low, 112, 1))
                + jnp.where(y_of > 0, pltpu.roll(own, 1, 1), before)
                + jnp.where(y_of < 15, pltpu.roll(own, 127, 1), after))

    def node_mirror(v):
        down = pltpu.roll(v, 1, 0)
        down = jnp.where(sub == 0, pltpu.roll(down, 32, 1), down)
        down = jnp.where(jnp.logical_and(sub == 0, quarter == 0), v, down)
        up = pltpu.roll(v, 7, 0)
        up = jnp.where(sub == 7, pltpu.roll(up, 96, 1), up)
        up = jnp.where(jnp.logical_and(sub == 7, quarter == 3), v, up)
        return 2.0 * v - down - up

    def over_quarters(v):
        return (v + pltpu.roll(v, 32, 1)) + (pltpu.roll(v, 64, 1) + pltpu.roll(v, 96, 1))

    def placed(block):
        return sub == block[0] + MIDDLE

    inside = {}
    for b in (-1, 0, 1):
        inside[b] = jnp.where(placed((0, b)), 1.0, 0.0) if b == 0 else zero
        for block in BLOCKS:
            if block[1] == b:
                inside[b] = jnp.where(
                    jnp.logical_and(placed(block), exists[block]), 1.0, inside[b])

    def potentials(turn, beside_step):
        depth, start = ROUNDS[turn], STARTS[turn]
        carried = ROUNDS[turn + 1] - 1 if turn + 1 < len(ROUNDS) else 0
        own = (0, 0)
        now = {own: (planes[start, 0:8],
                     [vecs[start, SHELLS - 1 - i] for i in range(depth + carried)])}
        coefs = {own: (exchange, slopes, diffusion)}
        fields = {-1: zero, 0: jnp.where(placed(own), planes[start, 8:16], 0.0), 1: zero}
        for block in BLOCKS:
            if message_rows(turn, block) == 0:
                continue
            updates = depth - steps_away(block)
            inbox = halo.at[turn, SLOT[block]]
            a, b = block
            if b:
                names = fields_of(turn, updates)
                found = {name: inbox[8 * i:8 * i + 8] for i, name in enumerate(names)}
                fields[b] = jnp.where(placed(block), found["pots"], fields[b])
                shells = [unpack(found["pots"], 2, -b)] if updates else []
                shells += [unpack(found["shells"], i, -b) for i in range(updates - 1)]
                now[block] = (unpack(found["pots"], 0, -b), shells)
                if updates:
                    source = halo[0, SLOT[block], 8:16]
                    coefs[block] = tuple(unpack(source, i, -b) for i in range(3))
                continue
            shells_at = 16 + (COEFS if turn == 0 else 0)
            fields[0] = jnp.where(placed(block), inbox[8:16], fields[0])
            now[block] = (inbox[0:8],
                          [inbox[shells_at + 8 * i:shells_at + 8 * i + 8] for i in range(updates)])
            if updates:
                source = halo.at[0, SLOT[block]]
                coefs[block] = (source[16:24], source[24:32], source[32:40])
        for b in (-1, 1):
            fields[b] = unpack(fields[b], 1, -b)
        before = fields_before = None
        for m in range(1, depth + 1):
            scale = (1.0 if m == 1 else 2.0) / HALF
            after, fields_after = {}, {}
            means = {-1: zero, 0: zero, 1: zero}
            for block in now:
                if steps_away(block) > depth - m:
                    continue
                a, b = block
                pot, shells = now[block]
                exchange_of, slope_of, diffusion_of = coefs[block]
                beside = [now.get(other) for other in (
                    (a - 1, b), (a + 1, b), (a, b - 1), (a, b + 1))]
                collector = jnp.broadcast_to(fields[b][a + MIDDLE:a + MIDDLE + 1], (8, 128))
                current = exchange_of * (pot - collector)
                means[b] = jnp.where(
                    placed(block),
                    jnp.broadcast_to(jnp.sum(current, axis=0, keepdims=True), (8, 128)), means[b])
                lateral = 4.0 * pot - around(
                    pot, *(None if other is None else other[0] for other in beside))
                new_pot = scale * (
                    node_cond * node_mirror(pot) + current - slope_of * shells[0]
                    + plane_cond * lateral - CENTER * pot)
                count = depth - m + carried if block == own else depth - steps_away(block) - m
                center_coef = scale * (1.0 - CENTER + 2.0 * diffusion_of)
                side_coef = scale * diffusion_of
                new_shells = []
                for i in range(count):
                    new = center_coef * shells[i] - side_coef * (shells[max(i - 1, 0)] + shells[i + 1])
                    if i == 0:
                        new = new + scale * current
                    if m > 1:
                        new = new - before[block][1][i]
                    new_shells.append(new)
                if m > 1:
                    new_pot = new_pot - before[block][0]
                if block != own:
                    new_pot = jnp.where(exists[block], new_pot, 0.0)
                after[block] = (new_pot, new_shells)
            for b in (-1, 0, 1):
                if m + abs(b) > depth:
                    fields_after[b] = zero
                    continue
                field = fields[b]
                lateral = 4.0 * field - around(
                    field, pltpu.roll(field, 1, 0), pltpu.roll(field, 7, 0),
                    fields.get(b - 1), fields.get(b + 1))
                new = scale * (collector_cond * lateral
                               - over_quarters(means[b]) * (1.0 / 32.0) - CENTER * field)
                if m > 1:
                    new = new - fields_before[b]
                fields_after[b] = jnp.where(inside[b] > 0.0, new, 0.0)
            planes[start + m, 0:8] = after[own][0]
            planes[start + m, 8:16] = jnp.broadcast_to(
                fields_after[0][MIDDLE:MIDDLE + 1], (8, 128))
            before, now = now, after
            fields_before, fields = fields, fields_after
            beside_step(start + m)
        if turn + 1 < len(ROUNDS):
            fill_outbox(turn + 1, now[own][0], planes[start + depth, 8:16], now[own][1], [])


    def bulk_shells(k, unrolled=False):
        scale = (1.0 if is_first(k) else 2.0) / HALF
        current = exchange * (planes[k, 0:8] - planes[k, 8:16])
        center_coef = scale * (1.0 - CENTER + 2.0 * diffusion)
        side_coef = scale * diffusion

        def shells(base, accs, last):
            accs = list(accs)
            low = vecs[k, max(base - 1, 0) if isinstance(base, int) else jnp.maximum(base - 1, 0)]
            here = vecs[k, base]
            for i in range(8):
                r = base + i
                high = here if last and i == 7 else vecs[k, r + 1]
                new = center_coef * here - side_coef * (low + high)
                if last and i == 7:
                    new = new + scale * current
                if not is_first(k):
                    new = new - vecs[k - 1, r]
                vecs[k + 1, r] = new
                for m in range(k):
                    accs[m] = accs[m] + new * vecs[m, r]
                accs[k] = accs[k] + new * here
                accs[k + 1] = accs[k + 1] + new * new
                low, here = here, high
            return tuple(accs)

        accs = (zero,) * (k + 2)
        if unrolled:
            for b in range(7):
                accs = shells(b * 8, accs, False)
        else:
            accs = lax.fori_loop(0, 7, lambda b, accs: shells(b * 8, accs, False), accs)
        return shells(SHELLS - 8, accs, True)

    def products(k, accs):
        new_pot, new_collector = planes[k + 1, 0:8], planes[k + 1, 8:16]
        for m in range(k + 2):
            acc = accs[m] + new_pot * planes[m, 0:8] + jnp.where(
                once, new_collector * planes[m, 8:16], 0.0)
            keep(k + 1, m, acc)

    for turn, start in enumerate(STARTS):
        end = start + ROUNDS[turn]
        accs = {start: bulk_shells(start)}
        each_message(turn, functools.partial(receive, turn))
        if turn + 1 < len(ROUNDS):
            potentials(turn, lambda k: None)
            send_round(turn + 1)
            for k in range(start + 1, end):
                accs[k] = bulk_shells(k)
        else:
            def beside(k):
                if k < end:
                    accs[k] = bulk_shells(k, True)

            potentials(turn, beside)
        for k in range(start, end):
            products(k, accs[k])

    def copy(stage, step):
        group = groups[stage]
        return pltpu.make_async_remote_copy(
            src_ref=sums[stage].at[group.slot],
            dst_ref=sums[stage].at[group.slot],
            send_sem=sum_sems.at[stage, 0],
            recv_sem=sum_sems.at[stage, 1],
            device_id=group.peer(step),
            device_id_type=MESH,
        )

    def all_copies(stage):
        group = groups[stage]
        rest = sums[stage].at[pl.ds(0, group.count - 1)]
        return pltpu.make_async_remote_copy(
            src_ref=rest,
            dst_ref=rest,
            send_sem=sum_sems.at[stage, 0],
            recv_sem=sum_sems.at[stage, 1],
            device_id=group.peer(1),
            device_id_type=MESH,
        )

    whole = jnp.sum(rows[...].T, axis=0, keepdims=True)
    for stage, group in enumerate(groups):
        sums[stage][pl.ds(group.slot, 1)] = whole.reshape(1, 1, 128)
        for step in range(1, group.count):
            copy(stage, step).start()
        all_copies(stage).wait_recv()
        whole = jnp.sum(sums[stage][...], axis=0)

    lane2 = lax.broadcasted_iota(jnp.int32, (16, 128), 1)
    sub2 = lax.broadcasted_iota(jnp.int32, (16, 128), 0)
    eye = sub2 == lane2
    whole = jnp.broadcast_to(whole, (16, 128))
    gram = jnp.zeros((16, 128), jnp.float32)
    for k in range(DIM):
        moved = whole if k == 0 else pltpu.roll(whole, (128 - DIM * k) % 128, 1)
        gram = jnp.where(sub2 == k, moved, gram)
    gram = jnp.where(lane2 < DIM, gram, 0.0)

    def down(v):
        return jnp.broadcast_to(jnp.sum(v, axis=0, keepdims=True), (16, 128))

    def turned(v):
        return jnp.broadcast_to(
            jnp.sum(jnp.where(eye, v, 0.0), axis=1, keepdims=True), (16, 128))

    diagonal = jnp.broadcast_to(
        jnp.sum(jnp.where(eye, gram, 0.0), axis=1, keepdims=True), (16, 128))
    lengths = jnp.sqrt(jnp.maximum(diagonal, 0.0))
    start_square = jnp.broadcast_to(diagonal[0:1], (16, 128)) + epsilon
    inverse = lax.rsqrt(start_square)
    beta = start_square * inverse
    up_coef = jnp.zeros((16, 128), jnp.float32)
    down_coef = jnp.zeros((16, 128), jnp.float32)
    for k in range(ITERS):
        up_coef = jnp.where(sub2 == k + 1, HALF if is_first(k) else HALF / 2, up_coef)
        if not is_first(k):
            down_coef = jnp.where(sub2 == k - 1, HALF / 2, down_coef)

    u_lane = jnp.where(lane2 == 0, 1.0, 0.0)
    u_sub = jnp.where(sub2 == 0, 1.0, 0.0)
    gu_lane = jnp.broadcast_to(gram[0:1], (16, 128))
    gu_sub = turned(gu_lane)
    rest_t = jnp.where(eye, 1.0, 0.0)
    gram_rest_t = gram
    images = jnp.zeros((16, 128), jnp.float32)
    coords = []
    trust = jnp.ones((16, 128), jnp.float32)

    cosines, sines, inverse_radii, upper = [], [], [], []
    target = [beta[0:1]]
    for j in range(ITERS):
        image = (CENTER * u_sub + up_coef * pltpu.roll(u_sub, 1, 0)
                 + down_coef * pltpu.roll(u_sub, 15, 0))
        p_lane = down(rest_t * image)
        gp_lane = down(gram_rest_t * image)
        p_sub, gp_sub = turned(p_lane), turned(gp_lane)
        h_sub = turned(down(images * image)) * inverse
        own = down(gu_sub * image) * (inverse * inverse)
        coords.append(u_sub * inverse)
        c_lane, g_sub, g_lane = u_lane * inverse, gu_sub * inverse, gu_lane * inverse
        rest_t = rest_t - g_sub * c_lane
        gram_rest_t = gram_rest_t - g_sub * g_lane
        images = jnp.where(lane2 == j, g_sub, images)
        u_sub, u_lane = (p_sub - u_sub * own) * inverse, (p_lane - u_lane * own) * inverse
        gu_sub, gu_lane = (gp_sub - gu_sub * own) * inverse, (gp_lane - gu_lane * own) * inverse
        square = down(u_sub * gu_sub)
        spread_square = down(jnp.abs(u_sub) * lengths)
        trust = jnp.where(square > TRUST * spread_square * spread_square, trust, 0.0)
        square = jnp.maximum(square, 0.0) + epsilon
        inverse = lax.rsqrt(square)
        entries = ([h_sub[i:i + 1] for i in range(j)] + [own[0:1], (square * inverse)[0:1]])
        for row in range(j):
            entries[row], entries[row + 1] = (
                cosines[row] * entries[row] + sines[row] * entries[row + 1],
                cosines[row] * entries[row + 1] - sines[row] * entries[row])
        inverse_radius = lax.rsqrt(entries[j] * entries[j] + entries[j + 1] * entries[j + 1])
        cosines.append(entries[j] * inverse_radius)
        sines.append(entries[j + 1] * inverse_radius)
        inverse_radii.append(inverse_radius)
        upper.append(entries[:j])
        lead = target[j]
        target[j] = cosines[j] * lead
        target.append(-sines[j] * lead)
    weights = [None] * ITERS
    for row in range(ITERS - 1, -1, -1):
        value = target[row]
        for later in range(ITERS - 1, row, -1):
            value = value - upper[later][row] * weights[later]
        weights[row] = value * inverse_radii[row]
    coef = weights[0] * coords[0]
    for j in range(1, ITERS):
        coef = coef + weights[j] * coords[j]
    plane_out[16:24] = trust[0:8]
    coefs = [jnp.broadcast_to(coef[k:k + 1], (8, 128)) for k in range(ITERS)]

    def combine(b, carry):
        for i in range(8):
            r = b * 8 + i
            value = coefs[0] * vecs[0, r]
            for k in range(1, ITERS):
                value = value + coefs[k] * vecs[k, r]
            tall_out[pl.ds(r, 8, stride=SHELLS), :] = value
        return carry

    lax.fori_loop(0, 8, combine, 0)
    sol = coefs[0] * planes[0, 0:8]
    sol_collector = coefs[0] * planes[0, 8:16]
    for k in range(1, ITERS):
        sol = sol + coefs[k] * planes[k, 0:8]
        sol_collector = sol_collector + coefs[k] * planes[k, 8:16]
    plane_out[0:8] = sol
    plane_out[8:16] = sol_collector

    for turn in range(len(ROUNDS)):
        each_message(turn, lambda block: halo_copy(turn, block).wait_send())
    for stage in range(len(STAGES)):
        all_copies(stage).wait_send()


def results(tall, planes, out_c, out_p, flag):
    for g in range(4):
        block = tall[g * 128:(g + 1) * 128, :].T
        for q in range(4):
            at = (4 * q + g) * 128
            out_c[:, :, at:at + 128] = block[q * 32:(q + 1) * 32].reshape(2, 16, 128)
    flag[0, 0] = jnp.min(planes[16:24])
    sol = planes[0:8]
    by_node = [sol if q == 0 else pltpu.roll(sol, 128 - 32 * q, 1) for q in range(4)]
    by_node = jnp.concatenate(
        by_node + [planes[8:16], jnp.zeros((88, 128), jnp.float32)], axis=0)
    out_p[...] = by_node.T[:CELLS, :CELLS + 1].reshape(2, 16, CELLS + 1)


def fast(nx, ny, *args):
    counts = [members(names, nx, ny) for names in STAGES]
    f32 = jnp.float32
    vmem = pl.BlockSpec(memory_space=pltpu.VMEM)
    tall, planes = pl.pallas_call(
        functools.partial(kernel, nx, ny),
        out_shape=(
            pltpu.VMEM((512, 128), f32),
            pltpu.VMEM((24, 128), f32),
        ),
        in_specs=[pl.BlockSpec(memory_space=pltpu.HBM)] * 5,
        out_specs=(vmem, vmem),
        scratch_shapes=[
            pltpu.VMEM((512, 128), f32),
            pltpu.VMEM((DIM, SHELLS, 8, 128), f32),
            pltpu.VMEM((DIM, 16, 128), f32),
            pltpu.VMEM((len(ROUNDS), 3, OUTBOX, 128), f32),
            pltpu.VMEM((len(ROUNDS), len(BLOCKS), OUTBOX, 128), f32),
            pltpu.VMEM((128, 128), f32),
            *(pltpu.VMEM(a.shape, f32) for a in args),
            pltpu.SemaphoreType.DMA((len(ROUNDS), len(BLOCKS))),
            pltpu.SemaphoreType.DMA((len(ROUNDS), len(BLOCKS))),
            pltpu.SemaphoreType.DMA((5,)),
            *(pltpu.VMEM((count, 1, 128), f32) for count in counts),
            pltpu.SemaphoreType.DMA((len(STAGES), 2)),
        ],
        compiler_params=pltpu.CompilerParams(collective_id=0, has_side_effects=True),
    )(*args)
    return pl.pallas_call(
        results,
        out_shape=(*(jax.ShapeDtypeStruct(a.shape, f32) for a in args[:2]),
                   jax.ShapeDtypeStruct((1, 1), f32)),
        in_specs=[vmem] * 2,
        out_specs=(vmem, vmem, pl.BlockSpec(memory_space=pltpu.SMEM)),
    )(*(pltpu.with_memory_space_constraint(a, pltpu.VMEM) for a in (tall, planes)))


def with_halo(shard, sides, width):
    edges = {}
    for axis, dim in sides:
        size, length = (lax.axis_size(axis), shard.shape[dim])
        up = [(i, (i + 1) % size) for i in range(size - 1)]
        last = lax.slice_in_dim(shard, length - width, length, axis=dim)
        initial = lax.slice_in_dim(shard, 0, width, axis=dim)
        edges[dim] = (
            lax.ppermute(last, axis, up),
            lax.ppermute(initial, axis, [(b, a) for a, b in up]),
        )
    done = []
    for _, dim in sides:
        low, high = edges[dim]
        around = [(width, width) if d in done else (0, 0) for d in range(shard.ndim)]
        shard = jnp.concatenate([jnp.pad(low, around), shard, jnp.pad(high, around)], axis=dim)
        done.append(dim)
    return shard


def total_of(shard):
    return lax.all_gather(shard, ("gx", "gy")).sum(axis=0)


def mirror_laplace(values):
    inner = jnp.concatenate([values[..., :1], values[..., :-1]], axis=-1)
    outer = jnp.concatenate([values[..., 1:], values[..., -1:]], axis=-1)
    return 2.0 * values - inner - outer


def local_operator(conc, padded, diffusion, exchange, slope):
    nodes = exchange.shape[2]
    shell_count = conc.shape[2] // nodes
    shells = conc.reshape(conc.shape[0], conc.shape[1], nodes, shell_count)
    center = padded[1:-1, 1:-1]
    lateral = (
        4.0 * center - padded[2:, 1:-1] - padded[:-2, 1:-1] - padded[1:-1, 2:] - padded[1:-1, :-2]
    )
    node_pot = center[..., :nodes]
    collector = center[..., nodes]
    current = exchange * (node_pot - collector[..., None])
    surface = shells[..., shell_count - 1]
    surface_flag = (lax.broadcasted_iota(jnp.int32, (shell_count,), 0) == shell_count - 1).astype(
        jnp.float32
    )
    new_shells = (
        shells + diffusion[..., None] * mirror_laplace(shells) + current[..., None] * surface_flag
    )
    new_nodes = (
        node_cond * mirror_laplace(node_pot)
        + current
        - slope * surface
        + plane_cond * lateral[..., :nodes]
    )
    new_collector = collector_cond * lateral[..., nodes] - jnp.mean(current, axis=-1)
    return (
        new_shells.reshape(conc.shape),
        jnp.concatenate([new_nodes, new_collector[..., None]], axis=-1),
    )


def step_by_step(rhs_conc, rhs_pots, diffusion, exchange, slope):
    first = jnp.sum(rhs_conc * rhs_conc) + jnp.sum(rhs_pots * rhs_pots)
    start_norm = jnp.sqrt(total_of(first.reshape(1))[0] + epsilon)
    all_conc = jnp.zeros((DIM, *rhs_conc.shape), jnp.float32).at[0].set(rhs_conc / start_norm)
    all_pots = jnp.zeros((DIM, *rhs_pots.shape), jnp.float32).at[0].set(rhs_pots / start_norm)
    matrix = jnp.zeros((DIM, DIM), jnp.float32)

    def arnoldi(step, state):
        all_conc, all_pots, matrix = state
        padded = with_halo(all_pots[step], (("gx", 0), ("gy", 1)), 1)
        image_conc, image_pots = local_operator(all_conc[step], padded, diffusion, exchange, slope)
        local_dots = jnp.sum(all_conc * image_conc, axis=(1, 2, 3)) + jnp.sum(
            all_pots * image_pots, axis=(1, 2, 3))
        coeffs = total_of(local_dots)
        rest_conc = image_conc - jnp.sum(coeffs[:, None, None, None] * all_conc, axis=0)
        rest_pots = image_pots - jnp.sum(coeffs[:, None, None, None] * all_pots, axis=0)
        rest = jnp.sum(rest_conc * rest_conc) + jnp.sum(rest_pots * rest_pots)
        height = jnp.sqrt(total_of(rest.reshape(1))[0] + epsilon)
        column = jnp.where(jnp.arange(DIM) == step + 1, height, coeffs)
        return (
            lax.dynamic_update_index_in_dim(all_conc, rest_conc / height, step + 1, 0),
            lax.dynamic_update_index_in_dim(all_pots, rest_pots / height, step + 1, 0),
            lax.dynamic_update_index_in_dim(matrix, column, step, 0),
        )

    all_conc, all_pots, matrix = lax.fori_loop(
        0, ITERS, arnoldi, (all_conc, all_pots, matrix))

    def rotate(step, state):
        matrix, target = state
        pair = matrix[step]
        lead, under = pair[step], pair[step + 1]
        radius = jnp.sqrt(lead * lead + under * under)
        cosine, sine = lead / radius, under / radius

        def turn(values):
            a = lax.dynamic_index_in_dim(values, step, values.ndim - 1)
            b = lax.dynamic_index_in_dim(values, step + 1, values.ndim - 1)
            values = lax.dynamic_update_slice_in_dim(
                values, cosine * a + sine * b, step, values.ndim - 1)
            return lax.dynamic_update_slice_in_dim(
                values, cosine * b - sine * a, step + 1, values.ndim - 1)

        return turn(matrix), turn(target)

    target = jnp.zeros((DIM,), jnp.float32).at[0].set(start_norm)
    matrix, target = lax.fori_loop(0, ITERS, rotate, (matrix, target))

    def back(i, weights):
        row = ITERS - 1 - i
        known = jnp.sum(matrix[:, row] * weights)
        return weights.at[row].set((target[row] - known) / matrix[row, row])

    weights = lax.fori_loop(0, ITERS, back, jnp.zeros((DIM,), jnp.float32))
    weights = weights[:, None, None, None]
    return jnp.sum(weights * all_conc, axis=0), jnp.sum(weights * all_pots, axis=0)


def solution(mesh):
    nx, ny = mesh.shape["gx"], mesh.shape["gy"]

    def shards(*args):
        conc, pots, flag = fast(nx, ny, *args)

        def again(state):
            conc, pots = step_by_step(*args)
            return conc, pots, jnp.ones_like(state[2])

        return lax.while_loop(
            lambda state: state[2] < 0.5, again, (conc, pots, flag[0, 0]))[:2]

    spec = P("gx", "gy", None)
    return jax.shard_map(
        shards, mesh=mesh, in_specs=(spec,) * 5, out_specs=(spec,) * 2, check_vma=False)
```

```python
import functools
import jax
import jax.numpy as jnp
from jax import lax
from jax.experimental import pallas as pl
from jax.experimental.pallas import tpu as pltpu
from jax.sharding import Mesh
from jax.sharding import PartitionSpec as P

ITERS = 10
MESH = pl.DeviceIdType.MESH
GX = ("gx_0", "gx_1", "gx_2")

node_cond = 1.0
plane_cond = 0.5
collector_cond = 2.0
epsilon = 1e-06

ROUNDS = (5, 5)
CENTER = 11.0
HALF = 10.0
TRUST = 4e-4

CELLS = 32
SHELLS = 64
DIM = ITERS + 1
STARTS = tuple(sum(ROUNDS[:i]) for i in range(len(ROUNDS)))


def steps_away(block):
    a, b = block
    return max(2 * abs(a) - 1, 0) + abs(b)


DEEPEST = max(ROUNDS)
BLOCKS = sorted(
    ((a, b) for a in range(-DEEPEST, DEEPEST + 1) for b in (-1, 0, 1)
     if 0 < steps_away((a, b)) <= DEEPEST),
    key=lambda block: (-steps_away(block), block))
SLOT = {block: i for i, block in enumerate(BLOCKS)}
COEFS = 24
OUTBOX = 16 + COEFS + 8 * (DEEPEST - 1)


def message_rows(turn, block):
    updates = ROUNDS[turn] - steps_away(block)
    if updates < 0:
        return 0
    if block[1]:
        return 8 * len(fields_of(turn, updates))
    if updates == 0:
        return 16
    return 16 + (COEFS if turn == 0 else 0) + 8 * updates


MIDDLE = 3
assert max(abs(a) for a, _ in BLOCKS) <= MIDDLE
WIDE = 5
assert DEEPEST <= WIDE


def fields_of(turn, updates):
    names = ["pots"]
    if updates and turn == 0:
        names.append("coefs")
    if updates > 1:
        names.append("shells")
    return names


STAGES = ("core", "z", "plane")


def members(name, nx, ny):
    return {"core": 2, "z": ny, "plane": nx // 2}[name]


class Group:
    def __init__(self, name, nx, ny, gx, gy):
        self.name, self.gx, self.gy = name, gx, gy
        self.core, self.plane = lax.rem(gx, 2), lax.div(gx, 2)
        self.count = members(name, nx, ny)
        self.slot = {"core": self.core, "z": gy, "plane": self.plane}[name]

    def peer(self, step):
        if self.count == 2:
            other = 1 - self.slot
        else:
            other = self.slot + step
            other = jnp.where(other >= self.count, other - self.count, other)
        if self.name == "core":
            return 2 * self.plane + other, self.gy
        if self.name == "z":
            return self.gx, other
        return 2 * other + self.core, self.gy


def is_first(k):
    return k in STARTS


def kernel(nx, ny, conc_in, pots_in, diff_in, exch_in, slope_in, tall_out, plane_out,
           tall, vecs, planes, outbox, halo, rows, conc, pots, diff, exch, slope, hs_sem, hr_sem, in_sem,
           *for_sums):
    *sums, sum_sems = for_sums
    loads = [
        pltpu.make_async_copy(source, target, in_sem.at[i])
        for i, (source, target) in enumerate((
            (conc_in, conc), (diff_in, diff), (exch_in, exch), (slope_in, slope), (pots_in, pots)))]
    for load in loads:
        load.start()

    gx = lax.axis_index("gx")
    gy = lax.axis_index("gy")
    groups = [Group(names, nx, ny, gx, gy) for names in STAGES]

    exists = {}
    for a, b in BLOCKS:
        inside = []
        if a:
            inside.append(gx + a < nx if a > 0 else gx + a >= 0)
        if b:
            inside.append(gy + b < ny if b > 0 else gy + b >= 0)
        exists[a, b] = inside[0] if len(inside) == 1 else jnp.logical_and(*inside)

    barrier = pltpu.get_barrier_semaphore()
    expected = 0
    for group in groups:
        for step in range(1, group.count):
            pl.semaphore_signal(
                barrier, inc=1, device_id=group.peer(step), device_id_type=MESH)
        expected = expected + group.count - 1
    for block in BLOCKS:
        @pl.when(exists[block])
        def _(block=block):
            pl.semaphore_signal(
                barrier, inc=1, device_id=(gx + block[0], gy + block[1]), device_id_type=MESH)
        expected = expected + exists[block].astype(jnp.int32)

    lane = lax.broadcasted_iota(jnp.int32, (8, 128), 1)
    sub = lax.broadcasted_iota(jnp.int32, (8, 128), 0)
    quarter = lane // 32
    x_of = (lane // 16) % 2
    y_of = lane % 16
    once = jnp.logical_and(sub == 0, quarter == 0)
    zero = jnp.zeros((8, 128), jnp.float32)

    for block in BLOCKS:
        @pl.when(jnp.logical_not(exists[block]))
        def _(block=block):
            for turn in range(len(ROUNDS)):
                count = message_rows(turn, block)
                if count:
                    halo[turn, SLOT[block], 0:count] = jnp.zeros((count, 128), jnp.float32)

    def spread(by_node):
        parts = [by_node[8 * q:8 * q + 8, :] for q in range(4)]
        return jnp.concatenate(parts, axis=1)

    def small(ref):
        return spread(ref[...].reshape(CELLS, CELLS).T)

    for load in loads:
        load.wait()
    diffusion = small(diff)
    exchange = small(exch)
    slopes = small(slope)
    pots_t = pots[...].reshape(CELLS, CELLS + 1).T
    pot = spread(pots_t[:CELLS])
    collector = jnp.broadcast_to(
        jnp.concatenate([pots_t[CELLS:CELLS + 1]] * 4, axis=1), (8, 128))
    planes[0, 0:8] = pot
    planes[0, 8:16] = collector
    rows[...] = jnp.zeros((128, 128), jnp.float32)

    flat = conc[...].reshape(CELLS, 2048)
    for g in range(4):
        block = jnp.concatenate(
            [flat[:, (4 * q + g) * 128:(4 * q + g + 1) * 128] for q in range(4)], axis=0)
        tall[g * 128:(g + 1) * 128, :] = block.T

    def pack(fields, side):
        start = 16 - WIDE if side == 1 else 0
        packed = zero
        for i, field in enumerate(fields):
            shift = (WIDE * i - start) % 128
            moved = pltpu.roll(field, shift, 1) if shift else field
            packed = jnp.where(jnp.logical_and(y_of >= WIDE * i, y_of < WIDE * (i + 1)), moved, packed)
        return packed

    def unpack(packed, i, side):
        start = 16 - WIDE if side == 1 else 0
        shift = (start - WIDE * i) % 128
        return pltpu.roll(packed, shift, 1) if shift else packed

    def fill_outbox(turn, pot, collector, shells, coefs):
        for i, field in enumerate([pot, collector] + coefs + shells):
            outbox[turn, 0, 8 * i:8 * i + 8] = field
        for side in (1, -1):
            fields = [pack([pot, collector] + shells[:1], side)]
            if coefs:
                fields.append(pack(coefs, side))
            if len(shells) > 1:
                fields.append(pack(shells[1:], side))
            for i, field in enumerate(fields):
                outbox[turn, side % 3, 8 * i:8 * i + 8] = field

    fill_outbox(0, pot, collector,
                [tall[pl.ds(SHELLS - 1 - i, 8, stride=SHELLS), :] for i in range(ROUNDS[0] - 1)],
                [exchange, slopes, diffusion])

    def first(b, acc):
        for i in range(8):
            r = b * 8 + i
            shell = tall[pl.ds(r, 8, stride=SHELLS), :]
            vecs[0, r] = shell
            acc = acc + shell * shell
        return acc

    def keep(k, i, acc):
        total = jnp.sum(acc, axis=0, keepdims=True)
        rows[DIM * k + i:DIM * k + i + 1, :] = total
        if i != k:
            rows[DIM * i + k:DIM * i + k + 1, :] = total

    def halo_copy(turn, block):
        a, b = block
        count = message_rows(turn, block)
        return pltpu.make_async_remote_copy(
            src_ref=outbox.at[turn, b % 3, pl.ds(0, count)],
            dst_ref=halo.at[turn, SLOT[-a, -b], pl.ds(0, count)],
            send_sem=hs_sem.at[turn, SLOT[block]],
            recv_sem=hr_sem.at[turn, SLOT[-a, -b]],
            device_id=(gx + a, gy + b),
            device_id_type=MESH,
        )

    def each_message(turn, act):
        for block in BLOCKS:
            if message_rows(turn, block):
                @pl.when(exists[block])
                def _(block=block):
                    act(block)

    def receive(turn, block):
        a, b = block
        count = message_rows(turn, block)
        pltpu.make_async_remote_copy(
            src_ref=outbox.at[turn, b % 3, pl.ds(0, count)],
            dst_ref=halo.at[turn, SLOT[block], pl.ds(0, count)],
            send_sem=hs_sem.at[turn, SLOT[block]],
            recv_sem=hr_sem.at[turn, SLOT[block]],
            device_id=(gx + a, gy + b),
            device_id_type=MESH,
        ).wait_recv()

    def send_round(turn):
        each_message(turn, lambda block: halo_copy(turn, block).start())

    pl.semaphore_wait(barrier, expected)
    send_round(0)
    acc = lax.fori_loop(0, 8, first, zero)
    keep(0, 0, acc + pot * pot + jnp.where(once, collector * collector, 0.0))

    def around(own, low_x, high_x, low_y, high_y):
        high = own if high_x is None else own + high_x
        low = own if low_x is None else own + low_x
        before = 0.0 if low_y is None else pltpu.roll(low_y, 113, 1)
        after = 0.0 if high_y is None else pltpu.roll(high_y, 15, 1)
        return (jnp.where(x_of == 1, pltpu.roll(high, 16, 1), pltpu.roll(low, 112, 1))
                + jnp.where(y_of > 0, pltpu.roll(own, 1, 1), before)
                + jnp.where(y_of < 15, pltpu.roll(own, 127, 1), after))

    def node_mirror(v):
        down = pltpu.roll(v, 1, 0)
        down = jnp.where(sub == 0, pltpu.roll(down, 32, 1), down)
        down = jnp.where(jnp.logical_and(sub == 0, quarter == 0), v, down)
        up = pltpu.roll(v, 7, 0)
        up = jnp.where(sub == 7, pltpu.roll(up, 96, 1), up)
        up = jnp.where(jnp.logical_and(sub == 7, quarter == 3), v, up)
        return 2.0 * v - down - up

    def over_quarters(v):
        return (v + pltpu.roll(v, 32, 1)) + (pltpu.roll(v, 64, 1) + pltpu.roll(v, 96, 1))

    def placed(block):
        return sub == block[0] + MIDDLE

    inside = {}
    for b in (-1, 0, 1):
        inside[b] = jnp.where(placed((0, b)), 1.0, 0.0) if b == 0 else zero
        for block in BLOCKS:
            if block[1] == b:
                inside[b] = jnp.where(
                    jnp.logical_and(placed(block), exists[block]), 1.0, inside[b])

    def potentials(turn, beside_step):
        depth, start = ROUNDS[turn], STARTS[turn]
        carried = ROUNDS[turn + 1] - 1 if turn + 1 < len(ROUNDS) else 0
        own = (0, 0)
        now = {own: (planes[start, 0:8],
                     [vecs[start, SHELLS - 1 - i] for i in range(depth + carried)])}
        coefs = {own: (exchange, slopes, diffusion)}
        fields = {-1: zero, 0: jnp.where(placed(own), planes[start, 8:16], 0.0), 1: zero}
        for block in BLOCKS:
            if message_rows(turn, block) == 0:
                continue
            updates = depth - steps_away(block)
            inbox = halo.at[turn, SLOT[block]]
            a, b = block
            if b:
                names = fields_of(turn, updates)
                found = {name: inbox[8 * i:8 * i + 8] for i, name in enumerate(names)}
                fields[b] = jnp.where(placed(block), found["pots"], fields[b])
                shells = [unpack(found["pots"], 2, -b)] if updates else []
                shells += [unpack(found["shells"], i, -b) for i in range(updates - 1)]
                now[block] = (unpack(found["pots"], 0, -b), shells)
                if updates:
                    source = halo[0, SLOT[block], 8:16]
                    coefs[block] = tuple(unpack(source, i, -b) for i in range(3))
                continue
            shells_at = 16 + (COEFS if turn == 0 else 0)
            fields[0] = jnp.where(placed(block), inbox[8:16], fields[0])
            now[block] = (inbox[0:8],
                          [inbox[shells_at + 8 * i:shells_at + 8 * i + 8] for i in range(updates)])
            if updates:
                source = halo.at[0, SLOT[block]]
                coefs[block] = (source[16:24], source[24:32], source[32:40])
        for b in (-1, 1):
            fields[b] = unpack(fields[b], 1, -b)
        before = fields_before = None
        for m in range(1, depth + 1):
            scale = (1.0 if m == 1 else 2.0) / HALF
            after, fields_after = {}, {}
            means = {-1: zero, 0: zero, 1: zero}
            for block in now:
                if steps_away(block) > depth - m:
                    continue
                a, b = block
                pot, shells = now[block]
                exchange_of, slope_of, diffusion_of = coefs[block]
                beside = [now.get(other) for other in (
                    (a - 1, b), (a + 1, b), (a, b - 1), (a, b + 1))]
                collector = jnp.broadcast_to(fields[b][a + MIDDLE:a + MIDDLE + 1], (8, 128))
                current = exchange_of * (pot - collector)
                means[b] = jnp.where(
                    placed(block),
                    jnp.broadcast_to(jnp.sum(current, axis=0, keepdims=True), (8, 128)), means[b])
                lateral = 4.0 * pot - around(
                    pot, *(None if other is None else other[0] for other in beside))
                new_pot = scale * (
                    node_cond * node_mirror(pot) + current - slope_of * shells[0]
                    + plane_cond * lateral - CENTER * pot)
                count = depth - m + carried if block == own else depth - steps_away(block) - m
                center_coef = scale * (1.0 - CENTER + 2.0 * diffusion_of)
                side_coef = scale * diffusion_of
                new_shells = []
                for i in range(count):
                    new = center_coef * shells[i] - side_coef * (shells[max(i - 1, 0)] + shells[i + 1])
                    if i == 0:
                        new = new + scale * current
                    if m > 1:
                        new = new - before[block][1][i]
                    new_shells.append(new)
                if m > 1:
                    new_pot = new_pot - before[block][0]
                if block != own:
                    new_pot = jnp.where(exists[block], new_pot, 0.0)
                after[block] = (new_pot, new_shells)
            for b in (-1, 0, 1):
                if m + abs(b) > depth:
                    fields_after[b] = zero
                    continue
                field = fields[b]
                lateral = 4.0 * field - around(
                    field, pltpu.roll(field, 1, 0), pltpu.roll(field, 7, 0),
                    fields.get(b - 1), fields.get(b + 1))
                new = scale * (collector_cond * lateral
                               - over_quarters(means[b]) * (1.0 / 32.0) - CENTER * field)
                if m > 1:
                    new = new - fields_before[b]
                fields_after[b] = jnp.where(inside[b] > 0.0, new, 0.0)
            planes[start + m, 0:8] = after[own][0]
            planes[start + m, 8:16] = jnp.broadcast_to(
                fields_after[0][MIDDLE:MIDDLE + 1], (8, 128))
            before, now = now, after
            fields_before, fields = fields, fields_after
            beside_step(start + m)
        if turn + 1 < len(ROUNDS):
            fill_outbox(turn + 1, now[own][0], planes[start + depth, 8:16], now[own][1], [])


    def bulk_shells(k, unrolled=False):
        scale = (1.0 if is_first(k) else 2.0) / HALF
        current = exchange * (planes[k, 0:8] - planes[k, 8:16])
        center_coef = scale * (1.0 - CENTER + 2.0 * diffusion)
        side_coef = scale * diffusion

        def shells(base, accs, last):
            accs = list(accs)
            low = vecs[k, max(base - 1, 0) if isinstance(base, int) else jnp.maximum(base - 1, 0)]
            here = vecs[k, base]
            for i in range(8):
                r = base + i
                high = here if last and i == 7 else vecs[k, r + 1]
                new = center_coef * here - side_coef * (low + high)
                if last and i == 7:
                    new = new + scale * current
                if not is_first(k):
                    new = new - vecs[k - 1, r]
                vecs[k + 1, r] = new
                for m in range(k):
                    accs[m] = accs[m] + new * vecs[m, r]
                accs[k] = accs[k] + new * here
                accs[k + 1] = accs[k + 1] + new * new
                low, here = here, high
            return tuple(accs)

        accs = (zero,) * (k + 2)
        if unrolled:
            for b in range(7):
                accs = shells(b * 8, accs, False)
        else:
            accs = lax.fori_loop(0, 7, lambda b, accs: shells(b * 8, accs, False), accs)
        return shells(SHELLS - 8, accs, True)

    def products(k, accs):
        new_pot, new_collector = planes[k + 1, 0:8], planes[k + 1, 8:16]
        for m in range(k + 2):
            acc = accs[m] + new_pot * planes[m, 0:8] + jnp.where(
                once, new_collector * planes[m, 8:16], 0.0)
            keep(k + 1, m, acc)

    for turn, start in enumerate(STARTS):
        end = start + ROUNDS[turn]
        accs = {start: bulk_shells(start)}
        each_message(turn, functools.partial(receive, turn))
        if turn + 1 < len(ROUNDS):
            potentials(turn, lambda k: None)
            send_round(turn + 1)
            for k in range(start + 1, end):
                accs[k] = bulk_shells(k)
        else:
            def beside(k):
                if k < end:
                    accs[k] = bulk_shells(k, True)

            potentials(turn, beside)
        for k in range(start, end):
            products(k, accs[k])

    def copy(stage, step):
        group = groups[stage]
        return pltpu.make_async_remote_copy(
            src_ref=sums[stage].at[group.slot],
            dst_ref=sums[stage].at[group.slot],
            send_sem=sum_sems.at[stage, 0],
            recv_sem=sum_sems.at[stage, 1],
            device_id=group.peer(step),
            device_id_type=MESH,
        )

    def all_copies(stage):
        group = groups[stage]
        rest = sums[stage].at[pl.ds(0, group.count - 1)]
        return pltpu.make_async_remote_copy(
            src_ref=rest,
            dst_ref=rest,
            send_sem=sum_sems.at[stage, 0],
            recv_sem=sum_sems.at[stage, 1],
            device_id=group.peer(1),
            device_id_type=MESH,
        )

    whole = jnp.sum(rows[...].T, axis=0, keepdims=True)
    for stage, group in enumerate(groups):
        sums[stage][pl.ds(group.slot, 1)] = whole.reshape(1, 1, 128)
        for step in range(1, group.count):
            copy(stage, step).start()
        all_copies(stage).wait_recv()
        whole = jnp.sum(sums[stage][...], axis=0)

    lane2 = lax.broadcasted_iota(jnp.int32, (16, 128), 1)
    sub2 = lax.broadcasted_iota(jnp.int32, (16, 128), 0)
    eye = sub2 == lane2
    whole = jnp.broadcast_to(whole, (16, 128))
    gram = jnp.zeros((16, 128), jnp.float32)
    for k in range(DIM):
        moved = whole if k == 0 else pltpu.roll(whole, (128 - DIM * k) % 128, 1)
        gram = jnp.where(sub2 == k, moved, gram)
    gram = jnp.where(lane2 < DIM, gram, 0.0)

    def down(v):
        return jnp.broadcast_to(jnp.sum(v, axis=0, keepdims=True), (16, 128))

    def turned(v):
        return jnp.broadcast_to(
            jnp.sum(jnp.where(eye, v, 0.0), axis=1, keepdims=True), (16, 128))

    diagonal = jnp.broadcast_to(
        jnp.sum(jnp.where(eye, gram, 0.0), axis=1, keepdims=True), (16, 128))
    lengths = jnp.sqrt(jnp.maximum(diagonal, 0.0))
    start_square = jnp.broadcast_to(diagonal[0:1], (16, 128)) + epsilon
    inverse = lax.rsqrt(start_square)
    beta = start_square * inverse
    up_coef = jnp.zeros((16, 128), jnp.float32)
    down_coef = jnp.zeros((16, 128), jnp.float32)
    for k in range(ITERS):
        up_coef = jnp.where(sub2 == k + 1, HALF if is_first(k) else HALF / 2, up_coef)
        if not is_first(k):
            down_coef = jnp.where(sub2 == k - 1, HALF / 2, down_coef)

    u_lane = jnp.where(lane2 == 0, 1.0, 0.0)
    u_sub = jnp.where(sub2 == 0, 1.0, 0.0)
    gu_lane = jnp.broadcast_to(gram[0:1], (16, 128))
    gu_sub = turned(gu_lane)
    rest_t = jnp.where(eye, 1.0, 0.0)
    gram_rest_t = gram
    images = jnp.zeros((16, 128), jnp.float32)
    coords = []
    trust = jnp.ones((16, 128), jnp.float32)

    cosines, sines, inverse_radii, upper = [], [], [], []
    target = [beta[0:1]]
    for j in range(ITERS):
        image = (CENTER * u_sub + up_coef * pltpu.roll(u_sub, 1, 0)
                 + down_coef * pltpu.roll(u_sub, 15, 0))
        p_lane = down(rest_t * image)
        gp_lane = down(gram_rest_t * image)
        p_sub, gp_sub = turned(p_lane), turned(gp_lane)
        h_sub = turned(down(images * image)) * inverse
        own = down(gu_sub * image) * (inverse * inverse)
        coords.append(u_sub * inverse)
        c_lane, g_sub, g_lane = u_lane * inverse, gu_sub * inverse, gu_lane * inverse
        rest_t = rest_t - g_sub * c_lane
        gram_rest_t = gram_rest_t - g_sub * g_lane
        images = jnp.where(lane2 == j, g_sub, images)
        u_sub, u_lane = (p_sub - u_sub * own) * inverse, (p_lane - u_lane * own) * inverse
        gu_sub, gu_lane = (gp_sub - gu_sub * own) * inverse, (gp_lane - gu_lane * own) * inverse
        square = down(u_sub * gu_sub)
        spread_square = down(jnp.abs(u_sub) * lengths)
        trust = jnp.where(square > TRUST * spread_square * spread_square, trust, 0.0)
        square = jnp.maximum(square, 0.0) + epsilon
        inverse = lax.rsqrt(square)
        entries = ([h_sub[i:i + 1] for i in range(j)] + [own[0:1], (square * inverse)[0:1]])
        for row in range(j):
            entries[row], entries[row + 1] = (
                cosines[row] * entries[row] + sines[row] * entries[row + 1],
                cosines[row] * entries[row + 1] - sines[row] * entries[row])
        inverse_radius = lax.rsqrt(entries[j] * entries[j] + entries[j + 1] * entries[j + 1])
        cosines.append(entries[j] * inverse_radius)
        sines.append(entries[j + 1] * inverse_radius)
        inverse_radii.append(inverse_radius)
        upper.append(entries[:j])
        lead = target[j]
        target[j] = cosines[j] * lead
        target.append(-sines[j] * lead)
    weights = [None] * ITERS
    for row in range(ITERS - 1, -1, -1):
        value = target[row]
        for later in range(ITERS - 1, row, -1):
            value = value - upper[later][row] * weights[later]
        weights[row] = value * inverse_radii[row]
    coef = weights[0] * coords[0]
    for j in range(1, ITERS):
        coef = coef + weights[j] * coords[j]
    plane_out[16:24] = trust[0:8]
    coefs = [jnp.broadcast_to(coef[k:k + 1], (8, 128)) for k in range(ITERS)]

    def combine(b, carry):
        for i in range(8):
            r = b * 8 + i
            value = coefs[0] * vecs[0, r]
            for k in range(1, ITERS):
                value = value + coefs[k] * vecs[k, r]
            tall_out[pl.ds(r, 8, stride=SHELLS), :] = value
        return carry

    lax.fori_loop(0, 8, combine, 0)
    sol = coefs[0] * planes[0, 0:8]
    sol_collector = coefs[0] * planes[0, 8:16]
    for k in range(1, ITERS):
        sol = sol + coefs[k] * planes[k, 0:8]
        sol_collector = sol_collector + coefs[k] * planes[k, 8:16]
    plane_out[0:8] = sol
    plane_out[8:16] = sol_collector

    for turn in range(len(ROUNDS)):
        each_message(turn, lambda block: halo_copy(turn, block).wait_send())
    for stage in range(len(STAGES)):
        all_copies(stage).wait_send()


def results(tall, planes, out_c, out_p, flag):
    for g in range(4):
        block = tall[g * 128:(g + 1) * 128, :].T
        for q in range(4):
            at = (4 * q + g) * 128
            out_c[:, :, at:at + 128] = block[q * 32:(q + 1) * 32].reshape(2, 16, 128)
    flag[0, 0] = jnp.min(planes[16:24])
    sol = planes[0:8]
    by_node = [sol if q == 0 else pltpu.roll(sol, 128 - 32 * q, 1) for q in range(4)]
    by_node = jnp.concatenate(
        by_node + [planes[8:16], jnp.zeros((88, 128), jnp.float32)], axis=0)
    out_p[...] = by_node.T[:CELLS, :CELLS + 1].reshape(2, 16, CELLS + 1)


def fast(nx, ny, *args):
    counts = [members(names, nx, ny) for names in STAGES]
    f32 = jnp.float32
    vmem = pl.BlockSpec(memory_space=pltpu.VMEM)
    tall, planes = pl.pallas_call(
        functools.partial(kernel, nx, ny),
        out_shape=(
            pltpu.VMEM((512, 128), f32),
            pltpu.VMEM((24, 128), f32),
        ),
        in_specs=[pl.BlockSpec(memory_space=pltpu.HBM)] * 5,
        out_specs=(vmem, vmem),
        scratch_shapes=[
            pltpu.VMEM((512, 128), f32),
            pltpu.VMEM((DIM, SHELLS, 8, 128), f32),
            pltpu.VMEM((DIM, 16, 128), f32),
            pltpu.VMEM((len(ROUNDS), 3, OUTBOX, 128), f32),
            pltpu.VMEM((len(ROUNDS), len(BLOCKS), OUTBOX, 128), f32),
            pltpu.VMEM((128, 128), f32),
            *(pltpu.VMEM(a.shape, f32) for a in args),
            pltpu.SemaphoreType.DMA((len(ROUNDS), len(BLOCKS))),
            pltpu.SemaphoreType.DMA((len(ROUNDS), len(BLOCKS))),
            pltpu.SemaphoreType.DMA((5,)),
            *(pltpu.VMEM((count, 1, 128), f32) for count in counts),
            pltpu.SemaphoreType.DMA((len(STAGES), 2)),
        ],
        compiler_params=pltpu.CompilerParams(collective_id=0, has_side_effects=True),
    )(*args)
    return pl.pallas_call(
        results,
        out_shape=(*(jax.ShapeDtypeStruct(a.shape, f32) for a in args[:2]),
                   jax.ShapeDtypeStruct((1, 1), f32)),
        in_specs=[vmem] * 2,
        out_specs=(vmem, vmem, pl.BlockSpec(memory_space=pltpu.SMEM)),
    )(*(pltpu.with_memory_space_constraint(a, pltpu.VMEM) for a in (tall, planes)))


def with_halo(shard, sides, width):
    edges = {}
    for axis, dim in sides:
        size, length = (lax.axis_size(axis), shard.shape[dim])
        up = [(i, (i + 1) % size) for i in range(size - 1)]
        last = lax.slice_in_dim(shard, length - width, length, axis=dim)
        initial = lax.slice_in_dim(shard, 0, width, axis=dim)
        edges[dim] = (
            lax.ppermute(last, axis, up),
            lax.ppermute(initial, axis, [(b, a) for a, b in up]),
        )
    done = []
    for _, dim in sides:
        low, high = edges[dim]
        around = [(width, width) if d in done else (0, 0) for d in range(shard.ndim)]
        shard = jnp.concatenate([jnp.pad(low, around), shard, jnp.pad(high, around)], axis=dim)
        done.append(dim)
    return shard


def total_of(shard):
    return lax.all_gather(shard, ("gx", "gy")).sum(axis=0)


def mirror_laplace(values):
    inner = jnp.concatenate([values[..., :1], values[..., :-1]], axis=-1)
    outer = jnp.concatenate([values[..., 1:], values[..., -1:]], axis=-1)
    return 2.0 * values - inner - outer


def local_operator(conc, padded, diffusion, exchange, slope):
    nodes = exchange.shape[2]
    shell_count = conc.shape[2] // nodes
    shells = conc.reshape(conc.shape[0], conc.shape[1], nodes, shell_count)
    center = padded[1:-1, 1:-1]
    lateral = (
        4.0 * center - padded[2:, 1:-1] - padded[:-2, 1:-1] - padded[1:-1, 2:] - padded[1:-1, :-2]
    )
    node_pot = center[..., :nodes]
    collector = center[..., nodes]
    current = exchange * (node_pot - collector[..., None])
    surface = shells[..., shell_count - 1]
    surface_flag = (lax.broadcasted_iota(jnp.int32, (shell_count,), 0) == shell_count - 1).astype(
        jnp.float32
    )
    new_shells = (
        shells + diffusion[..., None] * mirror_laplace(shells) + current[..., None] * surface_flag
    )
    new_nodes = (
        node_cond * mirror_laplace(node_pot)
        + current
        - slope * surface
        + plane_cond * lateral[..., :nodes]
    )
    new_collector = collector_cond * lateral[..., nodes] - jnp.mean(current, axis=-1)
    return (
        new_shells.reshape(conc.shape),
        jnp.concatenate([new_nodes, new_collector[..., None]], axis=-1),
    )


def step_by_step(rhs_conc, rhs_pots, diffusion, exchange, slope):
    first = jnp.sum(rhs_conc * rhs_conc) + jnp.sum(rhs_pots * rhs_pots)
    start_norm = jnp.sqrt(total_of(first.reshape(1))[0] + epsilon)
    all_conc = jnp.zeros((DIM, *rhs_conc.shape), jnp.float32).at[0].set(rhs_conc / start_norm)
    all_pots = jnp.zeros((DIM, *rhs_pots.shape), jnp.float32).at[0].set(rhs_pots / start_norm)
    matrix = jnp.zeros((DIM, DIM), jnp.float32)

    def arnoldi(step, state):
        all_conc, all_pots, matrix = state
        padded = with_halo(all_pots[step], (("gx", 0), ("gy", 1)), 1)
        image_conc, image_pots = local_operator(all_conc[step], padded, diffusion, exchange, slope)
        local_dots = jnp.sum(all_conc * image_conc, axis=(1, 2, 3)) + jnp.sum(
            all_pots * image_pots, axis=(1, 2, 3))
        coeffs = total_of(local_dots)
        rest_conc = image_conc - jnp.sum(coeffs[:, None, None, None] * all_conc, axis=0)
        rest_pots = image_pots - jnp.sum(coeffs[:, None, None, None] * all_pots, axis=0)
        rest = jnp.sum(rest_conc * rest_conc) + jnp.sum(rest_pots * rest_pots)
        height = jnp.sqrt(total_of(rest.reshape(1))[0] + epsilon)
        column = jnp.where(jnp.arange(DIM) == step + 1, height, coeffs)
        return (
            lax.dynamic_update_index_in_dim(all_conc, rest_conc / height, step + 1, 0),
            lax.dynamic_update_index_in_dim(all_pots, rest_pots / height, step + 1, 0),
            lax.dynamic_update_index_in_dim(matrix, column, step, 0),
        )

    all_conc, all_pots, matrix = lax.fori_loop(
        0, ITERS, arnoldi, (all_conc, all_pots, matrix))

    def rotate(step, state):
        matrix, target = state
        pair = matrix[step]
        lead, under = pair[step], pair[step + 1]
        radius = jnp.sqrt(lead * lead + under * under)
        cosine, sine = lead / radius, under / radius

        def turn(values):
            a = lax.dynamic_index_in_dim(values, step, values.ndim - 1)
            b = lax.dynamic_index_in_dim(values, step + 1, values.ndim - 1)
            values = lax.dynamic_update_slice_in_dim(
                values, cosine * a + sine * b, step, values.ndim - 1)
            return lax.dynamic_update_slice_in_dim(
                values, cosine * b - sine * a, step + 1, values.ndim - 1)

        return turn(matrix), turn(target)

    target = jnp.zeros((DIM,), jnp.float32).at[0].set(start_norm)
    matrix, target = lax.fori_loop(0, ITERS, rotate, (matrix, target))

    def back(i, weights):
        row = ITERS - 1 - i
        known = jnp.sum(matrix[:, row] * weights)
        return weights.at[row].set((target[row] - known) / matrix[row, row])

    weights = lax.fori_loop(0, ITERS, back, jnp.zeros((DIM,), jnp.float32))
    weights = weights[:, None, None, None]
    return jnp.sum(weights * all_conc, axis=0), jnp.sum(weights * all_pots, axis=0)


def solution(mesh):
    nx, ny = mesh.shape["gx"], mesh.shape["gy"]

    def shards(*args):
        conc, pots, flag = fast(nx, ny, *args)

        def again(state):
            conc, pots = step_by_step(*args)
            return conc, pots, jnp.ones_like(state[2])

        return lax.while_loop(
            lambda state: state[2] < 0.5, again, (conc, pots, flag[0, 0]))[:2]

    spec = P("gx", "gy", None)
    return jax.shard_map(
        shards, mesh=mesh, in_specs=(spec,) * 5, out_specs=(spec,) * 2, check_vma=False)
```

```python
import functools
import jax
import jax.numpy as jnp
from jax import lax
from jax.experimental import pallas as pl
from jax.experimental.pallas import tpu as pltpu
from jax.sharding import Mesh
from jax.sharding import PartitionSpec as P

ITERS = 10
MESH = pl.DeviceIdType.MESH
GX = ("gx_0", "gx_1", "gx_2")

node_cond = 1.0
plane_cond = 0.5
collector_cond = 2.0
epsilon = 1e-06

ROUNDS = (5, 5)
CENTER = 11.0
HALF = 10.0
TRUST = 4e-4

CELLS = 32
SHELLS = 64
DIM = ITERS + 1
STARTS = tuple(sum(ROUNDS[:i]) for i in range(len(ROUNDS)))


def steps_away(block):
    a, b = block
    return max(2 * abs(a) - 1, 0) + abs(b)


DEEPEST = max(ROUNDS)
BLOCKS = sorted(
    ((a, b) for a in range(-DEEPEST, DEEPEST + 1) for b in (-1, 0, 1)
     if 0 < steps_away((a, b)) <= DEEPEST),
    key=lambda block: (-steps_away(block), block))
SLOT = {block: i for i, block in enumerate(BLOCKS)}
COEFS = 24
OUTBOX = 16 + COEFS + 8 * (DEEPEST - 1)


def message_rows(turn, block):
    updates = ROUNDS[turn] - steps_away(block)
    if updates < 0:
        return 0
    if block[1]:
        return 8 * len(fields_of(turn, updates))
    if updates == 0:
        return 16
    return 16 + (COEFS if turn == 0 else 0) + 8 * updates


MIDDLE = 3
assert max(abs(a) for a, _ in BLOCKS) <= MIDDLE
WIDE = 5
assert DEEPEST <= WIDE


def fields_of(turn, updates):
    names = ["pots"]
    if updates and turn == 0:
        names.append("coefs")
    if updates > 1:
        names.append("shells")
    return names


STAGES = ("core", "z", "plane")


def members(name, nx, ny):
    return {"core": 2, "z": ny, "plane": nx // 2}[name]


class Group:
    def __init__(self, name, nx, ny, gx, gy):
        self.name, self.gx, self.gy = name, gx, gy
        self.core, self.plane = lax.rem(gx, 2), lax.div(gx, 2)
        self.count = members(name, nx, ny)
        self.slot = {"core": self.core, "z": gy, "plane": self.plane}[name]

    def peer(self, step):
        if self.count == 2:
            other = 1 - self.slot
        else:
            other = self.slot + step
            other = jnp.where(other >= self.count, other - self.count, other)
        if self.name == "core":
            return 2 * self.plane + other, self.gy
        if self.name == "z":
            return self.gx, other
        return 2 * other + self.core, self.gy


def is_first(k):
    return k in STARTS


def kernel(nx, ny, conc_in, pots_in, diff_in, exch_in, slope_in, tall_out, plane_out,
           tall, vecs, planes, outbox, halo, rows, conc, pots, diff, exch, slope, hs_sem, hr_sem, in_sem,
           *for_sums):
    *sums, sum_sems = for_sums
    loads = [
        pltpu.make_async_copy(source, target, in_sem.at[i])
        for i, (source, target) in enumerate((
            (conc_in, conc), (diff_in, diff), (exch_in, exch), (slope_in, slope), (pots_in, pots)))]
    for load in loads:
        load.start()

    gx = lax.axis_index("gx")
    gy = lax.axis_index("gy")
    groups = [Group(names, nx, ny, gx, gy) for names in STAGES]

    exists = {}
    for a, b in BLOCKS:
        inside = []
        if a:
            inside.append(gx + a < nx if a > 0 else gx + a >= 0)
        if b:
            inside.append(gy + b < ny if b > 0 else gy + b >= 0)
        exists[a, b] = inside[0] if len(inside) == 1 else jnp.logical_and(*inside)

    barrier = pltpu.get_barrier_semaphore()
    expected = 0
    for group in groups:
        for step in range(1, group.count):
            pl.semaphore_signal(
                barrier, inc=1, device_id=group.peer(step), device_id_type=MESH)
        expected = expected + group.count - 1
    for block in BLOCKS:
        @pl.when(exists[block])
        def _(block=block):
            pl.semaphore_signal(
                barrier, inc=1, device_id=(gx + block[0], gy + block[1]), device_id_type=MESH)
        expected = expected + exists[block].astype(jnp.int32)

    lane = lax.broadcasted_iota(jnp.int32, (8, 128), 1)
    sub = lax.broadcasted_iota(jnp.int32, (8, 128), 0)
    quarter = lane // 32
    x_of = (lane // 16) % 2
    y_of = lane % 16
    once = jnp.logical_and(sub == 0, quarter == 0)
    zero = jnp.zeros((8, 128), jnp.float32)

    for block in BLOCKS:
        @pl.when(jnp.logical_not(exists[block]))
        def _(block=block):
            for turn in range(len(ROUNDS)):
                count = message_rows(turn, block)
                if count:
                    halo[turn, SLOT[block], 0:count] = jnp.zeros((count, 128), jnp.float32)

    def spread(by_node):
        parts = [by_node[8 * q:8 * q + 8, :] for q in range(4)]
        return jnp.concatenate(parts, axis=1)

    def small(ref):
        return spread(ref[...].reshape(CELLS, CELLS).T)

    for load in loads:
        load.wait()
    diffusion = small(diff)
    exchange = small(exch)
    slopes = small(slope)
    pots_t = pots[...].reshape(CELLS, CELLS + 1).T
    pot = spread(pots_t[:CELLS])
    collector = jnp.broadcast_to(
        jnp.concatenate([pots_t[CELLS:CELLS + 1]] * 4, axis=1), (8, 128))
    planes[0, 0:8] = pot
    planes[0, 8:16] = collector
    rows[...] = jnp.zeros((128, 128), jnp.float32)

    flat = conc[...].reshape(CELLS, 2048)
    for g in range(4):
        block = jnp.concatenate(
            [flat[:, (4 * q + g) * 128:(4 * q + g + 1) * 128] for q in range(4)], axis=0)
        tall[g * 128:(g + 1) * 128, :] = block.T

    def pack(fields, side):
        start = 16 - WIDE if side == 1 else 0
        packed = zero
        for i, field in enumerate(fields):
            shift = (WIDE * i - start) % 128
            moved = pltpu.roll(field, shift, 1) if shift else field
            packed = jnp.where(jnp.logical_and(y_of >= WIDE * i, y_of < WIDE * (i + 1)), moved, packed)
        return packed

    def unpack(packed, i, side):
        start = 16 - WIDE if side == 1 else 0
        shift = (start - WIDE * i) % 128
        return pltpu.roll(packed, shift, 1) if shift else packed

    def fill_outbox(turn, pot, collector, shells, coefs):
        for i, field in enumerate([pot, collector] + coefs + shells):
            outbox[turn, 0, 8 * i:8 * i + 8] = field
        for side in (1, -1):
            fields = [pack([pot, collector] + shells[:1], side)]
            if coefs:
                fields.append(pack(coefs, side))
            if len(shells) > 1:
                fields.append(pack(shells[1:], side))
            for i, field in enumerate(fields):
                outbox[turn, side % 3, 8 * i:8 * i + 8] = field

    fill_outbox(0, pot, collector,
                [tall[pl.ds(SHELLS - 1 - i, 8, stride=SHELLS), :] for i in range(ROUNDS[0] - 1)],
                [exchange, slopes, diffusion])

    def first(b, acc):
        for i in range(8):
            r = b * 8 + i
            shell = tall[pl.ds(r, 8, stride=SHELLS), :]
            vecs[0, r] = shell
            acc = acc + shell * shell
        return acc

    def keep(k, i, acc):
        total = jnp.sum(acc, axis=0, keepdims=True)
        rows[DIM * k + i:DIM * k + i + 1, :] = total
        if i != k:
            rows[DIM * i + k:DIM * i + k + 1, :] = total

    def halo_copy(turn, block):
        a, b = block
        count = message_rows(turn, block)
        return pltpu.make_async_remote_copy(
            src_ref=outbox.at[turn, b % 3, pl.ds(0, count)],
            dst_ref=halo.at[turn, SLOT[-a, -b], pl.ds(0, count)],
            send_sem=hs_sem.at[turn, SLOT[block]],
            recv_sem=hr_sem.at[turn, SLOT[-a, -b]],
            device_id=(gx + a, gy + b),
            device_id_type=MESH,
        )

    def each_message(turn, act):
        for block in BLOCKS:
            if message_rows(turn, block):
                @pl.when(exists[block])
                def _(block=block):
                    act(block)

    def receive(turn, block):
        a, b = block
        count = message_rows(turn, block)
        pltpu.make_async_remote_copy(
            src_ref=outbox.at[turn, b % 3, pl.ds(0, count)],
            dst_ref=halo.at[turn, SLOT[block], pl.ds(0, count)],
            send_sem=hs_sem.at[turn, SLOT[block]],
            recv_sem=hr_sem.at[turn, SLOT[block]],
            device_id=(gx + a, gy + b),
            device_id_type=MESH,
        ).wait_recv()

    def send_round(turn):
        each_message(turn, lambda block: halo_copy(turn, block).start())

    pl.semaphore_wait(barrier, expected)
    send_round(0)
    acc = lax.fori_loop(0, 8, first, zero)
    keep(0, 0, acc + pot * pot + jnp.where(once, collector * collector, 0.0))

    def around(own, low_x, high_x, low_y, high_y):
        high = own if high_x is None else own + high_x
        low = own if low_x is None else own + low_x
        before = 0.0 if low_y is None else pltpu.roll(low_y, 113, 1)
        after = 0.0 if high_y is None else pltpu.roll(high_y, 15, 1)
        return (jnp.where(x_of == 1, pltpu.roll(high, 16, 1), pltpu.roll(low, 112, 1))
                + jnp.where(y_of > 0, pltpu.roll(own, 1, 1), before)
                + jnp.where(y_of < 15, pltpu.roll(own, 127, 1), after))

    def node_mirror(v):
        down = pltpu.roll(v, 1, 0)
        down = jnp.where(sub == 0, pltpu.roll(down, 32, 1), down)
        down = jnp.where(jnp.logical_and(sub == 0, quarter == 0), v, down)
        up = pltpu.roll(v, 7, 0)
        up = jnp.where(sub == 7, pltpu.roll(up, 96, 1), up)
        up = jnp.where(jnp.logical_and(sub == 7, quarter == 3), v, up)
        return 2.0 * v - down - up

    def over_quarters(v):
        return (v + pltpu.roll(v, 32, 1)) + (pltpu.roll(v, 64, 1) + pltpu.roll(v, 96, 1))

    def placed(block):
        return sub == block[0] + MIDDLE

    inside = {}
    for b in (-1, 0, 1):
        inside[b] = jnp.where(placed((0, b)), 1.0, 0.0) if b == 0 else zero
        for block in BLOCKS:
            if block[1] == b:
                inside[b] = jnp.where(
                    jnp.logical_and(placed(block), exists[block]), 1.0, inside[b])

    def potentials(turn, beside_step):
        depth, start = ROUNDS[turn], STARTS[turn]
        carried = ROUNDS[turn + 1] - 1 if turn + 1 < len(ROUNDS) else 0
        own = (0, 0)
        now = {own: (planes[start, 0:8],
                     [vecs[start, SHELLS - 1 - i] for i in range(depth + carried)])}
        coefs = {own: (exchange, slopes, diffusion)}
        fields = {-1: zero, 0: jnp.where(placed(own), planes[start, 8:16], 0.0), 1: zero}
        for block in BLOCKS:
            if message_rows(turn, block) == 0:
                continue
            updates = depth - steps_away(block)
            inbox = halo.at[turn, SLOT[block]]
            a, b = block
            if b:
                names = fields_of(turn, updates)
                found = {name: inbox[8 * i:8 * i + 8] for i, name in enumerate(names)}
                fields[b] = jnp.where(placed(block), found["pots"], fields[b])
                shells = [unpack(found["pots"], 2, -b)] if updates else []
                shells += [unpack(found["shells"], i, -b) for i in range(updates - 1)]
                now[block] = (unpack(found["pots"], 0, -b), shells)
                if updates:
                    source = halo[0, SLOT[block], 8:16]
                    coefs[block] = tuple(unpack(source, i, -b) for i in range(3))
                continue
            shells_at = 16 + (COEFS if turn == 0 else 0)
            fields[0] = jnp.where(placed(block), inbox[8:16], fields[0])
            now[block] = (inbox[0:8],
                          [inbox[shells_at + 8 * i:shells_at + 8 * i + 8] for i in range(updates)])
            if updates:
                source = halo.at[0, SLOT[block]]
                coefs[block] = (source[16:24], source[24:32], source[32:40])
        for b in (-1, 1):
            fields[b] = unpack(fields[b], 1, -b)
        before = fields_before = None
        for m in range(1, depth + 1):
            scale = (1.0 if m == 1 else 2.0) / HALF
            after, fields_after = {}, {}
            means = {-1: zero, 0: zero, 1: zero}
            for block in now:
                if steps_away(block) > depth - m:
                    continue
                a, b = block
                pot, shells = now[block]
                exchange_of, slope_of, diffusion_of = coefs[block]
                beside = [now.get(other) for other in (
                    (a - 1, b), (a + 1, b), (a, b - 1), (a, b + 1))]
                collector = jnp.broadcast_to(fields[b][a + MIDDLE:a + MIDDLE + 1], (8, 128))
                current = exchange_of * (pot - collector)
                means[b] = jnp.where(
                    placed(block),
                    jnp.broadcast_to(jnp.sum(current, axis=0, keepdims=True), (8, 128)), means[b])
                lateral = 4.0 * pot - around(
                    pot, *(None if other is None else other[0] for other in beside))
                new_pot = scale * (
                    node_cond * node_mirror(pot) + current - slope_of * shells[0]
                    + plane_cond * lateral - CENTER * pot)
                count = depth - m + carried if block == own else depth - steps_away(block) - m
                center_coef = scale * (1.0 - CENTER + 2.0 * diffusion_of)
                side_coef = scale * diffusion_of
                new_shells = []
                for i in range(count):
                    new = center_coef * shells[i] - side_coef * (shells[max(i - 1, 0)] + shells[i + 1])
                    if i == 0:
                        new = new + scale * current
                    if m > 1:
                        new = new - before[block][1][i]
                    new_shells.append(new)
                if m > 1:
                    new_pot = new_pot - before[block][0]
                if block != own:
                    new_pot = jnp.where(exists[block], new_pot, 0.0)
                after[block] = (new_pot, new_shells)
            for b in (-1, 0, 1):
                if m + abs(b) > depth:
                    fields_after[b] = zero
                    continue
                field = fields[b]
                lateral = 4.0 * field - around(
                    field, pltpu.roll(field, 1, 0), pltpu.roll(field, 7, 0),
                    fields.get(b - 1), fields.get(b + 1))
                new = scale * (collector_cond * lateral
                               - over_quarters(means[b]) * (1.0 / 32.0) - CENTER * field)
                if m > 1:
                    new = new - fields_before[b]
                fields_after[b] = jnp.where(inside[b] > 0.0, new, 0.0)
            planes[start + m, 0:8] = after[own][0]
            planes[start + m, 8:16] = jnp.broadcast_to(
                fields_after[0][MIDDLE:MIDDLE + 1], (8, 128))
            before, now = now, after
            fields_before, fields = fields, fields_after
            beside_step(start + m)
        if turn + 1 < len(ROUNDS):
            fill_outbox(turn + 1, now[own][0], planes[start + depth, 8:16], now[own][1], [])


    def bulk_shells(k, unrolled=False):
        scale = (1.0 if is_first(k) else 2.0) / HALF
        current = exchange * (planes[k, 0:8] - planes[k, 8:16])
        center_coef = scale * (1.0 - CENTER + 2.0 * diffusion)
        side_coef = scale * diffusion

        def shells(base, accs, last):
            accs = list(accs)
            low = vecs[k, max(base - 1, 0) if isinstance(base, int) else jnp.maximum(base - 1, 0)]
            here = vecs[k, base]
            for i in range(8):
                r = base + i
                high = here if last and i == 7 else vecs[k, r + 1]
                new = center_coef * here - side_coef * (low + high)
                if last and i == 7:
                    new = new + scale * current
                if not is_first(k):
                    new = new - vecs[k - 1, r]
                vecs[k + 1, r] = new
                for m in range(k):
                    accs[m] = accs[m] + new * vecs[m, r]
                accs[k] = accs[k] + new * here
                accs[k + 1] = accs[k + 1] + new * new
                low, here = here, high
            return tuple(accs)

        accs = (zero,) * (k + 2)
        if unrolled:
            for b in range(7):
                accs = shells(b * 8, accs, False)
        else:
            accs = lax.fori_loop(0, 7, lambda b, accs: shells(b * 8, accs, False), accs)
        return shells(SHELLS - 8, accs, True)

    def products(k, accs):
        new_pot, new_collector = planes[k + 1, 0:8], planes[k + 1, 8:16]
        for m in range(k + 2):
            acc = accs[m] + new_pot * planes[m, 0:8] + jnp.where(
                once, new_collector * planes[m, 8:16], 0.0)
            keep(k + 1, m, acc)

    for turn, start in enumerate(STARTS):
        end = start + ROUNDS[turn]
        accs = {start: bulk_shells(start)}
        each_message(turn, functools.partial(receive, turn))
        if turn + 1 < len(ROUNDS):
            potentials(turn, lambda k: None)
            send_round(turn + 1)
            for k in range(start + 1, end):
                accs[k] = bulk_shells(k)
        else:
            def beside(k):
                products(k - 1, accs[k - 1])
                if k < end:
                    accs[k] = bulk_shells(k, True)

            potentials(turn, beside)
            continue
        for k in range(start, end):
            products(k, accs[k])

    def copy(stage, step):
        group = groups[stage]
        return pltpu.make_async_remote_copy(
            src_ref=sums[stage].at[group.slot],
            dst_ref=sums[stage].at[group.slot],
            send_sem=sum_sems.at[stage, 0],
            recv_sem=sum_sems.at[stage, 1],
            device_id=group.peer(step),
            device_id_type=MESH,
        )

    def all_copies(stage):
        group = groups[stage]
        rest = sums[stage].at[pl.ds(0, group.count - 1)]
        return pltpu.make_async_remote_copy(
            src_ref=rest,
            dst_ref=rest,
            send_sem=sum_sems.at[stage, 0],
            recv_sem=sum_sems.at[stage, 1],
            device_id=group.peer(1),
            device_id_type=MESH,
        )

    whole = jnp.sum(rows[...].T, axis=0, keepdims=True)
    for stage, group in enumerate(groups):
        sums[stage][pl.ds(group.slot, 1)] = whole.reshape(1, 1, 128)
        for step in range(1, group.count):
            copy(stage, step).start()
        all_copies(stage).wait_recv()
        whole = jnp.sum(sums[stage][...], axis=0)

    lane2 = lax.broadcasted_iota(jnp.int32, (16, 128), 1)
    sub2 = lax.broadcasted_iota(jnp.int32, (16, 128), 0)
    eye = sub2 == lane2
    whole = jnp.broadcast_to(whole, (16, 128))
    gram = jnp.zeros((16, 128), jnp.float32)
    for k in range(DIM):
        moved = whole if k == 0 else pltpu.roll(whole, (128 - DIM * k) % 128, 1)
        gram = jnp.where(sub2 == k, moved, gram)
    gram = jnp.where(lane2 < DIM, gram, 0.0)

    def down(v):
        return jnp.broadcast_to(jnp.sum(v, axis=0, keepdims=True), (16, 128))

    def turned(v):
        return jnp.broadcast_to(
            jnp.sum(jnp.where(eye, v, 0.0), axis=1, keepdims=True), (16, 128))

    diagonal = jnp.broadcast_to(
        jnp.sum(jnp.where(eye, gram, 0.0), axis=1, keepdims=True), (16, 128))
    lengths = jnp.sqrt(jnp.maximum(diagonal, 0.0))
    start_square = jnp.broadcast_to(diagonal[0:1], (16, 128)) + epsilon
    inverse = lax.rsqrt(start_square)
    beta = start_square * inverse
    up_coef = jnp.zeros((16, 128), jnp.float32)
    down_coef = jnp.zeros((16, 128), jnp.float32)
    for k in range(ITERS):
        up_coef = jnp.where(sub2 == k + 1, HALF if is_first(k) else HALF / 2, up_coef)
        if not is_first(k):
            down_coef = jnp.where(sub2 == k - 1, HALF / 2, down_coef)

    u_lane = jnp.where(lane2 == 0, 1.0, 0.0)
    u_sub = jnp.where(sub2 == 0, 1.0, 0.0)
    gu_lane = jnp.broadcast_to(gram[0:1], (16, 128))
    gu_sub = turned(gu_lane)
    rest_t = jnp.where(eye, 1.0, 0.0)
    gram_rest_t = gram
    images = jnp.zeros((16, 128), jnp.float32)
    coords = []
    trust = jnp.ones((16, 128), jnp.float32)

    cosines, sines, inverse_radii, upper = [], [], [], []
    target = [beta[0:1]]
    for j in range(ITERS):
        image = (CENTER * u_sub + up_coef * pltpu.roll(u_sub, 1, 0)
                 + down_coef * pltpu.roll(u_sub, 15, 0))
        p_lane = down(rest_t * image)
        gp_lane = down(gram_rest_t * image)
        p_sub, gp_sub = turned(p_lane), turned(gp_lane)
        h_sub = turned(down(images * image)) * inverse
        own = down(gu_sub * image) * (inverse * inverse)
        coords.append(u_sub * inverse)
        c_lane, g_sub, g_lane = u_lane * inverse, gu_sub * inverse, gu_lane * inverse
        rest_t = rest_t - g_sub * c_lane
        gram_rest_t = gram_rest_t - g_sub * g_lane
        images = jnp.where(lane2 == j, g_sub, images)
        u_sub, u_lane = (p_sub - u_sub * own) * inverse, (p_lane - u_lane * own) * inverse
        gu_sub, gu_lane = (gp_sub - gu_sub * own) * inverse, (gp_lane - gu_lane * own) * inverse
        square = down(u_sub * gu_sub)
        spread_square = down(jnp.abs(u_sub) * lengths)
        trust = jnp.where(square > TRUST * spread_square * spread_square, trust, 0.0)
        square = jnp.maximum(square, 0.0) + epsilon
        inverse = lax.rsqrt(square)
        entries = ([h_sub[i:i + 1] for i in range(j)] + [own[0:1], (square * inverse)[0:1]])
        for row in range(j):
            entries[row], entries[row + 1] = (
                cosines[row] * entries[row] + sines[row] * entries[row + 1],
                cosines[row] * entries[row + 1] - sines[row] * entries[row])
        inverse_radius = lax.rsqrt(entries[j] * entries[j] + entries[j + 1] * entries[j + 1])
        cosines.append(entries[j] * inverse_radius)
        sines.append(entries[j + 1] * inverse_radius)
        inverse_radii.append(inverse_radius)
        upper.append(entries[:j])
        lead = target[j]
        target[j] = cosines[j] * lead
        target.append(-sines[j] * lead)
    weights = [None] * ITERS
    for row in range(ITERS - 1, -1, -1):
        value = target[row]
        for later in range(ITERS - 1, row, -1):
            value = value - upper[later][row] * weights[later]
        weights[row] = value * inverse_radii[row]
    coef = weights[0] * coords[0]
    for j in range(1, ITERS):
        coef = coef + weights[j] * coords[j]
    plane_out[16:24] = trust[0:8]
    coefs = [jnp.broadcast_to(coef[k:k + 1], (8, 128)) for k in range(ITERS)]

    def combine(b, carry):
        for i in range(8):
            r = b * 8 + i
            value = coefs[0] * vecs[0, r]
            for k in range(1, ITERS):
                value = value + coefs[k] * vecs[k, r]
            tall_out[pl.ds(r, 8, stride=SHELLS), :] = value
        return carry

    lax.fori_loop(0, 8, combine, 0)
    sol = coefs[0] * planes[0, 0:8]
    sol_collector = coefs[0] * planes[0, 8:16]
    for k in range(1, ITERS):
        sol = sol + coefs[k] * planes[k, 0:8]
        sol_collector = sol_collector + coefs[k] * planes[k, 8:16]
    plane_out[0:8] = sol
    plane_out[8:16] = sol_collector

    for turn in range(len(ROUNDS)):
        each_message(turn, lambda block: halo_copy(turn, block).wait_send())
    for stage in range(len(STAGES)):
        all_copies(stage).wait_send()


def results(tall, planes, out_c, out_p, flag):
    for g in range(4):
        block = tall[g * 128:(g + 1) * 128, :].T
        for q in range(4):
            at = (4 * q + g) * 128
            out_c[:, :, at:at + 128] = block[q * 32:(q + 1) * 32].reshape(2, 16, 128)
    flag[0, 0] = jnp.min(planes[16:24])
    sol = planes[0:8]
    by_node = [sol if q == 0 else pltpu.roll(sol, 128 - 32 * q, 1) for q in range(4)]
    by_node = jnp.concatenate(
        by_node + [planes[8:16], jnp.zeros((88, 128), jnp.float32)], axis=0)
    out_p[...] = by_node.T[:CELLS, :CELLS + 1].reshape(2, 16, CELLS + 1)


def fast(nx, ny, *args):
    counts = [members(names, nx, ny) for names in STAGES]
    f32 = jnp.float32
    vmem = pl.BlockSpec(memory_space=pltpu.VMEM)
    tall, planes = pl.pallas_call(
        functools.partial(kernel, nx, ny),
        out_shape=(
            pltpu.VMEM((512, 128), f32),
            pltpu.VMEM((24, 128), f32),
        ),
        in_specs=[pl.BlockSpec(memory_space=pltpu.HBM)] * 5,
        out_specs=(vmem, vmem),
        scratch_shapes=[
            pltpu.VMEM((512, 128), f32),
            pltpu.VMEM((DIM, SHELLS, 8, 128), f32),
            pltpu.VMEM((DIM, 16, 128), f32),
            pltpu.VMEM((len(ROUNDS), 3, OUTBOX, 128), f32),
            pltpu.VMEM((len(ROUNDS), len(BLOCKS), OUTBOX, 128), f32),
            pltpu.VMEM((128, 128), f32),
            *(pltpu.VMEM(a.shape, f32) for a in args),
            pltpu.SemaphoreType.DMA((len(ROUNDS), len(BLOCKS))),
            pltpu.SemaphoreType.DMA((len(ROUNDS), len(BLOCKS))),
            pltpu.SemaphoreType.DMA((5,)),
            *(pltpu.VMEM((count, 1, 128), f32) for count in counts),
            pltpu.SemaphoreType.DMA((len(STAGES), 2)),
        ],
        compiler_params=pltpu.CompilerParams(collective_id=0, has_side_effects=True),
    )(*args)
    return pl.pallas_call(
        results,
        out_shape=(*(jax.ShapeDtypeStruct(a.shape, f32) for a in args[:2]),
                   jax.ShapeDtypeStruct((1, 1), f32)),
        in_specs=[vmem] * 2,
        out_specs=(vmem, vmem, pl.BlockSpec(memory_space=pltpu.SMEM)),
    )(*(pltpu.with_memory_space_constraint(a, pltpu.VMEM) for a in (tall, planes)))


def with_halo(shard, sides, width):
    edges = {}
    for axis, dim in sides:
        size, length = (lax.axis_size(axis), shard.shape[dim])
        up = [(i, (i + 1) % size) for i in range(size - 1)]
        last = lax.slice_in_dim(shard, length - width, length, axis=dim)
        initial = lax.slice_in_dim(shard, 0, width, axis=dim)
        edges[dim] = (
            lax.ppermute(last, axis, up),
            lax.ppermute(initial, axis, [(b, a) for a, b in up]),
        )
    done = []
    for _, dim in sides:
        low, high = edges[dim]
        around = [(width, width) if d in done else (0, 0) for d in range(shard.ndim)]
        shard = jnp.concatenate([jnp.pad(low, around), shard, jnp.pad(high, around)], axis=dim)
        done.append(dim)
    return shard


def total_of(shard):
    return lax.all_gather(shard, ("gx", "gy")).sum(axis=0)


def mirror_laplace(values):
    inner = jnp.concatenate([values[..., :1], values[..., :-1]], axis=-1)
    outer = jnp.concatenate([values[..., 1:], values[..., -1:]], axis=-1)
    return 2.0 * values - inner - outer


def local_operator(conc, padded, diffusion, exchange, slope):
    nodes = exchange.shape[2]
    shell_count = conc.shape[2] // nodes
    shells = conc.reshape(conc.shape[0], conc.shape[1], nodes, shell_count)
    center = padded[1:-1, 1:-1]
    lateral = (
        4.0 * center - padded[2:, 1:-1] - padded[:-2, 1:-1] - padded[1:-1, 2:] - padded[1:-1, :-2]
    )
    node_pot = center[..., :nodes]
    collector = center[..., nodes]
    current = exchange * (node_pot - collector[..., None])
    surface = shells[..., shell_count - 1]
    surface_flag = (lax.broadcasted_iota(jnp.int32, (shell_count,), 0) == shell_count - 1).astype(
        jnp.float32
    )
    new_shells = (
        shells + diffusion[..., None] * mirror_laplace(shells) + current[..., None] * surface_flag
    )
    new_nodes = (
        node_cond * mirror_laplace(node_pot)
        + current
        - slope * surface
        + plane_cond * lateral[..., :nodes]
    )
    new_collector = collector_cond * lateral[..., nodes] - jnp.mean(current, axis=-1)
    return (
        new_shells.reshape(conc.shape),
        jnp.concatenate([new_nodes, new_collector[..., None]], axis=-1),
    )


def step_by_step(rhs_conc, rhs_pots, diffusion, exchange, slope):
    first = jnp.sum(rhs_conc * rhs_conc) + jnp.sum(rhs_pots * rhs_pots)
    start_norm = jnp.sqrt(total_of(first.reshape(1))[0] + epsilon)
    all_conc = jnp.zeros((DIM, *rhs_conc.shape), jnp.float32).at[0].set(rhs_conc / start_norm)
    all_pots = jnp.zeros((DIM, *rhs_pots.shape), jnp.float32).at[0].set(rhs_pots / start_norm)
    matrix = jnp.zeros((DIM, DIM), jnp.float32)

    def arnoldi(step, state):
        all_conc, all_pots, matrix = state
        padded = with_halo(all_pots[step], (("gx", 0), ("gy", 1)), 1)
        image_conc, image_pots = local_operator(all_conc[step], padded, diffusion, exchange, slope)
        local_dots = jnp.sum(all_conc * image_conc, axis=(1, 2, 3)) + jnp.sum(
            all_pots * image_pots, axis=(1, 2, 3))
        coeffs = total_of(local_dots)
        rest_conc = image_conc - jnp.sum(coeffs[:, None, None, None] * all_conc, axis=0)
        rest_pots = image_pots - jnp.sum(coeffs[:, None, None, None] * all_pots, axis=0)
        rest = jnp.sum(rest_conc * rest_conc) + jnp.sum(rest_pots * rest_pots)
        height = jnp.sqrt(total_of(rest.reshape(1))[0] + epsilon)
        column = jnp.where(jnp.arange(DIM) == step + 1, height, coeffs)
        return (
            lax.dynamic_update_index_in_dim(all_conc, rest_conc / height, step + 1, 0),
            lax.dynamic_update_index_in_dim(all_pots, rest_pots / height, step + 1, 0),
            lax.dynamic_update_index_in_dim(matrix, column, step, 0),
        )

    all_conc, all_pots, matrix = lax.fori_loop(
        0, ITERS, arnoldi, (all_conc, all_pots, matrix))

    def rotate(step, state):
        matrix, target = state
        pair = matrix[step]
        lead, under = pair[step], pair[step + 1]
        radius = jnp.sqrt(lead * lead + under * under)
        cosine, sine = lead / radius, under / radius

        def turn(values):
            a = lax.dynamic_index_in_dim(values, step, values.ndim - 1)
            b = lax.dynamic_index_in_dim(values, step + 1, values.ndim - 1)
            values = lax.dynamic_update_slice_in_dim(
                values, cosine * a + sine * b, step, values.ndim - 1)
            return lax.dynamic_update_slice_in_dim(
                values, cosine * b - sine * a, step + 1, values.ndim - 1)

        return turn(matrix), turn(target)

    target = jnp.zeros((DIM,), jnp.float32).at[0].set(start_norm)
    matrix, target = lax.fori_loop(0, ITERS, rotate, (matrix, target))

    def back(i, weights):
        row = ITERS - 1 - i
        known = jnp.sum(matrix[:, row] * weights)
        return weights.at[row].set((target[row] - known) / matrix[row, row])

    weights = lax.fori_loop(0, ITERS, back, jnp.zeros((DIM,), jnp.float32))
    weights = weights[:, None, None, None]
    return jnp.sum(weights * all_conc, axis=0), jnp.sum(weights * all_pots, axis=0)


def solution(mesh):
    nx, ny = mesh.shape["gx"], mesh.shape["gy"]

    def shards(*args):
        conc, pots, flag = fast(nx, ny, *args)

        def again(state):
            conc, pots = step_by_step(*args)
            return conc, pots, jnp.ones_like(state[2])

        return lax.while_loop(
            lambda state: state[2] < 0.5, again, (conc, pots, flag[0, 0]))[:2]

    spec = P("gx", "gy", None)
    return jax.shard_map(
        shards, mesh=mesh, in_specs=(spec,) * 5, out_specs=(spec,) * 2, check_vma=False)
```

```python
import functools
import jax
import jax.numpy as jnp
from jax import lax
from jax.experimental import pallas as pl
from jax.experimental.pallas import tpu as pltpu
from jax.sharding import Mesh
from jax.sharding import PartitionSpec as P

ITERS = 10
MESH = pl.DeviceIdType.MESH
GX = ("gx_0", "gx_1", "gx_2")

node_cond = 1.0
plane_cond = 0.5
collector_cond = 2.0
epsilon = 1e-06

ROUNDS = (5, 5)
CENTER = 11.0
HALF = 10.0
TRUST = 4e-4

CELLS = 32
SHELLS = 64
DIM = ITERS + 1
STARTS = tuple(sum(ROUNDS[:i]) for i in range(len(ROUNDS)))


def steps_away(block):
    a, b = block
    return max(2 * abs(a) - 1, 0) + abs(b)


DEEPEST = max(ROUNDS)
BLOCKS = sorted(
    ((a, b) for a in range(-DEEPEST, DEEPEST + 1) for b in (-1, 0, 1)
     if 0 < steps_away((a, b)) <= DEEPEST),
    key=lambda block: (-steps_away(block), block))
SLOT = {block: i for i, block in enumerate(BLOCKS)}
COEFS = 24
OUTBOX = 16 + COEFS + 8 * (DEEPEST - 1)


def message_rows(turn, block):
    updates = ROUNDS[turn] - steps_away(block)
    if updates < 0:
        return 0
    if block[1]:
        return 8 * len(fields_of(turn, updates))
    if updates == 0:
        return 16
    return 16 + (COEFS if turn == 0 else 0) + 8 * updates


MIDDLE = 3
assert max(abs(a) for a, _ in BLOCKS) <= MIDDLE
WIDE = 5
assert DEEPEST <= WIDE


def fields_of(turn, updates):
    names = ["pots"]
    if updates and turn == 0:
        names.append("coefs")
    if updates > 1:
        names.append("shells")
    return names


STAGES = ("core", "z", "plane")


def members(name, nx, ny):
    return {"core": 2, "z": ny, "plane": nx // 2}[name]


class Group:
    def __init__(self, name, nx, ny, gx, gy):
        self.name, self.gx, self.gy = name, gx, gy
        self.core, self.plane = lax.rem(gx, 2), lax.div(gx, 2)
        self.count = members(name, nx, ny)
        self.slot = {"core": self.core, "z": gy, "plane": self.plane}[name]

    def peer(self, step):
        if self.count == 2:
            other = 1 - self.slot
        else:
            other = self.slot + step
            other = jnp.where(other >= self.count, other - self.count, other)
        if self.name == "core":
            return 2 * self.plane + other, self.gy
        if self.name == "z":
            return self.gx, other
        return 2 * other + self.core, self.gy


def is_first(k):
    return k in STARTS


def kernel(nx, ny, conc_in, pots_in, diff_in, exch_in, slope_in, tall_out, plane_out,
           tall, vecs, planes, outbox, halo, rows, conc, pots, diff, exch, slope, hs_sem, hr_sem, in_sem,
           *for_sums):
    *sums, sum_sems = for_sums
    loads = [
        pltpu.make_async_copy(source, target, in_sem.at[i])
        for i, (source, target) in enumerate((
            (conc_in, conc), (diff_in, diff), (exch_in, exch), (slope_in, slope), (pots_in, pots)))]
    for load in loads:
        load.start()

    gx = lax.axis_index("gx")
    gy = lax.axis_index("gy")
    groups = [Group(names, nx, ny, gx, gy) for names in STAGES]

    exists = {}
    for a, b in BLOCKS:
        inside = []
        if a:
            inside.append(gx + a < nx if a > 0 else gx + a >= 0)
        if b:
            inside.append(gy + b < ny if b > 0 else gy + b >= 0)
        exists[a, b] = inside[0] if len(inside) == 1 else jnp.logical_and(*inside)

    barrier = pltpu.get_barrier_semaphore()
    expected = 0
    for group in groups:
        for step in range(1, group.count):
            pl.semaphore_signal(
                barrier, inc=1, device_id=group.peer(step), device_id_type=MESH)
        expected = expected + group.count - 1
    for block in BLOCKS:
        @pl.when(exists[block])
        def _(block=block):
            pl.semaphore_signal(
                barrier, inc=1, device_id=(gx + block[0], gy + block[1]), device_id_type=MESH)
        expected = expected + exists[block].astype(jnp.int32)

    lane = lax.broadcasted_iota(jnp.int32, (8, 128), 1)
    sub = lax.broadcasted_iota(jnp.int32, (8, 128), 0)
    quarter = lane // 32
    x_of = (lane // 16) % 2
    y_of = lane % 16
    once = jnp.logical_and(sub == 0, quarter == 0)
    zero = jnp.zeros((8, 128), jnp.float32)

    for block in BLOCKS:
        @pl.when(jnp.logical_not(exists[block]))
        def _(block=block):
            for turn in range(len(ROUNDS)):
                count = message_rows(turn, block)
                if count:
                    halo[turn, SLOT[block], 0:count] = jnp.zeros((count, 128), jnp.float32)

    def spread(by_node):
        parts = [by_node[8 * q:8 * q + 8, :] for q in range(4)]
        return jnp.concatenate(parts, axis=1)

    def small(ref):
        return spread(ref[...].reshape(CELLS, CELLS).T)

    for load in loads:
        load.wait()
    diffusion = small(diff)
    exchange = small(exch)
    slopes = small(slope)
    pots_t = pots[...].reshape(CELLS, CELLS + 1).T
    pot = spread(pots_t[:CELLS])
    collector = jnp.broadcast_to(
        jnp.concatenate([pots_t[CELLS:CELLS + 1]] * 4, axis=1), (8, 128))
    planes[0, 0:8] = pot
    planes[0, 8:16] = collector
    rows[...] = jnp.zeros((128, 128), jnp.float32)

    flat = conc[...].reshape(CELLS, 2048)
    for g in range(4):
        block = jnp.concatenate(
            [flat[:, (4 * q + g) * 128:(4 * q + g + 1) * 128] for q in range(4)], axis=0)
        tall[g * 128:(g + 1) * 128, :] = block.T

    def pack(fields, side):
        start = 16 - WIDE if side == 1 else 0
        packed = zero
        for i, field in enumerate(fields):
            shift = (WIDE * i - start) % 128
            moved = pltpu.roll(field, shift, 1) if shift else field
            packed = jnp.where(jnp.logical_and(y_of >= WIDE * i, y_of < WIDE * (i + 1)), moved, packed)
        return packed

    def unpack(packed, i, side):
        start = 16 - WIDE if side == 1 else 0
        shift = (start - WIDE * i) % 128
        return pltpu.roll(packed, shift, 1) if shift else packed

    def fill_outbox(turn, pot, collector, shells, coefs):
        for i, field in enumerate([pot, collector] + coefs + shells):
            outbox[turn, 0, 8 * i:8 * i + 8] = field
        for side in (1, -1):
            fields = [pack([pot, collector] + shells[:1], side)]
            if coefs:
                fields.append(pack(coefs, side))
            if len(shells) > 1:
                fields.append(pack(shells[1:], side))
            for i, field in enumerate(fields):
                outbox[turn, side % 3, 8 * i:8 * i + 8] = field

    fill_outbox(0, pot, collector,
                [tall[pl.ds(SHELLS - 1 - i, 8, stride=SHELLS), :] for i in range(ROUNDS[0] - 1)],
                [exchange, slopes, diffusion])

    def first(b, acc):
        for i in range(8):
            r = b * 8 + i
            shell = tall[pl.ds(r, 8, stride=SHELLS), :]
            vecs[0, r] = shell
            acc = acc + shell * shell
        return acc

    def keep(k, i, acc):
        total = jnp.sum(acc, axis=0, keepdims=True)
        rows[DIM * k + i:DIM * k + i + 1, :] = total
        if i != k:
            rows[DIM * i + k:DIM * i + k + 1, :] = total

    def halo_copy(turn, block):
        a, b = block
        count = message_rows(turn, block)
        return pltpu.make_async_remote_copy(
            src_ref=outbox.at[turn, b % 3, pl.ds(0, count)],
            dst_ref=halo.at[turn, SLOT[-a, -b], pl.ds(0, count)],
            send_sem=hs_sem.at[turn, SLOT[block]],
            recv_sem=hr_sem.at[turn, SLOT[-a, -b]],
            device_id=(gx + a, gy + b),
            device_id_type=MESH,
        )

    def each_message(turn, act):
        for block in BLOCKS:
            if message_rows(turn, block):
                @pl.when(exists[block])
                def _(block=block):
                    act(block)

    def receive(turn, block):
        a, b = block
        count = message_rows(turn, block)
        pltpu.make_async_remote_copy(
            src_ref=outbox.at[turn, b % 3, pl.ds(0, count)],
            dst_ref=halo.at[turn, SLOT[block], pl.ds(0, count)],
            send_sem=hs_sem.at[turn, SLOT[block]],
            recv_sem=hr_sem.at[turn, SLOT[block]],
            device_id=(gx + a, gy + b),
            device_id_type=MESH,
        ).wait_recv()

    def send_round(turn):
        each_message(turn, lambda block: halo_copy(turn, block).start())

    pl.semaphore_wait(barrier, expected)
    send_round(0)
    acc = lax.fori_loop(0, 8, first, zero)
    keep(0, 0, acc + pot * pot + jnp.where(once, collector * collector, 0.0))

    def around(own, low_x, high_x, low_y, high_y):
        high = own if high_x is None else own + high_x
        low = own if low_x is None else own + low_x
        before = 0.0 if low_y is None else pltpu.roll(low_y, 113, 1)
        after = 0.0 if high_y is None else pltpu.roll(high_y, 15, 1)
        return (jnp.where(x_of == 1, pltpu.roll(high, 16, 1), pltpu.roll(low, 112, 1))
                + jnp.where(y_of > 0, pltpu.roll(own, 1, 1), before)
                + jnp.where(y_of < 15, pltpu.roll(own, 127, 1), after))

    def node_mirror(v):
        down = pltpu.roll(v, 1, 0)
        down = jnp.where(sub == 0, pltpu.roll(down, 32, 1), down)
        down = jnp.where(jnp.logical_and(sub == 0, quarter == 0), v, down)
        up = pltpu.roll(v, 7, 0)
        up = jnp.where(sub == 7, pltpu.roll(up, 96, 1), up)
        up = jnp.where(jnp.logical_and(sub == 7, quarter == 3), v, up)
        return 2.0 * v - down - up

    def over_quarters(v):
        return (v + pltpu.roll(v, 32, 1)) + (pltpu.roll(v, 64, 1) + pltpu.roll(v, 96, 1))

    def placed(block):
        return sub == block[0] + MIDDLE

    inside = {}
    for b in (-1, 0, 1):
        inside[b] = jnp.where(placed((0, b)), 1.0, 0.0) if b == 0 else zero
        for block in BLOCKS:
            if block[1] == b:
                inside[b] = jnp.where(
                    jnp.logical_and(placed(block), exists[block]), 1.0, inside[b])

    def potentials(turn, beside_step):
        depth, start = ROUNDS[turn], STARTS[turn]
        carried = ROUNDS[turn + 1] - 1 if turn + 1 < len(ROUNDS) else 0
        own = (0, 0)
        now = {own: (planes[start, 0:8],
                     [vecs[start, SHELLS - 1 - i] for i in range(depth + carried)])}
        coefs = {own: (exchange, slopes, diffusion)}
        fields = {-1: zero, 0: jnp.where(placed(own), planes[start, 8:16], 0.0), 1: zero}
        for block in BLOCKS:
            if message_rows(turn, block) == 0:
                continue
            updates = depth - steps_away(block)
            inbox = halo.at[turn, SLOT[block]]
            a, b = block
            if b:
                names = fields_of(turn, updates)
                found = {name: inbox[8 * i:8 * i + 8] for i, name in enumerate(names)}
                fields[b] = jnp.where(placed(block), found["pots"], fields[b])
                shells = [unpack(found["pots"], 2, -b)] if updates else []
                shells += [unpack(found["shells"], i, -b) for i in range(updates - 1)]
                now[block] = (unpack(found["pots"], 0, -b), shells)
                if updates:
                    source = halo[0, SLOT[block], 8:16]
                    coefs[block] = tuple(unpack(source, i, -b) for i in range(3))
                continue
            shells_at = 16 + (COEFS if turn == 0 else 0)
            fields[0] = jnp.where(placed(block), inbox[8:16], fields[0])
            now[block] = (inbox[0:8],
                          [inbox[shells_at + 8 * i:shells_at + 8 * i + 8] for i in range(updates)])
            if updates:
                source = halo.at[0, SLOT[block]]
                coefs[block] = (source[16:24], source[24:32], source[32:40])
        for b in (-1, 1):
            fields[b] = unpack(fields[b], 1, -b)
        before = fields_before = None
        for m in range(1, depth + 1):
            scale = (1.0 if m == 1 else 2.0) / HALF
            after, fields_after = {}, {}
            means = {-1: zero, 0: zero, 1: zero}
            for block in now:
                if steps_away(block) > depth - m:
                    continue
                a, b = block
                pot, shells = now[block]
                exchange_of, slope_of, diffusion_of = coefs[block]
                beside = [now.get(other) for other in (
                    (a - 1, b), (a + 1, b), (a, b - 1), (a, b + 1))]
                collector = jnp.broadcast_to(fields[b][a + MIDDLE:a + MIDDLE + 1], (8, 128))
                current = exchange_of * (pot - collector)
                means[b] = jnp.where(
                    placed(block),
                    jnp.broadcast_to(jnp.sum(current, axis=0, keepdims=True), (8, 128)), means[b])
                lateral = 4.0 * pot - around(
                    pot, *(None if other is None else other[0] for other in beside))
                new_pot = scale * (
                    node_cond * node_mirror(pot) + current - slope_of * shells[0]
                    + plane_cond * lateral - CENTER * pot)
                count = depth - m + carried if block == own else depth - steps_away(block) - m
                center_coef = scale * (1.0 - CENTER + 2.0 * diffusion_of)
                side_coef = scale * diffusion_of
                new_shells = []
                for i in range(count):
                    new = center_coef * shells[i] - side_coef * (shells[max(i - 1, 0)] + shells[i + 1])
                    if i == 0:
                        new = new + scale * current
                    if m > 1:
                        new = new - before[block][1][i]
                    new_shells.append(new)
                if m > 1:
                    new_pot = new_pot - before[block][0]
                if block != own:
                    new_pot = jnp.where(exists[block], new_pot, 0.0)
                after[block] = (new_pot, new_shells)
            for b in (-1, 0, 1):
                if m + abs(b) > depth:
                    fields_after[b] = zero
                    continue
                field = fields[b]
                lateral = 4.0 * field - around(
                    field, pltpu.roll(field, 1, 0), pltpu.roll(field, 7, 0),
                    fields.get(b - 1), fields.get(b + 1))
                new = scale * (collector_cond * lateral
                               - over_quarters(means[b]) * (1.0 / 32.0) - CENTER * field)
                if m > 1:
                    new = new - fields_before[b]
                fields_after[b] = jnp.where(inside[b] > 0.0, new, 0.0)
            planes[start + m, 0:8] = after[own][0]
            planes[start + m, 8:16] = jnp.broadcast_to(
                fields_after[0][MIDDLE:MIDDLE + 1], (8, 128))
            before, now = now, after
            fields_before, fields = fields, fields_after
            beside_step(start + m)
        if turn + 1 < len(ROUNDS):
            fill_outbox(turn + 1, now[own][0], planes[start + depth, 8:16], now[own][1], [])


    def bulk_shells(k, unrolled=False):
        scale = (1.0 if is_first(k) else 2.0) / HALF
        current = exchange * (planes[k, 0:8] - planes[k, 8:16])
        center_coef = scale * (1.0 - CENTER + 2.0 * diffusion)
        side_coef = scale * diffusion

        def shells(base, accs, last):
            accs = list(accs)
            low = vecs[k, max(base - 1, 0) if isinstance(base, int) else jnp.maximum(base - 1, 0)]
            here = vecs[k, base]
            for i in range(8):
                r = base + i
                high = here if last and i == 7 else vecs[k, r + 1]
                new = center_coef * here - side_coef * (low + high)
                if last and i == 7:
                    new = new + scale * current
                if not is_first(k):
                    new = new - vecs[k - 1, r]
                vecs[k + 1, r] = new
                for m in range(k):
                    accs[m] = accs[m] + new * vecs[m, r]
                accs[k] = accs[k] + new * here
                accs[k + 1] = accs[k + 1] + new * new
                low, here = here, high
            return tuple(accs)

        accs = (zero,) * (k + 2)
        if unrolled:
            for b in range(7):
                accs = shells(b * 8, accs, False)
        else:
            accs = lax.fori_loop(0, 7, lambda b, accs: shells(b * 8, accs, False), accs)
        return shells(SHELLS - 8, accs, True)

    def products(k, accs):
        new_pot, new_collector = planes[k + 1, 0:8], planes[k + 1, 8:16]
        for m in range(k + 2):
            acc = accs[m] + new_pot * planes[m, 0:8] + jnp.where(
                once, new_collector * planes[m, 8:16], 0.0)
            keep(k + 1, m, acc)

    for turn, start in enumerate(STARTS):
        end = start + ROUNDS[turn]
        accs = {start: bulk_shells(start, True)}
        each_message(turn, functools.partial(receive, turn))
        if turn + 1 < len(ROUNDS):
            potentials(turn, lambda k: None)
            send_round(turn + 1)
            for k in range(start + 1, end):
                accs[k] = bulk_shells(k)
        else:
            def beside(k):
                if k < end:
                    accs[k] = bulk_shells(k, True)

            potentials(turn, beside)
        for k in range(start, end):
            products(k, accs[k])

    def copy(stage, step):
        group = groups[stage]
        return pltpu.make_async_remote_copy(
            src_ref=sums[stage].at[group.slot],
            dst_ref=sums[stage].at[group.slot],
            send_sem=sum_sems.at[stage, 0],
            recv_sem=sum_sems.at[stage, 1],
            device_id=group.peer(step),
            device_id_type=MESH,
        )

    def all_copies(stage):
        group = groups[stage]
        rest = sums[stage].at[pl.ds(0, group.count - 1)]
        return pltpu.make_async_remote_copy(
            src_ref=rest,
            dst_ref=rest,
            send_sem=sum_sems.at[stage, 0],
            recv_sem=sum_sems.at[stage, 1],
            device_id=group.peer(1),
            device_id_type=MESH,
        )

    whole = jnp.sum(rows[...].T, axis=0, keepdims=True)
    for stage, group in enumerate(groups):
        sums[stage][pl.ds(group.slot, 1)] = whole.reshape(1, 1, 128)
        for step in range(1, group.count):
            copy(stage, step).start()
        all_copies(stage).wait_recv()
        whole = jnp.sum(sums[stage][...], axis=0)

    lane2 = lax.broadcasted_iota(jnp.int32, (16, 128), 1)
    sub2 = lax.broadcasted_iota(jnp.int32, (16, 128), 0)
    eye = sub2 == lane2
    whole = jnp.broadcast_to(whole, (16, 128))
    gram = jnp.zeros((16, 128), jnp.float32)
    for k in range(DIM):
        moved = whole if k == 0 else pltpu.roll(whole, (128 - DIM * k) % 128, 1)
        gram = jnp.where(sub2 == k, moved, gram)
    gram = jnp.where(lane2 < DIM, gram, 0.0)

    def down(v):
        return jnp.broadcast_to(jnp.sum(v, axis=0, keepdims=True), (16, 128))

    def turned(v):
        return jnp.broadcast_to(
            jnp.sum(jnp.where(eye, v, 0.0), axis=1, keepdims=True), (16, 128))

    diagonal = jnp.broadcast_to(
        jnp.sum(jnp.where(eye, gram, 0.0), axis=1, keepdims=True), (16, 128))
    lengths = jnp.sqrt(jnp.maximum(diagonal, 0.0))
    start_square = jnp.broadcast_to(diagonal[0:1], (16, 128)) + epsilon
    inverse = lax.rsqrt(start_square)
    beta = start_square * inverse
    up_coef = jnp.zeros((16, 128), jnp.float32)
    down_coef = jnp.zeros((16, 128), jnp.float32)
    for k in range(ITERS):
        up_coef = jnp.where(sub2 == k + 1, HALF if is_first(k) else HALF / 2, up_coef)
        if not is_first(k):
            down_coef = jnp.where(sub2 == k - 1, HALF / 2, down_coef)

    u_lane = jnp.where(lane2 == 0, 1.0, 0.0)
    u_sub = jnp.where(sub2 == 0, 1.0, 0.0)
    gu_lane = jnp.broadcast_to(gram[0:1], (16, 128))
    gu_sub = turned(gu_lane)
    rest_t = jnp.where(eye, 1.0, 0.0)
    gram_rest_t = gram
    images = jnp.zeros((16, 128), jnp.float32)
    coords = []
    trust = jnp.ones((16, 128), jnp.float32)

    cosines, sines, inverse_radii, upper = [], [], [], []
    target = [beta[0:1]]
    for j in range(ITERS):
        image = (CENTER * u_sub + up_coef * pltpu.roll(u_sub, 1, 0)
                 + down_coef * pltpu.roll(u_sub, 15, 0))
        p_lane = down(rest_t * image)
        gp_lane = down(gram_rest_t * image)
        p_sub, gp_sub = turned(p_lane), turned(gp_lane)
        h_sub = turned(down(images * image)) * inverse
        own = down(gu_sub * image) * (inverse * inverse)
        coords.append(u_sub * inverse)
        c_lane, g_sub, g_lane = u_lane * inverse, gu_sub * inverse, gu_lane * inverse
        rest_t = rest_t - g_sub * c_lane
        gram_rest_t = gram_rest_t - g_sub * g_lane
        images = jnp.where(lane2 == j, g_sub, images)
        u_sub, u_lane = (p_sub - u_sub * own) * inverse, (p_lane - u_lane * own) * inverse
        gu_sub, gu_lane = (gp_sub - gu_sub * own) * inverse, (gp_lane - gu_lane * own) * inverse
        square = down(u_sub * gu_sub)
        spread_square = down(jnp.abs(u_sub) * lengths)
        trust = jnp.where(square > TRUST * spread_square * spread_square, trust, 0.0)
        square = jnp.maximum(square, 0.0) + epsilon
        inverse = lax.rsqrt(square)
        entries = ([h_sub[i:i + 1] for i in range(j)] + [own[0:1], (square * inverse)[0:1]])
        for row in range(j):
            entries[row], entries[row + 1] = (
                cosines[row] * entries[row] + sines[row] * entries[row + 1],
                cosines[row] * entries[row + 1] - sines[row] * entries[row])
        inverse_radius = lax.rsqrt(entries[j] * entries[j] + entries[j + 1] * entries[j + 1])
        cosines.append(entries[j] * inverse_radius)
        sines.append(entries[j + 1] * inverse_radius)
        inverse_radii.append(inverse_radius)
        upper.append(entries[:j])
        lead = target[j]
        target[j] = cosines[j] * lead
        target.append(-sines[j] * lead)
    weights = [None] * ITERS
    for row in range(ITERS - 1, -1, -1):
        value = target[row]
        for later in range(ITERS - 1, row, -1):
            value = value - upper[later][row] * weights[later]
        weights[row] = value * inverse_radii[row]
    coef = weights[0] * coords[0]
    for j in range(1, ITERS):
        coef = coef + weights[j] * coords[j]
    plane_out[16:24] = trust[0:8]
    coefs = [jnp.broadcast_to(coef[k:k + 1], (8, 128)) for k in range(ITERS)]

    def combine(b, carry):
        for i in range(8):
            r = b * 8 + i
            value = coefs[0] * vecs[0, r]
            for k in range(1, ITERS):
                value = value + coefs[k] * vecs[k, r]
            tall_out[pl.ds(r, 8, stride=SHELLS), :] = value
        return carry

    lax.fori_loop(0, 8, combine, 0)
    sol = coefs[0] * planes[0, 0:8]
    sol_collector = coefs[0] * planes[0, 8:16]
    for k in range(1, ITERS):
        sol = sol + coefs[k] * planes[k, 0:8]
        sol_collector = sol_collector + coefs[k] * planes[k, 8:16]
    plane_out[0:8] = sol
    plane_out[8:16] = sol_collector

    for turn in range(len(ROUNDS)):
        each_message(turn, lambda block: halo_copy(turn, block).wait_send())
    for stage in range(len(STAGES)):
        all_copies(stage).wait_send()


def results(tall, planes, out_c, out_p, flag):
    for g in range(4):
        block = tall[g * 128:(g + 1) * 128, :].T
        for q in range(4):
            at = (4 * q + g) * 128
            out_c[:, :, at:at + 128] = block[q * 32:(q + 1) * 32].reshape(2, 16, 128)
    flag[0, 0] = jnp.min(planes[16:24])
    sol = planes[0:8]
    by_node = [sol if q == 0 else pltpu.roll(sol, 128 - 32 * q, 1) for q in range(4)]
    by_node = jnp.concatenate(
        by_node + [planes[8:16], jnp.zeros((88, 128), jnp.float32)], axis=0)
    out_p[...] = by_node.T[:CELLS, :CELLS + 1].reshape(2, 16, CELLS + 1)


def fast(nx, ny, *args):
    counts = [members(names, nx, ny) for names in STAGES]
    f32 = jnp.float32
    vmem = pl.BlockSpec(memory_space=pltpu.VMEM)
    tall, planes = pl.pallas_call(
        functools.partial(kernel, nx, ny),
        out_shape=(
            pltpu.VMEM((512, 128), f32),
            pltpu.VMEM((24, 128), f32),
        ),
        in_specs=[pl.BlockSpec(memory_space=pltpu.HBM)] * 5,
        out_specs=(vmem, vmem),
        scratch_shapes=[
            pltpu.VMEM((512, 128), f32),
            pltpu.VMEM((DIM, SHELLS, 8, 128), f32),
            pltpu.VMEM((DIM, 16, 128), f32),
            pltpu.VMEM((len(ROUNDS), 3, OUTBOX, 128), f32),
            pltpu.VMEM((len(ROUNDS), len(BLOCKS), OUTBOX, 128), f32),
            pltpu.VMEM((128, 128), f32),
            *(pltpu.VMEM(a.shape, f32) for a in args),
            pltpu.SemaphoreType.DMA((len(ROUNDS), len(BLOCKS))),
            pltpu.SemaphoreType.DMA((len(ROUNDS), len(BLOCKS))),
            pltpu.SemaphoreType.DMA((5,)),
            *(pltpu.VMEM((count, 1, 128), f32) for count in counts),
            pltpu.SemaphoreType.DMA((len(STAGES), 2)),
        ],
        compiler_params=pltpu.CompilerParams(collective_id=0, has_side_effects=True),
    )(*args)
    return pl.pallas_call(
        results,
        out_shape=(*(jax.ShapeDtypeStruct(a.shape, f32) for a in args[:2]),
                   jax.ShapeDtypeStruct((1, 1), f32)),
        in_specs=[vmem] * 2,
        out_specs=(vmem, vmem, pl.BlockSpec(memory_space=pltpu.SMEM)),
    )(*(pltpu.with_memory_space_constraint(a, pltpu.VMEM) for a in (tall, planes)))


def with_halo(shard, sides, width):
    edges = {}
    for axis, dim in sides:
        size, length = (lax.axis_size(axis), shard.shape[dim])
        up = [(i, (i + 1) % size) for i in range(size - 1)]
        last = lax.slice_in_dim(shard, length - width, length, axis=dim)
        initial = lax.slice_in_dim(shard, 0, width, axis=dim)
        edges[dim] = (
            lax.ppermute(last, axis, up),
            lax.ppermute(initial, axis, [(b, a) for a, b in up]),
        )
    done = []
    for _, dim in sides:
        low, high = edges[dim]
        around = [(width, width) if d in done else (0, 0) for d in range(shard.ndim)]
        shard = jnp.concatenate([jnp.pad(low, around), shard, jnp.pad(high, around)], axis=dim)
        done.append(dim)
    return shard


def total_of(shard):
    return lax.all_gather(shard, ("gx", "gy")).sum(axis=0)


def mirror_laplace(values):
    inner = jnp.concatenate([values[..., :1], values[..., :-1]], axis=-1)
    outer = jnp.concatenate([values[..., 1:], values[..., -1:]], axis=-1)
    return 2.0 * values - inner - outer


def local_operator(conc, padded, diffusion, exchange, slope):
    nodes = exchange.shape[2]
    shell_count = conc.shape[2] // nodes
    shells = conc.reshape(conc.shape[0], conc.shape[1], nodes, shell_count)
    center = padded[1:-1, 1:-1]
    lateral = (
        4.0 * center - padded[2:, 1:-1] - padded[:-2, 1:-1] - padded[1:-1, 2:] - padded[1:-1, :-2]
    )
    node_pot = center[..., :nodes]
    collector = center[..., nodes]
    current = exchange * (node_pot - collector[..., None])
    surface = shells[..., shell_count - 1]
    surface_flag = (lax.broadcasted_iota(jnp.int32, (shell_count,), 0) == shell_count - 1).astype(
        jnp.float32
    )
    new_shells = (
        shells + diffusion[..., None] * mirror_laplace(shells) + current[..., None] * surface_flag
    )
    new_nodes = (
        node_cond * mirror_laplace(node_pot)
        + current
        - slope * surface
        + plane_cond * lateral[..., :nodes]
    )
    new_collector = collector_cond * lateral[..., nodes] - jnp.mean(current, axis=-1)
    return (
        new_shells.reshape(conc.shape),
        jnp.concatenate([new_nodes, new_collector[..., None]], axis=-1),
    )


def step_by_step(rhs_conc, rhs_pots, diffusion, exchange, slope):
    first = jnp.sum(rhs_conc * rhs_conc) + jnp.sum(rhs_pots * rhs_pots)
    start_norm = jnp.sqrt(total_of(first.reshape(1))[0] + epsilon)
    all_conc = jnp.zeros((DIM, *rhs_conc.shape), jnp.float32).at[0].set(rhs_conc / start_norm)
    all_pots = jnp.zeros((DIM, *rhs_pots.shape), jnp.float32).at[0].set(rhs_pots / start_norm)
    matrix = jnp.zeros((DIM, DIM), jnp.float32)

    def arnoldi(step, state):
        all_conc, all_pots, matrix = state
        padded = with_halo(all_pots[step], (("gx", 0), ("gy", 1)), 1)
        image_conc, image_pots = local_operator(all_conc[step], padded, diffusion, exchange, slope)
        local_dots = jnp.sum(all_conc * image_conc, axis=(1, 2, 3)) + jnp.sum(
            all_pots * image_pots, axis=(1, 2, 3))
        coeffs = total_of(local_dots)
        rest_conc = image_conc - jnp.sum(coeffs[:, None, None, None] * all_conc, axis=0)
        rest_pots = image_pots - jnp.sum(coeffs[:, None, None, None] * all_pots, axis=0)
        rest = jnp.sum(rest_conc * rest_conc) + jnp.sum(rest_pots * rest_pots)
        height = jnp.sqrt(total_of(rest.reshape(1))[0] + epsilon)
        column = jnp.where(jnp.arange(DIM) == step + 1, height, coeffs)
        return (
            lax.dynamic_update_index_in_dim(all_conc, rest_conc / height, step + 1, 0),
            lax.dynamic_update_index_in_dim(all_pots, rest_pots / height, step + 1, 0),
            lax.dynamic_update_index_in_dim(matrix, column, step, 0),
        )

    all_conc, all_pots, matrix = lax.fori_loop(
        0, ITERS, arnoldi, (all_conc, all_pots, matrix))

    def rotate(step, state):
        matrix, target = state
        pair = matrix[step]
        lead, under = pair[step], pair[step + 1]
        radius = jnp.sqrt(lead * lead + under * under)
        cosine, sine = lead / radius, under / radius

        def turn(values):
            a = lax.dynamic_index_in_dim(values, step, values.ndim - 1)
            b = lax.dynamic_index_in_dim(values, step + 1, values.ndim - 1)
            values = lax.dynamic_update_slice_in_dim(
                values, cosine * a + sine * b, step, values.ndim - 1)
            return lax.dynamic_update_slice_in_dim(
                values, cosine * b - sine * a, step + 1, values.ndim - 1)

        return turn(matrix), turn(target)

    target = jnp.zeros((DIM,), jnp.float32).at[0].set(start_norm)
    matrix, target = lax.fori_loop(0, ITERS, rotate, (matrix, target))

    def back(i, weights):
        row = ITERS - 1 - i
        known = jnp.sum(matrix[:, row] * weights)
        return weights.at[row].set((target[row] - known) / matrix[row, row])

    weights = lax.fori_loop(0, ITERS, back, jnp.zeros((DIM,), jnp.float32))
    weights = weights[:, None, None, None]
    return jnp.sum(weights * all_conc, axis=0), jnp.sum(weights * all_pots, axis=0)


def solution(mesh):
    nx, ny = mesh.shape["gx"], mesh.shape["gy"]

    def shards(*args):
        conc, pots, flag = fast(nx, ny, *args)

        def again(state):
            conc, pots = step_by_step(*args)
            return conc, pots, jnp.ones_like(state[2])

        return lax.while_loop(
            lambda state: state[2] < 0.5, again, (conc, pots, flag[0, 0]))[:2]

    spec = P("gx", "gy", None)
    return jax.shard_map(
        shards, mesh=mesh, in_specs=(spec,) * 5, out_specs=(spec,) * 2, check_vma=False)
```
